8 devices in a mesh: dp: 1 (over z), tp: 2 (over y), ctx: 4 (over x, core).
Axes of the slice: x: 2, y: 2, z: 1, core: 2. Of those that a mesh axis runs over, the one named last changes fastest.
Arguments:
- hidden: bfloat16 [512, 4096], P(('dp', 'ctx'))
- w_q: bfloat16 [4096, 4096], P(None, 'tp')
- w_k: bfloat16 [4096, 4096], P(None, 'tp')
- w_v: bfloat16 [4096, 4096], P(None, 'tp')
- w_o: bfloat16 [4096, 4096], P('tp')
- k_prefix: bfloat16 [4096, 32, 128], P(('dp', 'ctx'), 'tp')
- v_prefix: bfloat16 [4096, 32, 128], P(('dp', 'ctx'), 'tp')
- k_suffix: bfloat16 [512, 64, 32, 128], P(('dp', 'ctx'), None, 'tp')
- v_suffix: bfloat16 [512, 64, 32, 128], P(('dp', 'ctx'), None, 'tp')
- seq_lens: int32 [512], P(('dp', 'ctx'))
Outputs:
- output: bfloat16 [512, 4096], P(('dp', 'ctx'))
All inputs are finite; a program needn't handle non-finite values.
Results may differ from the reference program's by a relative error of at most 0.00420516.
Values are sent between devices in bfloat16 or wider.
A program may use at most 1 GiB of HBM per device.

```python
import math
import jax
import jax.numpy as jnp
from jax import lax

NUM_SEQS = 512
PREFIX_LEN = 4096
SUFFIX_LEN = 64
MODEL_DIM = 4096
NUM_HEADS = 32
KV_HEADS = 32
HEAD_DIM = 128
GROUP_SIZE = NUM_HEADS // KV_HEADS


def setup_inputs(seed: int = 0, part: int = 0) -> dict:
    root_key = jax.random.key(seed)
    part_key = jax.random.fold_in(root_key, part)
    weight_keys = jax.random.split(root_key, 4)
    draw_keys = jax.random.split(part_key, 10)
    topic_count = 16
    log_ratio = min(max(math.log(2.0 * PREFIX_LEN / (topic_count * SUFFIX_LEN)), -3.0), 3.0)
    amp_prefix = 2.0 + max(-log_ratio, 0.0)
    amp_suffix = 3.0 + max(log_ratio, 0.0)
    q_cols = NUM_HEADS * HEAD_DIM
    kv_cols = KV_HEADS * HEAD_DIM
    in_scale = MODEL_DIM ** -0.5
    w_q = jax.random.normal(weight_keys[0], (MODEL_DIM, q_cols), jnp.float32) * in_scale
    lead_cols = w_q.reshape(MODEL_DIM, KV_HEADS, GROUP_SIZE, HEAD_DIM)[:, :, 0, :].reshape(MODEL_DIM, kv_cols)
    w_k = 0.6 * lead_cols + 0.8 * in_scale * jax.random.normal(weight_keys[1], (MODEL_DIM, kv_cols), jnp.float32)
    w_v = in_scale * jax.random.normal(weight_keys[2], (MODEL_DIM, kv_cols), jnp.float32)
    w_o = jax.random.normal(weight_keys[3], (q_cols, MODEL_DIM), jnp.float32) * q_cols ** -0.5
    hidden = jax.random.normal(draw_keys[0], (NUM_SEQS, MODEL_DIM), jnp.float32)
    topic_hid = jax.random.normal(draw_keys[1], (topic_count, MODEL_DIM), jnp.float32)
    topic_key = jnp.dot(topic_hid, w_k).reshape(topic_count, KV_HEADS, HEAD_DIM)
    topic_val = jnp.dot(topic_hid, w_v).reshape(topic_count, KV_HEADS, HEAD_DIM)
    pos_topic = jnp.arange(PREFIX_LEN) * topic_count // PREFIX_LEN
    kv_shape = (PREFIX_LEN, KV_HEADS, HEAD_DIM)
    k_prefix = amp_prefix * topic_key[pos_topic] + jax.random.normal(draw_keys[2], kv_shape, jnp.float32)
    v_prefix = topic_val[pos_topic] + 0.5 * jax.random.normal(draw_keys[3], kv_shape, jnp.float32)
    own_hid = jax.random.normal(draw_keys[4], (NUM_SEQS, MODEL_DIM), jnp.float32)
    stale_hid = jax.random.normal(draw_keys[5], (NUM_SEQS, MODEL_DIM), jnp.float32)
    head_shape = (NUM_SEQS, 1, KV_HEADS, HEAD_DIM)
    own_key = jnp.dot(own_hid, w_k).reshape(head_shape)
    own_val = jnp.dot(own_hid, w_v).reshape(head_shape)
    stale_key = jnp.dot(stale_hid, w_k).reshape(head_shape)
    stale_val = jnp.dot(stale_hid, w_v).reshape(head_shape)
    seq_lens = jax.random.randint(draw_keys[6], (NUM_SEQS,), 0, SUFFIX_LEN)
    seq_lens = seq_lens.at[0].set(SUFFIX_LEN - 1).at[NUM_SEQS - 1].set(0)
    in_use = (jnp.arange(SUFFIX_LEN)[None, :] < seq_lens[:, None])[:, :, None, None]
    suf_shape = (NUM_SEQS, SUFFIX_LEN, KV_HEADS, HEAD_DIM)
    k_suffix = amp_suffix * jnp.where(in_use, own_key, stale_key) + jax.random.normal(draw_keys[7], suf_shape, jnp.float32)
    v_suffix = jnp.where(in_use, own_val, stale_val) + 0.5 * jax.random.normal(draw_keys[8], suf_shape, jnp.float32)
    return dict(hidden=hidden.astype(jnp.bfloat16), w_q=w_q.astype(jnp.bfloat16), w_k=w_k.astype(jnp.bfloat16), w_v=w_v.astype(jnp.bfloat16), w_o=w_o.astype(jnp.bfloat16), k_prefix=k_prefix.astype(jnp.bfloat16), v_prefix=v_prefix.astype(jnp.bfloat16), k_suffix=k_suffix.astype(jnp.bfloat16), v_suffix=v_suffix.astype(jnp.bfloat16), seq_lens=seq_lens)


def reference(hidden, w_q, w_k, w_v, w_o, k_prefix, v_prefix, k_suffix, v_suffix, seq_lens):
    q_all = jnp.dot(hidden, w_q, preferred_element_type=jnp.float32).astype(jnp.bfloat16)
    k_new = jnp.dot(hidden, w_k, preferred_element_type=jnp.float32).astype(jnp.bfloat16)
    v_new = jnp.dot(hidden, w_v, preferred_element_type=jnp.float32).astype(jnp.bfloat16)
    slot_ids = jnp.arange(SUFFIX_LEN)
    at_new = (slot_ids[None, :] == seq_lens[:, None])[:, :, None, None]
    k_cur = jnp.where(at_new, k_new.reshape(NUM_SEQS, 1, KV_HEADS, HEAD_DIM), k_suffix).astype(jnp.float32)
    v_cur = jnp.where(at_new, v_new.reshape(NUM_SEQS, 1, KV_HEADS, HEAD_DIM), v_suffix).astype(jnp.float32)
    visible = slot_ids[None, :] <= seq_lens[:, None]
    q_grp = q_all.astype(jnp.float32).reshape(NUM_SEQS, KV_HEADS, GROUP_SIZE, HEAD_DIM)
    k_pre32 = k_prefix.astype(jnp.float32)
    v_pre32 = v_prefix.astype(jnp.float32)
    score_scale = HEAD_DIM ** -0.5

    def one_sequence(seq_items):
        q_one, k_one, v_one, vis_one = seq_items
        s_pre = jnp.einsum('kgd,pkd->kgp', q_one, k_pre32) * score_scale
        s_suf = jnp.einsum('kgd,skd->kgs', q_one, k_one) * score_scale
        s_suf = jnp.where(vis_one[None, None, :], s_suf, -jnp.inf)
        run_max = jnp.maximum(jnp.max(s_pre, axis=-1), jnp.max(s_suf, axis=-1))[..., None]
        e_pre = jnp.exp(s_pre - run_max)
        e_suf = jnp.exp(s_suf - run_max)
        weight_sum = jnp.sum(e_pre, axis=-1) + jnp.sum(e_suf, axis=-1)
        weighted = jnp.einsum('kgp,pkd->kgd', e_pre, v_pre32) + jnp.einsum('kgs,skd->kgd', e_suf, v_one)
        return weighted / weight_sum[..., None]

    attn_out = lax.map(one_sequence, (q_grp, k_cur, v_cur, visible))
    attn_out = attn_out.reshape(NUM_SEQS, NUM_HEADS * HEAD_DIM).astype(jnp.bfloat16)
    out_hidden = hidden.astype(jnp.float32) + jnp.dot(attn_out, w_o, preferred_element_type=jnp.float32)
    return out_hidden.astype(jnp.bfloat16)
```

```python
import functools

import jax
import jax.numpy as jnp
from jax import lax
from jax.experimental import pallas as pl
from jax.experimental.pallas import tpu as pltpu
from jax.sharding import PartitionSpec as P

F32 = jnp.float32
BF16 = jnp.bfloat16
VM = pltpu.VMEM
LOG2E = 1.4426950408889634
BATCH = 8
SLOTS = 16
RING = 8
LIMIT = 56 * 2**20


def _cost(flops, nbytes):
    return pl.CostEstimate(flops=int(flops), bytes_accessed=int(nbytes), transcendentals=0)


def _dot(a, b, dims=(((1,), (0,)), ((), ()))):
    return lax.dot_general(a, b, dims, preferred_element_type=F32)


NT = (((1,), (1,)), ((), ()))


def _proj_kernel(x_ref, *refs):
    half = len(refs) // 2
    for w_ref, o_ref in zip(refs[:half], refs[half:]):
        y = _dot(x_ref[...], w_ref[...]).astype(BF16)
        for h in range(o_ref.shape[0]):
            o_ref[h] = y[:, h * 128:(h + 1) * 128]


def _project(x, ws, tile):
    rows, depth = x.shape
    cols = ws[0].shape[1]
    heads = cols // 128
    th = tile // 128
    n = len(ws)
    return pl.pallas_call(
        _proj_kernel,
        grid=(cols // tile,),
        in_specs=[pl.BlockSpec((rows, depth), lambda i: (0, 0))]
        + [pl.BlockSpec((depth, tile), lambda i: (0, i))] * n,
        out_specs=[pl.BlockSpec((th, rows, 128), lambda i: (i, 0, 0))] * n,
        out_shape=[jax.ShapeDtypeStruct((heads, rows, 128), BF16)] * n,
        compiler_params=pltpu.CompilerParams(vmem_limit_bytes=LIMIT),
        cost_estimate=_cost(2 * rows * depth * cols * n, 2 * depth * cols * n),
    )(x, *ws)


def _relayout_kernel(k_ref, v_ref, ko_ref, vo_ref):
    def body(i, c):
        at = pl.multiple_of(i * 16, 16)
        ko_ref[:, pl.ds(at, 16), :] = jnp.swapaxes(k_ref[pl.ds(i * 16, 16)], 0, 1)
        vo_ref[:, pl.ds(at, 16), :] = jnp.swapaxes(v_ref[pl.ds(i * 16, 16)], 0, 1)
        return c
    lax.fori_loop(0, k_ref.shape[0] // 16, body, 0, unroll=2)


def _relayout(k, v):
    n, heads, d = k.shape
    t = 128
    return pl.pallas_call(
        _relayout_kernel,
        grid=(n // t,),
        in_specs=[pl.BlockSpec((t, heads, d), lambda i: (i, 0, 0))] * 2,
        out_specs=[pl.BlockSpec((heads, t, d), lambda i: (0, i, 0))] * 2,
        out_shape=[jax.ShapeDtypeStruct((heads, n, d), BF16)] * 2,
        compiler_params=pltpu.CompilerParams(vmem_limit_bytes=LIMIT),
        cost_estimate=_cost(2e9, 8 * n * heads * d),
    )(k, v)


def _prefix_kernel(scale, q0_ref, q1_ref, k_ref, v_ref, o0_ref, o1_ref, l0_ref, l1_ref):
    h = pl.program_id(0)
    lane = lax.broadcasted_iota(jnp.int32, (128, 128), 1)

    @pl.when(h == 0)
    def _():
        l0_ref[...] = jnp.zeros_like(l0_ref)
        l1_ref[...] = jnp.zeros_like(l1_ref)

    k = k_ref[0]
    v = v_ref[0]
    for q_ref, o_ref, l_ref in ((q0_ref, o0_ref, l0_ref), (q1_ref, o1_ref, l1_ref)):
        s = _dot(q_ref[0], k, NT)
        m = jnp.max(s, axis=1, keepdims=True) * scale
        e = jnp.exp2(s * scale - m)
        l = jnp.sum(e, axis=1, keepdims=True)
        o = _dot(e.astype(BF16), v)
        o_ref[0] = o / l
        l_ref[...] = jnp.where(lane == h, m + jnp.log2(l), l_ref[...])


def _prefix(q0, q1, k, v, scale):
    heads, rows, d = q0.shape
    n = k.shape[1]
    head = lambda i: (i, 0, 0)
    return pl.pallas_call(
        functools.partial(_prefix_kernel, scale),
        grid=(heads,),
        in_specs=[pl.BlockSpec((1, rows, d), head)] * 2 + [pl.BlockSpec((1, n, d), head)] * 2,
        out_specs=[pl.BlockSpec((1, rows, d), head)] * 2 + [pl.BlockSpec((rows, 128), lambda i: (0, 0))] * 2,
        out_shape=[jax.ShapeDtypeStruct((heads, rows, d), F32)] * 2
        + [jax.ShapeDtypeStruct((rows, 128), F32)] * 2,
        compiler_params=pltpu.CompilerParams(vmem_limit_bytes=LIMIT),
        cost_estimate=_cost(8 * heads * rows * n * d, 4 * heads * n * d),
    )(q0, q1, k, v)


def _merge_kernel(o0_ref, l0_ref, o1_ref, l1_ref, o_ref, l_ref):
    l0, l1 = l0_ref[...], l1_ref[...]
    m = jnp.maximum(l0, l1)
    w0, w1 = jnp.exp2(l0 - m), jnp.exp2(l1 - m)
    t = w0 + w1
    l_ref[...] = m + jnp.log2(t)
    w0, w1 = w0 / t, w1 / t
    for h in range(o0_ref.shape[0]):
        o_ref[h] = (w0[:, h:h + 1] * o0_ref[h] + w1[:, h:h + 1] * o1_ref[h]).astype(BF16)


def _merge(o0, l0, o1, l1):
    return pl.pallas_call(
        _merge_kernel,
        in_specs=[pl.BlockSpec(memory_space=VM)] * 4,
        out_specs=[pl.BlockSpec(memory_space=VM)] * 2,
        out_shape=[jax.ShapeDtypeStruct(o0.shape, BF16), jax.ShapeDtypeStruct(l0.shape, F32)],
        compiler_params=pltpu.CompilerParams(vmem_limit_bytes=LIMIT),
        cost_estimate=_cost(1e9, 10 * o0.size),
    )(o0, l0, o1, l1)


def _suffix_kernel(scale, lens, q_ref, kn_ref, vn_ref, k_hbm, v_hbm, o_ref, lse_ref,
                   items, qb, acc, m_s, l_s, kbuf, vbuf, sbuf, ksem, vsem):
    heads, rows, d = q_ref.shape
    per = k_hbm.shape[0] // rows
    wide = SLOTS * heads
    dummy = rows * per

    for g in range(BATCH):
        items[g] = dummy

    def listing(b, t):
        for j in range(per):
            items[BATCH + t + j] = b * per + j
        return t + (lens[b] + SLOTS - 1) // SLOTS
    total = lax.fori_loop(0, rows, listing, 0)
    for g in range(2 * BATCH):
        items[BATCH + total + g] = dummy
    batches = (total + BATCH - 1) // BATCH

    def fetch(i):
        slot = lax.rem(i, RING)
        for g in range(BATCH):
            it = jnp.minimum(items[BATCH + i * BATCH + g], dummy - 1)
            pltpu.make_async_copy(k_hbm.at[it], kbuf.at[slot, g], ksem.at[slot]).start()
            pltpu.make_async_copy(v_hbm.at[it], vbuf.at[slot, g], vsem.at[slot]).start()

    def prime(i, c):
        fetch(i)
        return c
    lax.fori_loop(0, jnp.minimum(batches, RING - 1), prime, 0)

    for c in range(rows // 16):
        q = jnp.swapaxes(q_ref[:, c * 16:c * 16 + 16, :], 0, 1)
        kn = jnp.swapaxes(kn_ref[:, c * 16:c * 16 + 16, :], 0, 1)
        vn = jnp.swapaxes(vn_ref[:, c * 16:c * 16 + 16, :], 0, 1)
        qb[c * 16:c * 16 + 16] = q
        s = jnp.sum(q.astype(F32) * kn.astype(F32), axis=-1, keepdims=True) * scale
        m_s[c * 16:c * 16 + 16] = jnp.broadcast_to(s, (16, heads, 128))
        l_s[c * 16:c * 16 + 16] = jnp.ones((16, heads, 128), F32)
        acc[c * 16:c * 16 + 16] = vn.astype(F32)

    row = lax.broadcasted_iota(jnp.int32, (heads, wide), 0)
    col = lax.broadcasted_iota(jnp.int32, (heads, wide), 1)
    slot_of = jnp.where(lax.rem(col, heads) == row, col // heads, 1 << 20)

    def step(i, c):
        slot = lax.rem(i, RING)
        last = lax.rem(i + RING - 1, RING)
        par = lax.rem(i, 2)

        @pl.when(i < batches)
        def _():
            pltpu.make_async_copy(k_hbm.at[pl.ds(0, BATCH)], kbuf.at[slot], ksem.at[slot]).wait()

        @pl.when(i > 0)
        def _():
            pltpu.make_async_copy(v_hbm.at[pl.ds(0, BATCH)], vbuf.at[last], vsem.at[last]).wait()

        for g in range(BATCH):
            it = items[BATCH + i * BATCH + g]
            b = it // per
            left = lens[jnp.minimum(b, rows - 1)] - lax.rem(it, per) * SLOTS
            s = _dot(qb[b], kbuf[slot, g], NT) * scale
            sbuf[par, g] = jnp.where(slot_of < left, s, -jnp.inf)

        parts = []
        for g in range(0, BATCH, 2):
            ps = []
            for u in range(2):
                s = sbuf[1 - par, g + u]
                m = jnp.max(s, axis=1, keepdims=True)
                p = jnp.exp2(s - m)
                parts.append([m, jnp.sum(p, axis=1, keepdims=True), None])
                ps.append(p.astype(BF16))
            o = _dot(jnp.concatenate(ps, axis=0),
                     jnp.concatenate([vbuf[last, g], vbuf[last, g + 1]], axis=1))
            parts[g][2] = o[:heads, :d]
            parts[g + 1][2] = o[heads:, d:]
        for g in range(BATCH):
            b = items[i * BATCH + g] // per
            m, l, o = parts[g]
            m_old = m_s[b]
            m_new = jnp.maximum(m_old, m)
            w_old = jnp.exp2(m_old - m_new)
            w = jnp.exp2(m - m_new)
            m_s[b] = m_new
            l_s[b] = l_s[b] * w_old + l * w
            acc[b] = acc[b] * w_old + o * w

        @pl.when(i + RING - 1 < batches)
        def _():
            fetch(i + RING - 1)
        return c

    lax.fori_loop(0, batches + 1, step, 0)

    lane = lax.broadcasted_iota(jnp.int32, (16, 128), 1)
    for c in range(rows // 16):
        l = l_s[c * 16:c * 16 + 16]
        o = acc[c * 16:c * 16 + 16] / l
        lse = m_s[c * 16:c * 16 + 16] + jnp.log2(l)
        o_ref[:, c * 16:c * 16 + 16, :] = jnp.swapaxes(o, 0, 1)
        lse = jnp.swapaxes(lse, 0, 1)
        out = jnp.zeros((16, 128), F32)
        for h in range(heads):
            out = jnp.where(lane == h, lse[h], out)
        lse_ref[c * 16:c * 16 + 16, :] = out


def _suffix(lens, q, kn, vn, k, v, scale):
    heads, rows, d = q.shape
    slots = k.shape[1]
    per = slots // SLOTS
    wide = SLOTS * heads
    k = k.reshape(rows * per, wide, d)
    v = v.reshape(rows * per, wide, d)
    return pl.pallas_call(
        functools.partial(_suffix_kernel, scale),
        in_specs=[pl.BlockSpec(memory_space=pltpu.SMEM)] + [pl.BlockSpec(memory_space=VM)] * 3
        + [pl.BlockSpec(memory_space=pl.ANY)] * 2,
        out_specs=[pl.BlockSpec(memory_space=VM)] * 2,
        out_shape=[jax.ShapeDtypeStruct((heads, rows, d), F32), jax.ShapeDtypeStruct((rows, 128), F32)],
        scratch_shapes=[
            pltpu.SMEM((rows * per + 4 * BATCH,), jnp.int32),
            VM((rows + 1, heads, d), BF16),
            VM((rows + 1, heads, d), F32),
            VM((rows + 1, heads, 128), F32),
            VM((rows + 1, heads, 128), F32),
            VM((RING, BATCH, wide, d), BF16),
            VM((RING, BATCH, wide, d), BF16),
            VM((2, BATCH, heads, wide), F32),
            pltpu.SemaphoreType.DMA((RING,)),
            pltpu.SemaphoreType.DMA((RING,)),
        ],
        compiler_params=pltpu.CompilerParams(vmem_limit_bytes=LIMIT),
        cost_estimate=_cost(2e10, 4 * k.size),
    )(lens, q, kn, vn, k, v)


def _merge4_kernel(*refs):
    o_refs, l_refs, att_ref = refs[0:8:2], refs[1:8:2], refs[8]
    ls = [r[...] for r in l_refs]
    m = functools.reduce(jnp.maximum, ls)
    ws = [jnp.exp2(l - m) for l in ls]
    t = functools.reduce(jnp.add, ws)
    ws = [w / t for w in ws]
    for h in range(o_refs[0].shape[0]):
        a = ws[0][:, h:h + 1] * o_refs[0][h].astype(F32)
        for w, r in zip(ws[1:], o_refs[1:]):
            a += w[:, h:h + 1] * r[h].astype(F32)
        att_ref[:, h * 128:(h + 1) * 128] = a.astype(BF16)


def _merge4(parts):
    heads, rows, d = parts[0][0].shape
    flat = [a for p in parts for a in p]
    return pl.pallas_call(
        _merge4_kernel,
        in_specs=[pl.BlockSpec(memory_space=VM)] * 8,
        out_specs=pl.BlockSpec(memory_space=VM),
        out_shape=jax.ShapeDtypeStruct((rows, heads * d), BF16),
        compiler_params=pltpu.CompilerParams(vmem_limit_bytes=LIMIT),
        cost_estimate=_cost(1e9, 20 * heads * rows * d),
    )(*flat)


def _send_kernel(at, a_ref, w_ref, o_ref):
    o_ref[...] = _dot(a_ref[...], w_ref[...]).astype(BF16)


def _keep_kernel(at, a_ref, w_ref, x_ref, o_ref):
    o_ref[...] = _dot(a_ref[...], w_ref[...]) + x_ref[...].astype(F32)


def _out_proj(att, w_o, x, first, cols, tile):
    rows, depth = att.shape
    in_specs = [pl.BlockSpec((rows, depth), lambda i, at: (0, 0)),
                pl.BlockSpec((depth, tile), lambda i, at: (0, at[0] + i))]
    args = [att, w_o]
    if x is not None:
        in_specs.append(pl.BlockSpec((rows, tile), lambda i, at: (0, at[0] + i)))
        args.append(x)
    return pl.pallas_call(
        _send_kernel if x is None else _keep_kernel,
        grid_spec=pltpu.PrefetchScalarGridSpec(
            num_scalar_prefetch=1, grid=(cols // tile,), in_specs=in_specs,
            out_specs=pl.BlockSpec((rows, tile), lambda i, at: (0, i))),
        out_shape=jax.ShapeDtypeStruct((rows, cols), BF16 if x is None else F32),
        compiler_params=pltpu.CompilerParams(vmem_limit_bytes=LIMIT),
        cost_estimate=_cost(2 * rows * depth * cols, 2 * depth * cols),
    )(first, *args)


def solution(mesh):
    n_ctx = mesh.shape['ctx']
    row_axes = ('dp', 'ctx')
    chip_swap = [(i, i ^ 2) for i in range(n_ctx)]
    core_swap = [(i, i ^ 1) for i in range(n_ctx)]
    tp_swap = [(0, 1), (1, 0)]

    def device_step(hidden, w_q, w_k, w_v, w_o, k_prefix, v_prefix, k_suffix, v_suffix, seq_lens):
        scale = LOG2E * k_prefix.shape[2] ** -0.5
        far = lambda a: lax.ppermute(a, 'ctx', chip_swap)
        near = lambda a: lax.ppermute(a, 'ctx', core_swap)
        (q,) = _project(hidden, [w_q], 512)
        q_far = far(q)
        q_near = near(q)
        kn, vn = _project(hidden, [w_k, w_v], 256)
        kt, vt = _relayout(k_prefix, v_prefix)
        q_diag = near(q_far)
        o_diag, o_far, l_diag, l_far = _prefix(q_diag, q_far, kt, vt, scale)
        o_x, l_x = _merge(o_far, l_far, near(o_diag), near(l_diag))
        o_x, l_x = far(o_x), far(l_x)
        o_near, o_own, l_near, l_own = _prefix(q_near, q, kt, vt, scale)
        o_near, l_near = near(o_near), near(l_near)
        o_suf, l_suf = _suffix(seq_lens, q, kn, vn, k_suffix, v_suffix, scale)
        att = _merge4([(o_own, l_own), (o_near, l_near), (o_x, l_x), (o_suf, l_suf)])

        me = lax.axis_index('tp')
        half = w_o.shape[1] // 2
        parts = 2
        cols = half // parts
        tile = 512
        sent = [lax.ppermute(_out_proj(att, w_o, None, ((1 - me) * half + p * cols)[None] // tile, cols, tile), 'tp', tp_swap)
                for p in range(parts)]
        kept = [_out_proj(att, w_o, hidden, (me * half + p * cols)[None] // tile, cols, tile) for p in range(parts)]
        mine = [(a + b.astype(F32)).astype(BF16) for a, b in zip(kept, sent)]
        other = [lax.ppermute(a, 'tp', tp_swap) for a in mine]
        mine, other = jnp.concatenate(mine, axis=1), jnp.concatenate(other, axis=1)
        return jnp.where(me == 0, jnp.concatenate([mine, other], axis=1), jnp.concatenate([other, mine], axis=1))

    spec_in = (P(row_axes, None), P(None, 'tp'), P(None, 'tp'), P(None, 'tp'), P('tp', None),
               P(row_axes, 'tp', None), P(row_axes, 'tp', None), P(row_axes, None, 'tp', None),
               P(row_axes, None, 'tp', None), P(row_axes))
    return jax.shard_map(device_step, mesh=mesh, in_specs=spec_in, out_specs=P(row_axes, None), check_vma=False)
```

```python
import functools

import jax
import jax.numpy as jnp
from jax import lax
from jax.experimental import pallas as pl
from jax.experimental.pallas import tpu as pltpu
from jax.sharding import PartitionSpec as P

F32 = jnp.float32
BF16 = jnp.bfloat16
VM = pltpu.VMEM
LOG2E = 1.4426950408889634
BATCH = 16
SLOTS = 16
RING = 5
CHUNK = 256
RINGW = 10
LIMIT = 56 * 2**20


def _cost(flops, nbytes):
    return pl.CostEstimate(flops=int(flops), bytes_accessed=int(nbytes), transcendentals=0)


def _dot(a, b, dims=(((1,), (0,)), ((), ()))):
    return lax.dot_general(a, b, dims, preferred_element_type=F32)


NT = (((1,), (1,)), ((), ()))


def _stream(x_ref, ws, bufs, sem, acc, chunk, emit, extra_start=None, extra_body=None):
    depth = ws[0].shape[0]
    n = depth // chunk
    total = n * len(ws)

    def start(g):
        for i, w in enumerate(ws):
            @pl.when((g >= i * n) & (g < (i + 1) * n))
            def _():
                at = pl.multiple_of((g - i * n) * chunk, chunk)
                pltpu.make_async_copy(w.at[pl.ds(at, chunk)], bufs.at[lax.rem(g, RINGW)],
                                      sem.at[lax.rem(g, RINGW)]).start()
        if extra_start is not None:
            @pl.when(g < total)
            def _():
                extra_start(g)

    def run():
        for i, w in enumerate(ws):
            def body(c, carry):
                g = i * n + c
                slot = lax.rem(g, RINGW)
                pltpu.make_async_copy(w.at[pl.ds(0, chunk)], bufs.at[slot], sem.at[slot]).wait()
                at = pl.multiple_of(c * chunk, chunk)
                y = _dot(x_ref[:, pl.ds(at, chunk)], bufs[slot])

                @pl.when(c == 0)
                def _():
                    acc[...] = y

                @pl.when(c > 0)
                def _():
                    acc[...] += y
                if extra_body is not None:
                    extra_body(g)
                start(g + RINGW)
                return carry
            lax.fori_loop(0, n, body, 0)
            emit(i)
    return start, run


def _prime(start, count):
    def body(g, c):
        start(g)
        return c
    lax.fori_loop(0, count, body, 0)


def _heads_out(acc, o_ref):
    for h in range(o_ref.shape[0]):
        o_ref[h] = acc[:, h * 128:(h + 1) * 128].astype(BF16)


def _q_kernel(x_hbm, w_hbm, o_ref, x_ref, bufs, acc, xsem, sem):
    cp = pltpu.make_async_copy(x_hbm, x_ref, xsem)
    cp.start()
    start, run = _stream(x_ref, [w_hbm], bufs, sem, acc, bufs.shape[1], lambda i: _heads_out(acc, o_ref))
    _prime(start, RINGW)
    cp.wait()
    run()


def _project_q(x, w):
    rows, depth = x.shape
    cols = w.shape[1]
    return pl.pallas_call(
        _q_kernel,
        in_specs=[pl.BlockSpec(memory_space=pl.ANY)] * 2,
        out_specs=pl.BlockSpec(memory_space=VM),
        out_shape=jax.ShapeDtypeStruct((cols // 128, rows, 128), BF16),
        scratch_shapes=[VM((rows, depth), BF16), VM((RINGW, CHUNK, cols), BF16), VM((rows, cols), F32),
                        pltpu.SemaphoreType.DMA, pltpu.SemaphoreType.DMA((RINGW,))],
        compiler_params=pltpu.CompilerParams(vmem_limit_bytes=LIMIT),
        cost_estimate=_cost(2 * rows * depth * cols, 2 * depth * cols),
    )(x, w)


def _kv_kernel(x_hbm, wk_hbm, wv_hbm, kp_hbm, vp_hbm, kn_ref, vn_ref, kt_hbm, vt_hbm,
               x_ref, bufs, acc, raw, out, xsem, sem, psem, osem):
    cp = pltpu.make_async_copy(x_hbm, x_ref, xsem)
    cp.start()
    chunk = bufs.shape[1]
    total = 2 * x_hbm.shape[1] // chunk
    pos = kp_hbm.shape[0] // total
    stage = total // 4

    def pieces(g):
        at = pl.ds(g * pos, pos)
        return [pltpu.make_async_copy(src.at[at], raw.at[j, at], psem.at[lax.rem(g, RINGW)])
                for j, src in enumerate((kp_hbm, vp_hbm))]

    def stores(s):
        at = pl.ds(pl.multiple_of(s * stage * pos, stage * pos), stage * pos)
        return [pltpu.make_async_copy(out.at[j, :, at], dst.at[:, at], osem)
                for j, dst in enumerate((kt_hbm, vt_hbm))]

    def extra_start(g):
        for c in pieces(g):
            c.start()

    def extra_body(g):
        for c in pieces(g):
            c.wait()
        for j in range(2):
            for u in range(pos // 16):
                at = pl.multiple_of(g * pos + u * 16, 16)
                out[j, :, pl.ds(at, 16), :] = jnp.swapaxes(raw[j, pl.ds(g * pos + u * 16, 16)], 0, 1)

        @pl.when(lax.rem(g + 1, stage) == 0)
        def _():
            for c in stores(g // stage):
                c.start()

    start, run = _stream(x_ref, [wk_hbm, wv_hbm], bufs, sem, acc, chunk,
                         lambda i: _heads_out(acc, (kn_ref, vn_ref)[i]), extra_start, extra_body)
    _prime(start, RINGW)
    cp.wait()
    run()
    for s in range(4):
        for c in stores(s):
            c.wait()


def _project_kv(x, wk, wv, kp, vp):
    rows, depth = x.shape
    cols = wk.shape[1]
    n, heads, d = kp.shape
    return pl.pallas_call(
        _kv_kernel,
        in_specs=[pl.BlockSpec(memory_space=pl.ANY)] * 5,
        out_specs=[pl.BlockSpec(memory_space=VM)] * 2 + [pl.BlockSpec(memory_space=pl.ANY)] * 2,
        out_shape=[jax.ShapeDtypeStruct((cols // 128, rows, 128), BF16)] * 2
        + [jax.ShapeDtypeStruct((heads, n, d), BF16)] * 2,
        scratch_shapes=[VM((rows, depth), BF16), VM((RINGW, CHUNK, cols), BF16), VM((rows, cols), F32),
                        VM((2, n, heads, d), BF16), VM((2, heads, n, d), BF16),
                        pltpu.SemaphoreType.DMA, pltpu.SemaphoreType.DMA((RINGW,)),
                        pltpu.SemaphoreType.DMA((RINGW,)), pltpu.SemaphoreType.DMA],
        compiler_params=pltpu.CompilerParams(vmem_limit_bytes=LIMIT),
        cost_estimate=_cost(2e10, 4 * depth * cols),
    )(x, wk, wv, kp, vp)


def _prefix_kernel(scale, q0_ref, q1_ref, k_ref, v_ref, o0_ref, o1_ref):
    group = k_ref.shape[0]
    heads = o0_ref.shape[0] - 1
    i = pl.program_id(0)
    rows = q0_ref.shape[1]
    lane = lax.broadcasted_iota(jnp.int32, (rows, 128), 1)

    @pl.when(i == 0)
    def _():
        o0_ref[heads] = jnp.zeros_like(o0_ref[heads])
        o1_ref[heads] = jnp.zeros_like(o1_ref[heads])

    units = [(u, q, o) for u in range(group) for q, o in ((q0_ref, o0_ref), (q1_ref, o1_ref))]
    lses = {id(o0_ref): [], id(o1_ref): []}
    for u, q_ref, o_ref in units:
        s = _dot(q_ref[u], k_ref[u], NT)
        m = jnp.max(s, axis=1, keepdims=True) * scale
        e = jnp.exp2(s * scale - m)
        l = jnp.sum(e, axis=1, keepdims=True)
        o = _dot(e.astype(BF16), v_ref[u])
        o_ref[i * group + u] = o / l
        lses[id(o_ref)].append(m + jnp.log2(l))
    for o_ref in (o0_ref, o1_ref):
        x = o_ref[heads]
        for u, lse in enumerate(lses[id(o_ref)]):
            x = jnp.where(lane == i * group + u, lse, x)
        o_ref[heads] = x


def _prefix(q0, q1, k, v, scale):
    heads, rows, d = q0.shape
    n = k.shape[1]
    group = 2
    head = lambda i: (i, 0, 0)
    return pl.pallas_call(
        functools.partial(_prefix_kernel, scale),
        grid=(heads // group,),
        in_specs=[pl.BlockSpec((group, rows, d), head)] * 2 + [pl.BlockSpec((group, n, d), head)] * 2,
        out_specs=[pl.BlockSpec((heads + 1, rows, d), lambda i: (0, 0, 0))] * 2,
        out_shape=[jax.ShapeDtypeStruct((heads + 1, rows, d), F32)] * 2,
        compiler_params=pltpu.CompilerParams(vmem_limit_bytes=LIMIT),
        cost_estimate=_cost(8 * heads * rows * n * d, 4 * heads * n * d),
    )(q0, q1, k, v)


def _merge_kernel(a_ref, b_ref, o_ref):
    heads = a_ref.shape[0] - 1
    l0, l1 = a_ref[heads], b_ref[heads]
    m = jnp.maximum(l0, l1)
    w0, w1 = jnp.exp2(l0 - m), jnp.exp2(l1 - m)
    t = w0 + w1
    w0, w1 = w0 / t, w1 / t
    for h in range(heads):
        o_ref[h] = (w0[:, h:h + 1] * a_ref[h] + w1[:, h:h + 1] * b_ref[h]).astype(BF16)
    lse = m + jnp.log2(t)
    for j in range(3):
        term = lse.astype(BF16)
        o_ref[heads + j] = term
        lse = lse - term.astype(F32)


def _merge(a, b):
    heads = a.shape[0] - 1
    return pl.pallas_call(
        _merge_kernel,
        in_specs=[pl.BlockSpec(memory_space=VM)] * 2,
        out_specs=pl.BlockSpec(memory_space=VM),
        out_shape=jax.ShapeDtypeStruct((heads + 3,) + a.shape[1:], BF16),
        compiler_params=pltpu.CompilerParams(vmem_limit_bytes=LIMIT),
        cost_estimate=_cost(1e9, 10 * a.size),
    )(a, b)


def _suffix_kernel(scale, lens, q_ref, kn_ref, vn_ref, k_hbm, v_hbm, o_ref,
                   items, qb, acc, m_s, l_s, kbuf, vbuf, sbuf, ksem, vsem):
    heads, rows, d = q_ref.shape
    per = k_hbm.shape[0] // rows
    wide = SLOTS * heads
    dummy = rows * per

    for g in range(BATCH):
        items[g] = dummy

    def listing(b, t):
        for j in range(per):
            items[BATCH + t + j] = b * per + j
        return t + (lens[b] + SLOTS - 1) // SLOTS
    total = lax.fori_loop(0, rows, listing, 0)
    for g in range(2 * BATCH):
        items[BATCH + total + g] = dummy
    batches = (total + BATCH - 1) // BATCH

    def fetch(i):
        slot = lax.rem(i, RING)
        for g in range(BATCH):
            it = jnp.minimum(items[BATCH + i * BATCH + g], dummy - 1)
            pltpu.make_async_copy(k_hbm.at[it], kbuf.at[slot, g], ksem.at[slot]).start()
            pltpu.make_async_copy(v_hbm.at[it], vbuf.at[slot, g], vsem.at[slot]).start()

    def prime(i, c):
        fetch(i)
        return c
    lax.fori_loop(0, jnp.minimum(batches, RING - 1), prime, 0)

    for c in range(rows // 16):
        q = jnp.swapaxes(q_ref[:, c * 16:c * 16 + 16, :], 0, 1)
        kn = jnp.swapaxes(kn_ref[:, c * 16:c * 16 + 16, :], 0, 1)
        vn = jnp.swapaxes(vn_ref[:, c * 16:c * 16 + 16, :], 0, 1)
        qb[c * 16:c * 16 + 16] = q
        s = jnp.sum(q.astype(F32) * kn.astype(F32), axis=-1, keepdims=True) * scale
        m_s[c * 16:c * 16 + 16] = jnp.broadcast_to(s, (16, heads, 128))
        l_s[c * 16:c * 16 + 16] = jnp.ones((16, heads, 128), F32)
        acc[c * 16:c * 16 + 16] = vn.astype(F32)

    row = lax.broadcasted_iota(jnp.int32, (heads, wide), 0)
    col = lax.broadcasted_iota(jnp.int32, (heads, wide), 1)
    slot_of = jnp.where(lax.rem(col, heads) == row, col // heads, 1 << 20)

    def step(i, c):
        slot = lax.rem(i, RING)
        last = lax.rem(i + RING - 1, RING)
        par = lax.rem(i, 2)

        @pl.when(i < batches)
        def _():
            pltpu.make_async_copy(k_hbm.at[pl.ds(0, BATCH)], kbuf.at[slot], ksem.at[slot]).wait()

        @pl.when(i > 0)
        def _():
            pltpu.make_async_copy(v_hbm.at[pl.ds(0, BATCH)], vbuf.at[last], vsem.at[last]).wait()

        for g in range(BATCH):
            it = items[BATCH + i * BATCH + g]
            b = it // per
            left = lens[jnp.minimum(b, rows - 1)] - lax.rem(it, per) * SLOTS
            s = _dot(qb[b], kbuf[slot, g], NT) * scale
            sbuf[par, g] = jnp.where(slot_of < left, s, -jnp.inf)

        parts = []
        for g in range(0, BATCH, 2):
            ps = []
            for u in range(2):
                s = sbuf[1 - par, g + u]
                m = jnp.max(s, axis=1, keepdims=True)
                p = jnp.exp2(s - m)
                parts.append([m, jnp.sum(p, axis=1, keepdims=True), None])
                ps.append(p.astype(BF16))
            o = _dot(jnp.concatenate(ps, axis=0),
                     jnp.concatenate([vbuf[last, g], vbuf[last, g + 1]], axis=1))
            parts[g][2] = o[:heads, :d]
            parts[g + 1][2] = o[heads:, d:]
        for g in range(BATCH):
            b = items[i * BATCH + g] // per
            m, l, o = parts[g]
            m_old = m_s[b]
            m_new = jnp.maximum(m_old, m)
            w_old = jnp.exp2(m_old - m_new)
            w = jnp.exp2(m - m_new)
            m_s[b] = m_new
            l_s[b] = l_s[b] * w_old + l * w
            acc[b] = acc[b] * w_old + o * w

        @pl.when(i + RING - 1 < batches)
        def _():
            fetch(i + RING - 1)
        return c

    lax.fori_loop(0, batches + 1, step, 0)

    lane = lax.broadcasted_iota(jnp.int32, (16, 128), 1)
    for c in range(rows // 16):
        l = l_s[c * 16:c * 16 + 16]
        o = acc[c * 16:c * 16 + 16] / l
        lse = m_s[c * 16:c * 16 + 16] + jnp.log2(l)
        o_ref[:heads, c * 16:c * 16 + 16, :] = jnp.swapaxes(o, 0, 1)
        lse = jnp.swapaxes(lse, 0, 1)
        out = jnp.zeros((16, 128), F32)
        for h in range(heads):
            out = jnp.where(lane == h, lse[h], out)
        o_ref[heads, c * 16:c * 16 + 16, :] = out


def _suffix(lens, q, kn, vn, k, v, scale):
    heads, rows, d = q.shape
    slots = k.shape[1]
    per = slots // SLOTS
    wide = SLOTS * heads
    k = k.reshape(rows * per, wide, d)
    v = v.reshape(rows * per, wide, d)
    return pl.pallas_call(
        functools.partial(_suffix_kernel, scale),
        in_specs=[pl.BlockSpec(memory_space=pltpu.SMEM)] + [pl.BlockSpec(memory_space=VM)] * 3
        + [pl.BlockSpec(memory_space=pl.ANY)] * 2,
        out_specs=pl.BlockSpec(memory_space=VM),
        out_shape=jax.ShapeDtypeStruct((heads + 1, rows, d), F32),
        scratch_shapes=[
            pltpu.SMEM((rows * per + 4 * BATCH,), jnp.int32),
            VM((rows + 1, heads, d), BF16),
            VM((rows + 1, heads, d), F32),
            VM((rows + 1, heads, 128), F32),
            VM((rows + 1, heads, 128), F32),
            VM((RING, BATCH, wide, d), BF16),
            VM((RING, BATCH, wide, d), BF16),
            VM((2, BATCH, heads, wide), F32),
            pltpu.SemaphoreType.DMA((RING,)),
            pltpu.SemaphoreType.DMA((RING,)),
        ],
        compiler_params=pltpu.CompilerParams(vmem_limit_bytes=LIMIT),
        cost_estimate=_cost(2e10, 4 * k.size),
    )(lens, q, kn, vn, k, v)


def _weights(ls):
    m = functools.reduce(jnp.maximum, ls)
    ws = [jnp.exp2(l - m) for l in ls]
    t = functools.reduce(jnp.add, ws)
    return [w / t for w in ws]


def _half(w_hbm, other):
    half = w_hbm.shape[1] // 2
    me = lax.axis_index('tp')
    return w_hbm.at[:, pl.ds(pl.multiple_of((1 - me if other else me) * half, half), half)]


def _send_kernel(own_ref, near_ref, far_ref, suf_ref, w_hbm, att_ref, o0_ref, o1_ref, bufs, acc, sem):
    heads = own_ref.shape[0] - 1
    cols = o0_ref.shape[1]

    def emit(i):
        o0_ref[...] = acc[:, :cols].astype(BF16)
        o1_ref[...] = acc[:, cols:].astype(BF16)
    start, run = _stream(att_ref, [_half(w_hbm, True)], bufs, sem, acc, bufs.shape[1], emit)
    _prime(start, 8)
    far_lse = far_ref[heads].astype(F32) + far_ref[heads + 1].astype(F32) + far_ref[heads + 2].astype(F32)
    ws = _weights([own_ref[heads], near_ref[heads], far_lse, suf_ref[heads]])
    for h in range(heads):
        a = ws[0][:, h:h + 1] * own_ref[h]
        for w, r in zip(ws[1:], (near_ref, far_ref, suf_ref)):
            a += w[:, h:h + 1] * r[h].astype(F32)
        att_ref[:, h * 128:(h + 1) * 128] = a.astype(BF16)
    run()


def _keep_kernel(att_hbm, x_hbm, w_hbm, o0_ref, o1_ref, att_ref, x_ref, bufs, acc, xsem, sem):
    cols = o0_ref.shape[1]
    half = 2 * cols
    at = pl.multiple_of(lax.axis_index('tp') * half, half)
    cps = [pltpu.make_async_copy(att_hbm, att_ref, xsem.at[0]),
           pltpu.make_async_copy(x_hbm.at[:, pl.ds(at, half)], x_ref, xsem.at[1])]

    def emit(i):
        cps[1].wait()
        y = acc[...] + x_ref[...].astype(F32)
        o0_ref[...] = y[:, :cols]
        o1_ref[...] = y[:, cols:]
    start, run = _stream(att_ref, [_half(w_hbm, False)], bufs, sem, acc, bufs.shape[1], emit)
    for c in cps:
        c.start()
    _prime(start, 8)
    cps[0].wait()
    run()


def _out_send(own, near, far, suf, w_o):
    rows = own.shape[1]
    depth, cols = w_o.shape
    cols //= 2
    return pl.pallas_call(
        _send_kernel,
        in_specs=[pl.BlockSpec(memory_space=VM)] * 4 + [pl.BlockSpec(memory_space=pl.ANY)],
        out_specs=[pl.BlockSpec(memory_space=VM)] * 3,
        out_shape=[jax.ShapeDtypeStruct((rows, depth), BF16)] + [jax.ShapeDtypeStruct((rows, cols // 2), BF16)] * 2,
        scratch_shapes=[VM((RINGW, CHUNK, cols), BF16), VM((rows, cols), F32), pltpu.SemaphoreType.DMA((RINGW,))],
        compiler_params=pltpu.CompilerParams(vmem_limit_bytes=LIMIT),
        cost_estimate=_cost(2 * rows * depth * cols, 2 * depth * cols),
    )(own, near, far, suf, w_o)


def _out_keep(att, x, w_o):
    rows, depth = att.shape
    cols = w_o.shape[1] // 2
    return pl.pallas_call(
        _keep_kernel,
        in_specs=[pl.BlockSpec(memory_space=pl.ANY)] * 3,
        out_specs=[pl.BlockSpec(memory_space=VM)] * 2,
        out_shape=[jax.ShapeDtypeStruct((rows, cols // 2), F32)] * 2,
        scratch_shapes=[VM((rows, depth), BF16), VM((rows, cols), BF16), VM((RINGW, CHUNK, cols), BF16),
                        VM((rows, cols), F32), pltpu.SemaphoreType.DMA((2,)), pltpu.SemaphoreType.DMA((RINGW,))],
        compiler_params=pltpu.CompilerParams(vmem_limit_bytes=LIMIT),
        cost_estimate=_cost(2 * rows * depth * cols, 2 * depth * cols),
    )(att, x, w_o)


def solution(mesh):
    n_ctx = mesh.shape['ctx']
    row_axes = ('dp', 'ctx')
    chip_swap = [(i, i ^ 2) for i in range(n_ctx)]
    core_swap = [(i, i ^ 1) for i in range(n_ctx)]
    tp_swap = [(0, 1), (1, 0)]

    def device_step(hidden, w_q, w_k, w_v, w_o, k_prefix, v_prefix, k_suffix, v_suffix, seq_lens):
        scale = LOG2E * k_prefix.shape[2] ** -0.5
        far = lambda a: lax.ppermute(a, 'ctx', chip_swap)
        near = lambda a: lax.ppermute(a, 'ctx', core_swap)
        q = _project_q(hidden, w_q)
        q_far = far(q)
        q_near = near(q)
        kn, vn, kt, vt = _project_kv(hidden, w_k, w_v, k_prefix, v_prefix)
        q_far, kt = lax.optimization_barrier((q_far, kt))
        o_diag, o_far = _prefix(near(q_far), q_far, kt, vt, scale)
        o_diag, q_near = lax.optimization_barrier((o_diag, q_near))
        o_diag = near(o_diag)
        o_near, o_own = _prefix(q_near, q, kt, vt, scale)
        o_x = far(_merge(o_far, o_diag))
        o_near = near(o_near)
        o_suf = _suffix(seq_lens, q, kn, vn, k_suffix, v_suffix, scale)
        att, s0, s1 = _out_send(o_own, o_near, o_x, o_suf, w_o)
        swap = lambda a: lax.ppermute(a, 'tp', tp_swap)
        sent = [swap(s0), swap(s1)]
        kept = _out_keep(att, hidden, w_o)
        mine = [(a + b.astype(F32)).astype(BF16) for a, b in zip(kept, sent)]
        other = [swap(a) for a in mine]
        mine, other = jnp.concatenate(mine, axis=1), jnp.concatenate(other, axis=1)
        me = lax.axis_index('tp')
        return jnp.where(me == 0, jnp.concatenate([mine, other], axis=1), jnp.concatenate([other, mine], axis=1))

    spec_in = (P(row_axes, None), P(None, 'tp'), P(None, 'tp'), P(None, 'tp'), P('tp', None),
               P(row_axes, 'tp', None), P(row_axes, 'tp', None), P(row_axes, None, 'tp', None),
               P(row_axes, None, 'tp', None), P(row_axes))
    return jax.shard_map(device_step, mesh=mesh, in_specs=spec_in, out_specs=P(row_axes, None), check_vma=False)
```

```python
import functools

import jax
import jax.numpy as jnp
from jax import lax
from jax.experimental import pallas as pl
from jax.experimental.pallas import tpu as pltpu
from jax.sharding import PartitionSpec as P

F32 = jnp.float32
BF16 = jnp.bfloat16
VM = pltpu.VMEM
LOG2E = 1.4426950408889634
BATCH = 16
SLOTS = 16
RING = 5
CHUNK = 512
RINGW = 5
LIMIT = 56 * 2**20


def _cost(flops, nbytes):
    return pl.CostEstimate(flops=int(flops), bytes_accessed=int(nbytes), transcendentals=0)


def _dot(a, b, dims=(((1,), (0,)), ((), ()))):
    return lax.dot_general(a, b, dims, preferred_element_type=F32)


NT = (((1,), (1,)), ((), ()))


MESH = pl.DeviceIdType.MESH


def _stream(x_ref, ws, bufs, sem, acc, emit, extra_start=None, extra_body=None):
    ring, chunk, cols = bufs.shape
    n = ws[0].shape[0] // chunk
    total = n * len(ws)
    part = 512

    def start(g):
        slot = lax.rem(g, ring)
        for i, w in enumerate(ws):
            @pl.when((g >= i * n) & (g < (i + 1) * n))
            def _():
                at = pl.multiple_of((g - i * n) * chunk, chunk)
                pltpu.make_async_copy(w.at[pl.ds(at, chunk)], bufs.at[slot], sem.at[slot]).start()
        if extra_start is not None:
            extra_start(g)

    def prime():
        def body(g, c):
            start(g)
            return c
        lax.fori_loop(0, min(ring, total), body, 0)

    def run():
        for i, w in enumerate(ws):
            acc[...] = jnp.zeros_like(acc)

            def body(c, carry):
                g = i * n + c
                slot = lax.rem(g, ring)
                pltpu.make_async_copy(w.at[pl.ds(0, chunk)], bufs.at[slot], sem.at[slot]).wait()
                x = x_ref[:, pl.ds(pl.multiple_of(c * chunk, chunk), chunk)]
                for j in range(0, cols, part):
                    acc[:, j:j + part] += _dot(x, bufs[slot, :, j:j + part])
                if extra_body is not None:
                    extra_body(i, g)
                start(g + ring)
                return carry
            lax.fori_loop(0, n, body, 0)
            emit(i)
    return prime, run


def _front_kernel(scale, x_hbm, wq_hbm, wk_hbm, wv_hbm, kp_hbm, vp_hbm, q_hbm, kn_hbm, vn_hbm, out_ref,
                  x_ref, bufs, acc, raw, kt, vt, qs, kvn, ds, dr, ns, nr, fo, wo, xs, xr, xl, xlr,
                  xsem, sem, psem, osem, q_s, q_r, d_s, d_r, n_s, n_r, x_s, x_r):
    heads, n_pos, d = kt.shape
    rows = x_ref.shape[0]
    ring, chunk, _ = bufs.shape
    me = lax.axis_index('ctx')
    near = me + 1 - 2 * lax.rem(me, 2)
    far = me + 2 - 4 * (me // 2)
    n = x_hbm.shape[1] // chunk
    pos = n_pos // (2 * n)

    cp = pltpu.make_async_copy(x_hbm, x_ref, xsem)
    cp.start()

    def remote(src, dst, s, r, to):
        return pltpu.make_async_remote_copy(src_ref=src, dst_ref=dst, send_sem=s, recv_sem=r,
                                            device_id={'ctx': to}, device_id_type=MESH)

    hh = heads // 2
    q_near = remote(qs.at[0], qs.at[1], q_s.at[0], q_r.at[0], near)
    q_far = [remote(qs.at[0, pl.ds(j * hh, hh)], qs.at[2, pl.ds(j * hh, hh)], q_s.at[1 + j], q_r.at[1 + j], far)
             for j in range(2)]
    q_diag = [remote(qs.at[2, pl.ds(j * hh, hh)], qs.at[3, pl.ds(j * hh, hh)], q_s.at[3 + j], q_r.at[3 + j], near)
              for j in range(2)]
    outs = [pltpu.make_async_copy(qs.at[0], q_hbm, osem.at[0]),
            pltpu.make_async_copy(kvn.at[0], kn_hbm, osem.at[1]),
            pltpu.make_async_copy(kvn.at[1], vn_hbm, osem.at[2])]

    def pieces(g):
        at = pl.ds((g - n) * pos, pos)
        slot = lax.rem(g, ring)
        return [pltpu.make_async_copy(src.at[at], raw.at[slot, j], psem.at[slot, j])
                for j, src in enumerate((kp_hbm, vp_hbm))]

    def extra_start(g):
        @pl.when((g >= n) & (g < 3 * n))
        def _():
            for c in pieces(g):
                c.start()

    def extra_body(i, g):
        if i == 0:
            return
        slot = lax.rem(g, ring)
        for c in pieces(g):
            c.wait()
        for j, dst in enumerate((kt, vt)):
            for u in range(pos // 16):
                at = pl.multiple_of((g - n) * pos + u * 16, 16)
                dst[:, pl.ds(at, 16), :] = jnp.swapaxes(raw[slot, j, u * 16:u * 16 + 16], 0, 1)

    def emit(i):
        dst = qs.at[0] if i == 0 else kvn.at[i - 1]
        for h in range(heads):
            dst[h] = acc[:, h * d:(h + 1) * d].astype(BF16)
        if i == 0:
            pl.semaphore_wait(barrier, 2)
            for c in (q_far[0], q_far[1], q_near):
                c.start()
        outs[i].start()

    prime, run = _stream(x_ref, [wq_hbm, wk_hbm, wv_hbm], bufs, sem, acc, emit, extra_start, extra_body)
    prime()
    barrier = pltpu.get_barrier_semaphore()
    for to in (near, far):
        pl.semaphore_signal(barrier, inc=1, device_id={'ctx': to}, device_id_type=MESH)
    cp.wait()
    run()

    for j in range(2):
        q_far[j].wait_recv()
        q_diag[j].start()

    lane = lax.broadcasted_iota(jnp.int32, (rows, d), 1)
    group = 2
    steps = heads // group

    def attend(units):
        for qi, h, dst in units:
            s = _dot(qs[qi, h], kt[h], NT)
            m = jnp.max(s, axis=1, keepdims=True) * scale
            e = jnp.exp2(s * scale - m)
            l = jnp.sum(e, axis=1, keepdims=True)
            o = _dot(e.astype(BF16), vt[h])
            dst[h, 0] = o / l
            dst[h, 1] = jnp.broadcast_to(m + jnp.log2(l), (rows, d))

    def d_copy(i):
        at = pl.ds(i * group, group)
        return remote(ds.at[at], dr.at[at], d_s.at[i], d_r.at[i], near)

    def n_copy(i):
        at = pl.ds(i * group, group)
        return remote(ns.at[at], nr.at[at], n_s.at[i], n_r.at[i], near)

    def x_copy(i):
        at = pl.ds(i * group, group)
        return remote(xs.at[at], xr.at[at], x_s.at[i], x_r.at[i], far)

    xl_copy = remote(xl, xlr, x_s.at[steps], x_r.at[steps], far)

    def merge_far(i):
        d_copy(i).wait_recv()
        for u in range(group):
            h = i * group + u
            l0, l1 = fo[h, 1], dr[h, 1]
            m = jnp.maximum(l0, l1)
            w0, w1 = jnp.exp2(l0 - m), jnp.exp2(l1 - m)
            t = w0 + w1
            xs[h] = ((w0 * fo[h, 0] + w1 * dr[h, 0]) / t).astype(BF16)
            xl[...] = jnp.where(lane == h, m + jnp.log2(t), xl[...])
        x_copy(i).start()

    q_diag[0].wait_recv()
    q_diag[1].wait_recv()
    xl[...] = jnp.zeros_like(xl)

    def far_step(i, c):
        attend([(qi, i * group + u, dst) for u in range(group) for qi, dst in ((3, ds), (2, fo))])
        d_copy(i).start()

        @pl.when(i > 0)
        def _():
            merge_far(i - 1)
        return c
    lax.fori_loop(0, steps, far_step, 0)

    q_near.wait_recv()

    def near_step(i, c):
        attend([(qi, i * group + u, dst) for u in range(group) for qi, dst in ((1, ns), (0, wo))])
        n_copy(i).start()

        @pl.when(i == 0)
        def _():
            merge_far(steps - 1)
            xl_copy.start()
        return c
    lax.fori_loop(0, steps, near_step, 0)

    xl_copy.wait_recv()
    far_lse = xlr[...]
    lse_out = jnp.zeros((rows, d), F32)
    for h in range(heads):
        if h % group == 0:
            n_copy(h // group).wait_recv()
            x_copy(h // group).wait_recv()
        l0, l1, l2 = wo[h, 1], nr[h, 1], jnp.broadcast_to(far_lse[:, h:h + 1], (rows, d))
        m = jnp.maximum(jnp.maximum(l0, l1), l2)
        w0, w1, w2 = jnp.exp2(l0 - m), jnp.exp2(l1 - m), jnp.exp2(l2 - m)
        t = w0 + w1 + w2
        out_ref[h] = (w0 * wo[h, 0] + w1 * nr[h, 0] + w2 * xr[h].astype(F32)) / t
        lse_out = jnp.where(lane == h, m + jnp.log2(t), lse_out)
    out_ref[heads] = lse_out

    for c in outs:
        c.wait()
    for c in [q_near] + q_far + q_diag + [xl_copy]:
        c.wait_send()

    def drain(i, c):
        d_copy(i).wait_send()
        n_copy(i).wait_send()
        x_copy(i).wait_send()
        return c
    lax.fori_loop(0, steps, drain, 0)


def _front(x, wq, wk, wv, kp, vp, scale):
    rows, depth = x.shape
    cols = wq.shape[1]
    n, heads, d = kp.shape
    pos = n // (2 * depth // CHUNK)
    dma = pltpu.SemaphoreType.DMA
    blk = (heads, rows, d)
    pair = (heads, 2, rows, d)
    return pl.pallas_call(
        functools.partial(_front_kernel, scale),
        in_specs=[pl.BlockSpec(memory_space=pl.ANY)] * 6,
        out_specs=[pl.BlockSpec(memory_space=pl.ANY)] * 3 + [pl.BlockSpec(memory_space=VM)],
        out_shape=[jax.ShapeDtypeStruct(blk, BF16)] * 3 + [jax.ShapeDtypeStruct((heads + 1, rows, d), F32)],
        scratch_shapes=[
            VM((rows, depth), BF16), VM((RINGW, CHUNK, cols), BF16), VM((rows, cols), F32),
            VM((RINGW, 2, pos, heads, d), BF16), VM((heads, n, d), BF16), VM((heads, n, d), BF16),
            VM((4,) + blk, BF16), VM((2,) + blk, BF16),
            VM(pair, F32), VM(pair, F32), VM(pair, F32), VM(pair, F32), VM(pair, F32), VM(pair, F32),
            VM(blk, BF16), VM(blk, BF16), VM((rows, d), F32), VM((rows, d), F32),
            dma, dma((RINGW,)), dma((RINGW, 2)), dma((3,)), dma((5,)), dma((5,)),
            dma((heads // 2,)), dma((heads // 2,)), dma((heads // 2,)), dma((heads // 2,)),
            dma((heads // 2 + 1,)), dma((heads // 2 + 1,))],
        compiler_params=pltpu.CompilerParams(vmem_limit_bytes=LIMIT, collective_id=0, has_side_effects=True),
        cost_estimate=_cost(5e10, 6 * depth * cols),
    )(x, wq, wk, wv, kp, vp)


def _suffix_kernel(scale, lens, q_ref, kn_ref, vn_ref, k_hbm, v_hbm, o_ref,
                   items, qb, acc, m_s, l_s, kbuf, vbuf, sbuf, ksem, vsem):
    heads, rows, d = q_ref.shape
    per = k_hbm.shape[0] // rows
    wide = SLOTS * heads
    dummy = rows * per

    for g in range(BATCH):
        items[g] = dummy

    def listing(b, t):
        for j in range(per):
            items[BATCH + t + j] = b * per + j
        return t + (lens[b] + SLOTS - 1) // SLOTS
    total = lax.fori_loop(0, rows, listing, 0)
    for g in range(2 * BATCH):
        items[BATCH + total + g] = dummy
    batches = (total + BATCH - 1) // BATCH

    def fetch(i):
        slot = lax.rem(i, RING)
        for g in range(BATCH):
            it = jnp.minimum(items[BATCH + i * BATCH + g], dummy - 1)
            pltpu.make_async_copy(k_hbm.at[it], kbuf.at[slot, g], ksem.at[slot]).start()
            pltpu.make_async_copy(v_hbm.at[it], vbuf.at[slot, g], vsem.at[slot]).start()

    def prime(i, c):
        fetch(i)
        return c
    lax.fori_loop(0, jnp.minimum(batches, RING - 1), prime, 0)

    for c in range(rows // 16):
        q = jnp.swapaxes(q_ref[:, c * 16:c * 16 + 16, :], 0, 1)
        kn = jnp.swapaxes(kn_ref[:, c * 16:c * 16 + 16, :], 0, 1)
        vn = jnp.swapaxes(vn_ref[:, c * 16:c * 16 + 16, :], 0, 1)
        qb[c * 16:c * 16 + 16] = q
        s = jnp.sum(q.astype(F32) * kn.astype(F32), axis=-1, keepdims=True) * scale
        m_s[c * 16:c * 16 + 16] = jnp.broadcast_to(s, (16, heads, 128))
        l_s[c * 16:c * 16 + 16] = jnp.ones((16, heads, 128), F32)
        acc[c * 16:c * 16 + 16] = vn.astype(F32)

    row = lax.broadcasted_iota(jnp.int32, (heads, wide), 0)
    col = lax.broadcasted_iota(jnp.int32, (heads, wide), 1)
    slot_of = jnp.where(lax.rem(col, heads) == row, col // heads, 1 << 20)

    def step(i, c):
        slot = lax.rem(i, RING)
        last = lax.rem(i + RING - 1, RING)
        par = lax.rem(i, 2)

        @pl.when(i < batches)
        def _():
            pltpu.make_async_copy(k_hbm.at[pl.ds(0, BATCH)], kbuf.at[slot], ksem.at[slot]).wait()

        @pl.when(i > 0)
        def _():
            pltpu.make_async_copy(v_hbm.at[pl.ds(0, BATCH)], vbuf.at[last], vsem.at[last]).wait()

        for g in range(BATCH):
            it = items[BATCH + i * BATCH + g]
            b = it // per
            left = lens[jnp.minimum(b, rows - 1)] - lax.rem(it, per) * SLOTS
            s = _dot(qb[b], kbuf[slot, g], NT) * scale
            sbuf[par, g] = jnp.where(slot_of < left, s, -jnp.inf)

        parts = []
        for g in range(0, BATCH, 2):
            ps = []
            for u in range(2):
                s = sbuf[1 - par, g + u]
                m = jnp.max(s, axis=1, keepdims=True)
                p = jnp.exp2(s - m)
                parts.append([m, jnp.sum(p, axis=1, keepdims=True), None])
                ps.append(p.astype(BF16))
            o = _dot(jnp.concatenate(ps, axis=0),
                     jnp.concatenate([vbuf[last, g], vbuf[last, g + 1]], axis=1))
            parts[g][2] = o[:heads, :d]
            parts[g + 1][2] = o[heads:, d:]
        for g in range(BATCH):
            b = items[i * BATCH + g] // per
            m, l, o = parts[g]
            m_old = m_s[b]
            m_new = jnp.maximum(m_old, m)
            w_old = jnp.exp2(m_old - m_new)
            w = jnp.exp2(m - m_new)
            m_s[b] = m_new
            l_s[b] = l_s[b] * w_old + l * w
            acc[b] = acc[b] * w_old + o * w

        @pl.when(i + RING - 1 < batches)
        def _():
            fetch(i + RING - 1)
        return c

    lax.fori_loop(0, batches + 1, step, 0)

    lane = lax.broadcasted_iota(jnp.int32, (16, 128), 1)
    for c in range(rows // 16):
        l = l_s[c * 16:c * 16 + 16]
        o = acc[c * 16:c * 16 + 16] / l
        lse = m_s[c * 16:c * 16 + 16] + jnp.log2(l)
        o_ref[:heads, c * 16:c * 16 + 16, :] = jnp.swapaxes(o, 0, 1)
        lse = jnp.swapaxes(lse, 0, 1)
        out = jnp.zeros((16, 128), F32)
        for h in range(heads):
            out = jnp.where(lane == h, lse[h], out)
        o_ref[heads, c * 16:c * 16 + 16, :] = out


def _suffix(lens, q, kn, vn, k, v, scale):
    heads, rows, d = q.shape
    slots = k.shape[1]
    per = slots // SLOTS
    wide = SLOTS * heads
    k = k.reshape(rows * per, wide, d)
    v = v.reshape(rows * per, wide, d)
    return pl.pallas_call(
        functools.partial(_suffix_kernel, scale),
        in_specs=[pl.BlockSpec(memory_space=pltpu.SMEM)] + [pl.BlockSpec(memory_space=VM)] * 3
        + [pl.BlockSpec(memory_space=pl.ANY)] * 2,
        out_specs=pl.BlockSpec(memory_space=VM),
        out_shape=jax.ShapeDtypeStruct((heads + 1, rows, d), F32),
        scratch_shapes=[
            pltpu.SMEM((rows * per + 4 * BATCH,), jnp.int32),
            VM((rows + 1, heads, d), BF16),
            VM((rows + 1, heads, d), F32),
            VM((rows + 1, heads, 128), F32),
            VM((rows + 1, heads, 128), F32),
            VM((RING, BATCH, wide, d), BF16),
            VM((RING, BATCH, wide, d), BF16),
            VM((2, BATCH, heads, wide), F32),
            pltpu.SemaphoreType.DMA((RING,)),
            pltpu.SemaphoreType.DMA((RING,)),
        ],
        compiler_params=pltpu.CompilerParams(vmem_limit_bytes=LIMIT),
        cost_estimate=_cost(2e10, 4 * k.size),
    )(lens, q, kn, vn, k, v)


def _weights(ls):
    m = functools.reduce(jnp.maximum, ls)
    ws = [jnp.exp2(l - m) for l in ls]
    t = functools.reduce(jnp.add, ws)
    return [w / t for w in ws]


def _half(w_hbm, other):
    half = w_hbm.shape[1] // 2
    me = lax.axis_index('tp')
    return w_hbm.at[:, pl.ds(pl.multiple_of((1 - me if other else me) * half, half), half)]


def _send_kernel(pre_ref, suf_ref, w_hbm, att_ref, o0_ref, o1_ref, bufs, acc, sem):
    heads = pre_ref.shape[0] - 1
    cols = o0_ref.shape[1]

    def emit(i):
        o0_ref[...] = acc[:, :cols].astype(BF16)
        o1_ref[...] = acc[:, cols:].astype(BF16)
    prime, run = _stream(att_ref, [_half(w_hbm, True)], bufs, sem, acc, emit)
    prime()
    ws = _weights([pre_ref[heads], suf_ref[heads]])
    for h in range(heads):
        a = ws[0][:, h:h + 1] * pre_ref[h] + ws[1][:, h:h + 1] * suf_ref[h]
        att_ref[:, h * 128:(h + 1) * 128] = a.astype(BF16)
    run()


def _keep_kernel(att_hbm, x_hbm, w_hbm, o0_ref, o1_ref, att_ref, x_ref, bufs, acc, xsem, sem):
    cols = o0_ref.shape[1]
    half = 2 * cols
    at = pl.multiple_of(lax.axis_index('tp') * half, half)
    cps = [pltpu.make_async_copy(att_hbm, att_ref, xsem.at[0]),
           pltpu.make_async_copy(x_hbm.at[:, pl.ds(at, half)], x_ref, xsem.at[1])]

    def emit(i):
        cps[1].wait()
        y = acc[...] + x_ref[...].astype(F32)
        o0_ref[...] = y[:, :cols]
        o1_ref[...] = y[:, cols:]
    prime, run = _stream(att_ref, [_half(w_hbm, False)], bufs, sem, acc, emit)
    for c in cps:
        c.start()
    prime()
    cps[0].wait()
    run()


def _out_send(pre, suf, w_o):
    rows = pre.shape[1]
    depth, cols = w_o.shape
    cols //= 2
    return pl.pallas_call(
        _send_kernel,
        in_specs=[pl.BlockSpec(memory_space=VM)] * 2 + [pl.BlockSpec(memory_space=pl.ANY)],
        out_specs=[pl.BlockSpec(memory_space=VM)] * 3,
        out_shape=[jax.ShapeDtypeStruct((rows, depth), BF16)] + [jax.ShapeDtypeStruct((rows, cols // 2), BF16)] * 2,
        scratch_shapes=[VM((RINGW, CHUNK, cols), BF16), VM((rows, cols), F32), pltpu.SemaphoreType.DMA((RINGW,))],
        compiler_params=pltpu.CompilerParams(vmem_limit_bytes=LIMIT),
        cost_estimate=_cost(2 * rows * depth * cols, 2 * depth * cols),
    )(pre, suf, w_o)


def _out_keep(att, x, w_o):
    rows, depth = att.shape
    cols = w_o.shape[1] // 2
    return pl.pallas_call(
        _keep_kernel,
        in_specs=[pl.BlockSpec(memory_space=pl.ANY)] * 3,
        out_specs=[pl.BlockSpec(memory_space=VM)] * 2,
        out_shape=[jax.ShapeDtypeStruct((rows, cols // 2), F32)] * 2,
        scratch_shapes=[VM((rows, depth), BF16), VM((rows, cols), BF16), VM((RINGW, CHUNK, cols), BF16),
                        VM((rows, cols), F32), pltpu.SemaphoreType.DMA((2,)), pltpu.SemaphoreType.DMA((RINGW,))],
        compiler_params=pltpu.CompilerParams(vmem_limit_bytes=LIMIT),
        cost_estimate=_cost(2 * rows * depth * cols, 2 * depth * cols),
    )(att, x, w_o)


def solution(mesh):
    row_axes = ('dp', 'ctx')
    tp_swap = [(0, 1), (1, 0)]

    def device_step(hidden, w_q, w_k, w_v, w_o, k_prefix, v_prefix, k_suffix, v_suffix, seq_lens):
        scale = LOG2E * k_prefix.shape[2] ** -0.5
        q, kn, vn, pre = _front(hidden, w_q, w_k, w_v, k_prefix, v_prefix, scale)
        suf = _suffix(seq_lens, q, kn, vn, k_suffix, v_suffix, scale)
        att, s0, s1 = _out_send(pre, suf, w_o)
        swap = lambda a: lax.ppermute(a, 'tp', tp_swap)
        sent = [swap(s0), swap(s1)]
        kept = _out_keep(att, hidden, w_o)
        mine = [(a + b.astype(F32)).astype(BF16) for a, b in zip(kept, sent)]
        other = [swap(a) for a in mine]
        mine, other = jnp.concatenate(mine, axis=1), jnp.concatenate(other, axis=1)
        me = lax.axis_index('tp')
        return jnp.where(me == 0, jnp.concatenate([mine, other], axis=1), jnp.concatenate([other, mine], axis=1))

    spec_in = (P(row_axes, None), P(None, 'tp'), P(None, 'tp'), P(None, 'tp'), P('tp', None),
               P(row_axes, 'tp', None), P(row_axes, 'tp', None), P(row_axes, None, 'tp', None),
               P(row_axes, None, 'tp', None), P(row_axes))
    return jax.shard_map(device_step, mesh=mesh, in_specs=spec_in, out_specs=P(row_axes, None), check_vma=False)
```

```python
import functools

import jax
import jax.numpy as jnp
from jax import lax
from jax.experimental import pallas as pl
from jax.experimental.pallas import tpu as pltpu
from jax.sharding import PartitionSpec as P

F32 = jnp.float32
BF16 = jnp.bfloat16
VM = pltpu.VMEM
LOG2E = 1.4426950408889634
BATCH = 16
SLOTS = 16
RING = 5
CHUNK = 512
RINGW = 5
LIMIT = 56 * 2**20


def _cost(flops, nbytes):
    return pl.CostEstimate(flops=int(flops), bytes_accessed=int(nbytes), transcendentals=0)


def _dot(a, b, dims=(((1,), (0,)), ((), ()))):
    return lax.dot_general(a, b, dims, preferred_element_type=F32)


NT = (((1,), (1,)), ((), ()))


MESH = pl.DeviceIdType.MESH


def _stream(x_ref, ws, bufs, sem, acc, emit, extra_start=None, extra_body=None):
    ring, chunk, cols = bufs.shape
    n = ws[0].shape[0] // chunk
    total = n * len(ws)
    part = 512

    def start(g):
        slot = lax.rem(g, ring)
        for i, w in enumerate(ws):
            @pl.when((g >= i * n) & (g < (i + 1) * n))
            def _():
                at = pl.multiple_of((g - i * n) * chunk, chunk)
                pltpu.make_async_copy(w.at[pl.ds(at, chunk)], bufs.at[slot], sem.at[slot]).start()
        if extra_start is not None:
            extra_start(g)

    def prime():
        def body(g, c):
            start(g)
            return c
        lax.fori_loop(0, min(ring, total), body, 0)

    def run():
        for i, w in enumerate(ws):
            acc[...] = jnp.zeros_like(acc)

            def body(c, carry):
                g = i * n + c
                slot = lax.rem(g, ring)
                pltpu.make_async_copy(w.at[pl.ds(0, chunk)], bufs.at[slot], sem.at[slot]).wait()
                x = x_ref[:, pl.ds(pl.multiple_of(c * chunk, chunk), chunk)]
                for j in range(0, cols, part):
                    acc[:, j:j + part] += _dot(x, bufs[slot, :, j:j + part])
                if extra_body is not None:
                    extra_body(i, g)
                start(g + ring)
                return carry
            lax.fori_loop(0, n, body, 0)
            emit(i)
    return prime, run


def _peers():
    me = lax.axis_index('ctx')
    return me + 1 - 2 * lax.rem(me, 2), me + 2 - 4 * (me // 2)


def _remote(src, dst, s, r, **to):
    return pltpu.make_async_remote_copy(src_ref=src, dst_ref=dst, send_sem=s, recv_sem=r,
                                        device_id=to, device_id_type=MESH)


def _front_kernel(x_hbm, wq_hbm, wk_hbm, wv_hbm, kp_hbm, vp_hbm, q_hbm, kn_hbm, vn_hbm, kt_hbm, vt_hbm,
                  x_ref, bufs, acc, raw, kt, vt, qs, kvn,
                  xsem, sem, psem, osem, tsem, q_s, q_r):
    heads, n_pos, d = kt.shape
    ring, chunk, _ = bufs.shape
    near, far = _peers()
    n = x_hbm.shape[1] // chunk
    pos = n_pos // (2 * n)
    stages = 4
    span = n_pos // stages

    cp = pltpu.make_async_copy(x_hbm, x_ref, xsem)
    cp.start()

    hh = heads // 2
    half = [pl.ds(j * hh, hh) for j in range(2)]
    q_near = _remote(qs.at[0], qs.at[1], q_s.at[0], q_r.at[0], ctx=near)
    q_far = [_remote(qs.at[0, at], qs.at[2, at], q_s.at[1 + j], q_r.at[1 + j], ctx=far) for j, at in enumerate(half)]
    q_diag = [_remote(qs.at[2, at], qs.at[3, at], q_s.at[3 + j], q_r.at[3 + j], ctx=near) for j, at in enumerate(half)]
    outs = [pltpu.make_async_copy(qs.at[0], q_hbm.at[0], osem.at[0]),
            pltpu.make_async_copy(kvn.at[0], kn_hbm, osem.at[1]),
            pltpu.make_async_copy(kvn.at[1], vn_hbm, osem.at[2])]

    def pieces(g):
        at = pl.ds((g - n) * pos, pos)
        slot = lax.rem(g, ring)
        return [pltpu.make_async_copy(src.at[at], raw.at[slot, j], psem.at[slot, j])
                for j, src in enumerate((kp_hbm, vp_hbm))]

    def stores(t):
        at = pl.ds(pl.multiple_of(t * span, span), span)
        return [pltpu.make_async_copy(src.at[:, at], dst.at[:, at], tsem.at[j, t])
                for j, (src, dst) in enumerate(((kt, kt_hbm), (vt, vt_hbm)))]

    def extra_start(g):
        @pl.when((g >= n) & (g < 3 * n))
        def _():
            for c in pieces(g):
                c.start()

    def extra_body(i, g):
        if i == 0:
            return
        slot = lax.rem(g, ring)
        for c in pieces(g):
            c.wait()
        for j, dst in enumerate((kt, vt)):
            for u in range(pos // 16):
                at = pl.multiple_of((g - n) * pos + u * 16, 16)
                dst[:, pl.ds(at, 16), :] = jnp.swapaxes(raw[slot, j, u * 16:u * 16 + 16], 0, 1)
        done = (g - n + 1) * pos

        @pl.when(lax.rem(done, span) == 0)
        def _():
            for c in stores(done // span - 1):
                c.start()

    def emit(i):
        dst = qs.at[0] if i == 0 else kvn.at[i - 1]
        for h in range(heads):
            dst[h] = acc[:, h * d:(h + 1) * d].astype(BF16)
        if i == 0:
            pl.semaphore_wait(barrier, 2)
            for c in (q_far[0], q_far[1], q_near):
                c.start()
        outs[i].start()

    prime, run = _stream(x_ref, [wq_hbm, wk_hbm, wv_hbm], bufs, sem, acc, emit, extra_start, extra_body)
    prime()
    barrier = pltpu.get_barrier_semaphore()
    for to in (near, far):
        pl.semaphore_signal(barrier, inc=1, device_id={'ctx': to}, device_id_type=MESH)
    cp.wait()
    run()

    for j in range(2):
        q_far[j].wait_recv()
        q_diag[j].start()
    q_near.wait_recv()
    for c in q_diag:
        c.wait_recv()
    rest = pltpu.make_async_copy(qs.at[pl.ds(1, 3)], q_hbm.at[pl.ds(1, 3)], xsem)
    rest.start()
    for c in outs + [rest]:
        c.wait()
    for t in range(stages):
        for c in stores(t):
            c.wait()
    for c in [q_near] + q_far + q_diag:
        c.wait_send()


def _front(x, wq, wk, wv, kp, vp):
    rows, depth = x.shape
    cols = wq.shape[1]
    n, heads, d = kp.shape
    pos = n // (2 * depth // CHUNK)
    dma = pltpu.SemaphoreType.DMA
    blk = (heads, rows, d)
    return pl.pallas_call(
        _front_kernel,
        in_specs=[pl.BlockSpec(memory_space=pl.ANY)] * 6,
        out_specs=[pl.BlockSpec(memory_space=pl.ANY)] * 5,
        out_shape=[jax.ShapeDtypeStruct((4,) + blk, BF16)] + [jax.ShapeDtypeStruct(blk, BF16)] * 2
        + [jax.ShapeDtypeStruct((heads, n, d), BF16)] * 2,
        scratch_shapes=[
            VM((rows, depth), BF16), VM((RINGW, CHUNK, cols), BF16), VM((rows, cols), F32),
            VM((RINGW, 2, pos, heads, d), BF16), VM((heads, n, d), BF16), VM((heads, n, d), BF16),
            VM((4,) + blk, BF16), VM((2,) + blk, BF16),
            dma, dma((RINGW,)), dma((RINGW, 2)), dma((3,)), dma((2, 4)), dma((5,)), dma((5,))],
        compiler_params=pltpu.CompilerParams(vmem_limit_bytes=LIMIT, collective_id=0, has_side_effects=True),
        cost_estimate=_cost(2e10, 6 * depth * cols),
    )(x, wq, wk, wv, kp, vp)


def _back_kernel(scale, q_hbm, kt_hbm, vt_hbm, suf_hbm, x_hbm, w_hbm, y_ref,
                 qs, kt, vt, suf, x_ref, wo, ds, dr, ns, nr, fo, mo, xs, xr, xl, xlr, att, keep, ps, pr,
                 qsem, ksem, wsem, d_s, d_r, n_s, n_r, x_s, x_r, p_s, p_r, y_s, y_r):
    heads, n_pos, d = kt.shape
    rows = x_ref.shape[0]
    rh = rows // 2
    cols = x_ref.shape[1]
    half = cols // 2
    near, far = _peers()
    tp = lax.axis_index('tp')
    steps = 4
    group = heads // steps
    wide = ps.shape[-1]
    blocks = half // wide

    barrier = pltpu.get_barrier_semaphore()
    for to in ({'ctx': near}, {'ctx': far}, {'tp': 1 - tp}):
        pl.semaphore_signal(barrier, inc=1, device_id=to, device_id_type=MESH)
    q_cp = pltpu.make_async_copy(q_hbm, qs, qsem.at[0])
    q_cp.start()
    kv_cp = [[pltpu.make_async_copy(src.at[pl.ds(i * group, group)], dst.at[pl.ds(i * group, group)], ksem.at[j, i])
              for j, (src, dst) in enumerate(((kt_hbm, kt), (vt_hbm, vt)))] for i in range(steps)]
    for cs in kv_cp:
        for c in cs:
            c.start()
    suf_cp = pltpu.make_async_copy(suf_hbm, suf, qsem.at[1])
    x_cp = pltpu.make_async_copy(x_hbm, x_ref, qsem.at[2])
    wr = w_hbm.shape[0] // 4
    w_cp = [pltpu.make_async_copy(w_hbm.at[pl.ds(i * wr, wr)], wo.at[pl.ds(i * wr, wr)], wsem.at[i]) for i in range(4)]
    for c in [suf_cp, x_cp] + w_cp:
        c.start()

    lane = lax.broadcasted_iota(jnp.int32, (rh, d), 1)

    def d_copy(a, i):
        at = pl.ds(i * group, group)
        return _remote(ds.at[a, at], dr.at[a, at], d_s.at[a, i], d_r.at[a, i], ctx=near)

    def n_copy(a, i):
        at = pl.ds(i * group, group)
        return _remote(ns.at[a, at], nr.at[a, at], n_s.at[a, i], n_r.at[a, i], ctx=near)

    def x_copy(a, i):
        at = pl.ds(i * group, group)
        return _remote(xs.at[a, at], xr.at[a, at], x_s.at[a, i], x_r.at[a, i], ctx=far)

    def l_copy(a):
        return _remote(xl.at[a], xlr.at[a], x_s.at[a, steps], x_r.at[a, steps], ctx=far)

    def p_copy(a, j):
        return _remote(ps.at[a, j], pr.at[a, j], p_s.at[a, j], p_r.at[a, j], tp=1 - tp)

    def y_copy(a, j):
        at = (pl.ds(a * rh, rh), pl.ds(pl.multiple_of(tp * half + j * wide, wide), wide))
        return _remote(y_ref.at[at], y_ref.at[at], y_s.at[a, j], y_r.at[a, j], tp=1 - tp)

    def attend(a, h, q0, q1, dst0, dst1):
        at = slice(a * rh, (a + 1) * rh)
        q = jnp.concatenate([qs[q0, h, at], qs[q1, h, at]], axis=0)
        s = _dot(q, kt[h], NT)
        m = jnp.max(s, axis=1, keepdims=True) * scale
        e = jnp.exp2(s * scale - m)
        l = jnp.sum(e, axis=1, keepdims=True)
        o = _dot(e.astype(BF16), vt[h]) / l
        lse = jnp.broadcast_to(m + jnp.log2(l), (rows, d))
        dst0[h, 0], dst0[h, 1] = o[:rh], lse[:rh]
        dst1[h, 0], dst1[h, 1] = o[rh:], lse[rh:]

    def merge_far(a, i):
        d_copy(a, i).wait_recv()
        for u in range(group):
            h = i * group + u
            l0, l1 = fo[h, 1], dr[a, h, 1]
            m = jnp.maximum(l0, l1)
            w0, w1 = jnp.exp2(l0 - m), jnp.exp2(l1 - m)
            t = w0 + w1
            xs[a, h] = ((w0 * fo[h, 0] + w1 * dr[a, h, 0]) / t).astype(BF16)
            xl[a] = jnp.where(lane == h, m + jnp.log2(t), xl[a])
        x_copy(a, i).start()

    def add_peer(a):
        for j in range(blocks):
            p_copy(a, j).wait_recv()
            y = (keep[a, j] + pr[a, j].astype(F32)).astype(BF16)
            y_ref[a * rh:(a + 1) * rh, pl.ds(pl.multiple_of(tp * half + j * wide, wide), wide)] = y
            y_copy(a, j).start()

    xl[...] = jnp.zeros_like(xl)
    q_cp.wait()
    for a in range(2):
        def far_step(i, c):
            if a == 0:
                for k in range(steps):
                    @pl.when(i == k)
                    def _():
                        for cp in kv_cp[k]:
                            cp.wait()
            for u in range(group):
                attend(a, i * group + u, 3, 2, ds.at[a], fo)
            if a == 0:
                @pl.when(i == 0)
                def _():
                    pl.semaphore_wait(barrier, 3)
            d_copy(a, i).start()

            @pl.when(i > 0)
            def _():
                merge_far(a, i - 1)
            return c
        lax.fori_loop(0, steps, far_step, 0)

        def near_step(i, c):
            for u in range(group):
                attend(a, i * group + u, 1, 0, ns.at[a], mo)
            n_copy(a, i).start()

            @pl.when(i == 0)
            def _():
                merge_far(a, steps - 1)
                l_copy(a).start()
                if a == 1:
                    add_peer(0)
            return c
        lax.fori_loop(0, steps, near_step, 0)

        if a == 0:
            suf_cp.wait()
            x_cp.wait()
        at = slice(a * rh, (a + 1) * rh)
        l_copy(a).wait_recv()
        far_lse, suf_lse = xlr[a], suf[heads, at]
        for h in range(heads):
            if h % group == 0:
                n_copy(a, h // group).wait_recv()
                x_copy(a, h // group).wait_recv()
            ls = [mo[h, 1], nr[a, h, 1], jnp.broadcast_to(far_lse[:, h:h + 1], (rh, d)),
                  jnp.broadcast_to(suf_lse[:, h:h + 1], (rh, d))]
            m = functools.reduce(jnp.maximum, ls)
            ws = [jnp.exp2(l - m) for l in ls]
            o = ws[0] * mo[h, 0] + ws[1] * nr[a, h, 0] + ws[2] * xr[a, h].astype(F32) + ws[3] * suf[h, at]
            att[:, h * d:(h + 1) * d] = (o / functools.reduce(jnp.add, ws)).astype(BF16)
        if a == 0:
            for c in w_cp:
                c.wait()

        def send_block(j, c):
            cols_at = pl.ds(pl.multiple_of((1 - tp) * half + j * wide, wide), wide)
            ps[a, j] = _dot(att[...], wo[:, cols_at]).astype(BF16)
            p_copy(a, j).start()
            return c
        lax.fori_loop(0, blocks, send_block, 0)

        def keep_block(j, c):
            cols_at = pl.ds(pl.multiple_of(tp * half + j * wide, wide), wide)
            keep[a, j] = _dot(att[...], wo[:, cols_at]) + x_ref[at, cols_at].astype(F32)
            return c
        lax.fori_loop(0, blocks, keep_block, 0)

    add_peer(1)
    for a in range(2):
        for j in range(blocks):
            y_copy(a, j).wait_recv()
            y_copy(a, j).wait_send()
            p_copy(a, j).wait_send()
        for i in range(steps):
            d_copy(a, i).wait_send()
            n_copy(a, i).wait_send()
            x_copy(a, i).wait_send()
        l_copy(a).wait_send()


def _back(q, kt, vt, suf, x, w_o, scale):
    _, heads, rows, d = q.shape
    n = kt.shape[1]
    depth, cols = w_o.shape
    dma = pltpu.SemaphoreType.DMA
    rh, wide, steps = rows // 2, 512, 4
    blocks = cols // 2 // wide
    return pl.pallas_call(
        functools.partial(_back_kernel, scale),
        in_specs=[pl.BlockSpec(memory_space=pl.ANY)] * 6,
        out_specs=pl.BlockSpec(memory_space=VM),
        out_shape=jax.ShapeDtypeStruct((rows, cols), BF16),
        scratch_shapes=[
            VM(q.shape, BF16), VM(kt.shape, BF16), VM(vt.shape, BF16), VM(suf.shape, F32), VM((rows, cols), BF16),
            VM(w_o.shape, BF16)]
        + [VM((2, heads, 2, rh, d), F32)] * 4 + [VM((heads, 2, rh, d), F32)] * 2
        + [VM((2, heads, rh, d), BF16)] * 2 + [VM((2, rh, d), F32)] * 2
        + [VM((rh, depth), BF16), VM((2, blocks, rh, wide), F32)] + [VM((2, blocks, rh, wide), BF16)] * 2
        + [dma((3,)), dma((2, steps)), dma((4,))]
        + [dma((2, steps))] * 4 + [dma((2, steps + 1))] * 2 + [dma((2, blocks))] * 4,
        compiler_params=pltpu.CompilerParams(vmem_limit_bytes=62 * 2**20, collective_id=1, has_side_effects=True),
        cost_estimate=_cost(5e10, 2 * depth * cols),
    )(q, kt, vt, suf, x, w_o)


def _suffix_kernel(scale, lens, q_hbm, kn_hbm, vn_hbm, k_hbm, v_hbm, o_ref,
                   new, newsem, items, qb, acc, m_s, l_s, kbuf, vbuf, sbuf, ksem, vsem):
    _, heads, rows, d = new.shape
    news = [pltpu.make_async_copy(src, new.at[j], newsem.at[j])
            for j, src in enumerate((q_hbm.at[0], kn_hbm, vn_hbm))]
    for c in news:
        c.start()
    per = k_hbm.shape[0] // rows
    wide = SLOTS * heads
    dummy = rows * per

    for g in range(BATCH):
        items[g] = dummy

    def listing(b, t):
        for j in range(per):
            items[BATCH + t + j] = b * per + j
        return t + (lens[b] + SLOTS - 1) // SLOTS
    total = lax.fori_loop(0, rows, listing, 0)
    for g in range(2 * BATCH):
        items[BATCH + total + g] = dummy
    batches = (total + BATCH - 1) // BATCH

    def fetch(i):
        slot = lax.rem(i, RING)
        for g in range(BATCH):
            it = jnp.minimum(items[BATCH + i * BATCH + g], dummy - 1)
            pltpu.make_async_copy(k_hbm.at[it], kbuf.at[slot, g], ksem.at[slot]).start()
            pltpu.make_async_copy(v_hbm.at[it], vbuf.at[slot, g], vsem.at[slot]).start()

    def prime(i, c):
        fetch(i)
        return c
    lax.fori_loop(0, jnp.minimum(batches, RING - 1), prime, 0)

    for c in news:
        c.wait()
    for c in range(rows // 16):
        q, kn, vn = [jnp.swapaxes(new[j, :, c * 16:c * 16 + 16, :], 0, 1) for j in range(3)]
        qb[c * 16:c * 16 + 16] = q
        s = jnp.sum(q.astype(F32) * kn.astype(F32), axis=-1, keepdims=True) * scale
        m_s[c * 16:c * 16 + 16] = jnp.broadcast_to(s, (16, heads, 128))
        l_s[c * 16:c * 16 + 16] = jnp.ones((16, heads, 128), F32)
        acc[c * 16:c * 16 + 16] = vn.astype(F32)

    row = lax.broadcasted_iota(jnp.int32, (heads, wide), 0)
    col = lax.broadcasted_iota(jnp.int32, (heads, wide), 1)
    slot_of = jnp.where(lax.rem(col, heads) == row, col // heads, 1 << 20)

    def step(i, c):
        slot = lax.rem(i, RING)
        last = lax.rem(i + RING - 1, RING)
        par = lax.rem(i, 2)

        @pl.when(i < batches)
        def _():
            pltpu.make_async_copy(k_hbm.at[pl.ds(0, BATCH)], kbuf.at[slot], ksem.at[slot]).wait()

        @pl.when(i > 0)
        def _():
            pltpu.make_async_copy(v_hbm.at[pl.ds(0, BATCH)], vbuf.at[last], vsem.at[last]).wait()

        for g in range(BATCH):
            it = items[BATCH + i * BATCH + g]
            b = it // per
            left = lens[jnp.minimum(b, rows - 1)] - lax.rem(it, per) * SLOTS
            s = _dot(qb[b], kbuf[slot, g], NT) * scale
            sbuf[par, g] = jnp.where(slot_of < left, s, -jnp.inf)

        parts = []
        for g in range(0, BATCH, 2):
            ps = []
            for u in range(2):
                s = sbuf[1 - par, g + u]
                m = jnp.max(s, axis=1, keepdims=True)
                p = jnp.exp2(s - m)
                parts.append([m, jnp.sum(p, axis=1, keepdims=True), None])
                ps.append(p.astype(BF16))
            o = _dot(jnp.concatenate(ps, axis=0),
                     jnp.concatenate([vbuf[last, g], vbuf[last, g + 1]], axis=1))
            parts[g][2] = o[:heads, :d]
            parts[g + 1][2] = o[heads:, d:]
        for g in range(BATCH):
            b = items[i * BATCH + g] // per
            m, l, o = parts[g]
            m_old = m_s[b]
            m_new = jnp.maximum(m_old, m)
            w_old = jnp.exp2(m_old - m_new)
            w = jnp.exp2(m - m_new)
            m_s[b] = m_new
            l_s[b] = l_s[b] * w_old + l * w
            acc[b] = acc[b] * w_old + o * w

        @pl.when(i + RING - 1 < batches)
        def _():
            fetch(i + RING - 1)
        return c

    lax.fori_loop(0, batches + 1, step, 0)

    lane = lax.broadcasted_iota(jnp.int32, (16, 128), 1)
    for c in range(rows // 16):
        l = l_s[c * 16:c * 16 + 16]
        o = acc[c * 16:c * 16 + 16] / l
        lse = m_s[c * 16:c * 16 + 16] + jnp.log2(l)
        o_ref[:heads, c * 16:c * 16 + 16, :] = jnp.swapaxes(o, 0, 1)
        lse = jnp.swapaxes(lse, 0, 1)
        out = jnp.zeros((16, 128), F32)
        for h in range(heads):
            out = jnp.where(lane == h, lse[h], out)
        o_ref[heads, c * 16:c * 16 + 16, :] = out


def _suffix(lens, q, kn, vn, k, v, scale):
    _, heads, rows, d = q.shape
    slots = k.shape[1]
    per = slots // SLOTS
    wide = SLOTS * heads
    k = k.reshape(rows * per, wide, d)
    v = v.reshape(rows * per, wide, d)
    return pl.pallas_call(
        functools.partial(_suffix_kernel, scale),
        in_specs=[pl.BlockSpec(memory_space=pltpu.SMEM)] + [pl.BlockSpec(memory_space=pl.ANY)] * 5,
        out_specs=pl.BlockSpec(memory_space=VM),
        out_shape=jax.ShapeDtypeStruct((heads + 1, rows, d), F32),
        scratch_shapes=[
            VM((3, heads, rows, d), BF16),
            pltpu.SemaphoreType.DMA((3,)),
            pltpu.SMEM((rows * per + 4 * BATCH,), jnp.int32),
            VM((rows + 1, heads, d), BF16),
            VM((rows + 1, heads, d), F32),
            VM((rows + 1, heads, 128), F32),
            VM((rows + 1, heads, 128), F32),
            VM((RING, BATCH, wide, d), BF16),
            VM((RING, BATCH, wide, d), BF16),
            VM((2, BATCH, heads, wide), F32),
            pltpu.SemaphoreType.DMA((RING,)),
            pltpu.SemaphoreType.DMA((RING,)),
        ],
        compiler_params=pltpu.CompilerParams(vmem_limit_bytes=LIMIT),
        cost_estimate=_cost(2e10, 4 * k.size),
    )(lens, q, kn, vn, k, v)


def solution(mesh):
    row_axes = ('dp', 'ctx')
    def device_step(hidden, w_q, w_k, w_v, w_o, k_prefix, v_prefix, k_suffix, v_suffix, seq_lens):
        scale = LOG2E * k_prefix.shape[2] ** -0.5
        q, kn, vn, kt, vt = _front(hidden, w_q, w_k, w_v, k_prefix, v_prefix)
        suf = _suffix(seq_lens, q, kn, vn, k_suffix, v_suffix, scale)
        return _back(q, kt, vt, suf, hidden, w_o, scale)

    spec_in = (P(row_axes, None), P(None, 'tp'), P(None, 'tp'), P(None, 'tp'), P('tp', None),
               P(row_axes, 'tp', None), P(row_axes, 'tp', None), P(row_axes, None, 'tp', None),
               P(row_axes, None, 'tp', None), P(row_axes))
    return jax.shard_map(device_step, mesh=mesh, in_specs=spec_in, out_specs=P(row_axes, None), check_vma=False)
```

```python
import functools

import jax
import jax.numpy as jnp
from jax import lax
from jax.experimental import pallas as pl
from jax.experimental.pallas import tpu as pltpu
from jax.sharding import PartitionSpec as P

F32 = jnp.float32
BF16 = jnp.bfloat16
VM = pltpu.VMEM
LOG2E = 1.4426950408889634
BATCH = 16
SLOTS = 16
RING = 5
CHUNK = 512
RINGW = 5
LIMIT = 56 * 2**20


def _cost(flops, nbytes):
    return pl.CostEstimate(flops=int(flops), bytes_accessed=int(nbytes), transcendentals=0)


def _dot(a, b, dims=(((1,), (0,)), ((), ()))):
    return lax.dot_general(a, b, dims, preferred_element_type=F32)


NT = (((1,), (1,)), ((), ()))


MESH = pl.DeviceIdType.MESH


def _stream(x_ref, ws, bufs, sem, acc, emit, extra_start=None, extra_body=None):
    ring, chunk, cols = bufs.shape
    n = ws[0].shape[0] // chunk
    total = n * len(ws)
    part = 512

    def start(g):
        slot = lax.rem(g, ring)
        for i, w in enumerate(ws):
            @pl.when((g >= i * n) & (g < (i + 1) * n))
            def _():
                at = pl.multiple_of((g - i * n) * chunk, chunk)
                pltpu.make_async_copy(w.at[pl.ds(at, chunk)], bufs.at[slot], sem.at[slot]).start()
        if extra_start is not None:
            extra_start(g)

    def prime():
        def body(g, c):
            start(g)
            return c
        lax.fori_loop(0, min(ring, total), body, 0)

    def run():
        for i, w in enumerate(ws):
            acc[...] = jnp.zeros_like(acc)

            def body(c, carry):
                g = i * n + c
                slot = lax.rem(g, ring)
                pltpu.make_async_copy(w.at[pl.ds(0, chunk)], bufs.at[slot], sem.at[slot]).wait()
                x = x_ref[:, pl.ds(pl.multiple_of(c * chunk, chunk), chunk)]
                for j in range(0, cols, part):
                    acc[:, j:j + part] += _dot(x, bufs[slot, :, j:j + part])
                if extra_body is not None:
                    extra_body(i, g)
                start(g + ring)
                return carry
            lax.fori_loop(0, n, body, 0)
            emit(i)
    return prime, run


def _peers():
    me = lax.axis_index('ctx')
    return me + 1 - 2 * lax.rem(me, 2), me + 2 - 4 * (me // 2)


def _remote(src, dst, s, r, **to):
    return pltpu.make_async_remote_copy(src_ref=src, dst_ref=dst, send_sem=s, recv_sem=r,
                                        device_id=to, device_id_type=MESH)


def _front_kernel(x_hbm, wq_hbm, wk_hbm, wv_hbm, kp_hbm, vp_hbm, q_hbm, kn_hbm, vn_hbm, kt_hbm, vt_hbm,
                  x_ref, bufs, acc, raw, kt, vt, qs, kvn,
                  xsem, sem, psem, osem, tsem, q_s, q_r):
    heads, n_pos, d = kt.shape
    ring, chunk, _ = bufs.shape
    near, far = _peers()
    n = x_hbm.shape[1] // chunk
    pos = n_pos // (2 * n)
    stages = 4
    span = n_pos // stages

    cp = pltpu.make_async_copy(x_hbm, x_ref, xsem)
    cp.start()

    hh = heads // 2
    half = [pl.ds(j * hh, hh) for j in range(2)]
    q_near = _remote(qs.at[0], qs.at[1], q_s.at[0], q_r.at[0], ctx=near)
    q_far = [_remote(qs.at[0, at], qs.at[2, at], q_s.at[1 + j], q_r.at[1 + j], ctx=far) for j, at in enumerate(half)]
    q_diag = [_remote(qs.at[2, at], qs.at[3, at], q_s.at[3 + j], q_r.at[3 + j], ctx=near) for j, at in enumerate(half)]
    outs = [pltpu.make_async_copy(qs.at[0], q_hbm.at[0], osem.at[0]),
            pltpu.make_async_copy(kvn.at[0], kn_hbm, osem.at[1]),
            pltpu.make_async_copy(kvn.at[1], vn_hbm, osem.at[2])]

    def pieces(g):
        at = pl.ds((g - n) * pos, pos)
        slot = lax.rem(g, ring)
        return [pltpu.make_async_copy(src.at[at], raw.at[slot, j], psem.at[slot, j])
                for j, src in enumerate((kp_hbm, vp_hbm))]

    def stores(t):
        at = pl.ds(pl.multiple_of(t * span, span), span)
        return [pltpu.make_async_copy(src.at[:, at], dst.at[:, at], tsem.at[j, t])
                for j, (src, dst) in enumerate(((kt, kt_hbm), (vt, vt_hbm)))]

    def extra_start(g):
        @pl.when((g >= n) & (g < 3 * n))
        def _():
            for c in pieces(g):
                c.start()

    def extra_body(i, g):
        if i == 0:
            return
        slot = lax.rem(g, ring)
        for c in pieces(g):
            c.wait()
        for j, dst in enumerate((kt, vt)):
            for u in range(pos // 16):
                at = pl.multiple_of((g - n) * pos + u * 16, 16)
                dst[:, pl.ds(at, 16), :] = jnp.swapaxes(raw[slot, j, u * 16:u * 16 + 16], 0, 1)
        done = (g - n + 1) * pos

        @pl.when(lax.rem(done, span) == 0)
        def _():
            for c in stores(done // span - 1):
                c.start()

    def emit(i):
        dst = qs.at[0] if i == 0 else kvn.at[i - 1]
        for h in range(heads):
            dst[h] = acc[:, h * d:(h + 1) * d].astype(BF16)
        if i == 0:
            pl.semaphore_wait(barrier, 2)
            for c in (q_far[0], q_far[1], q_near):
                c.start()
        outs[i].start()

    prime, run = _stream(x_ref, [wq_hbm, wk_hbm, wv_hbm], bufs, sem, acc, emit, extra_start, extra_body)
    prime()
    barrier = pltpu.get_barrier_semaphore()
    for to in (near, far):
        pl.semaphore_signal(barrier, inc=1, device_id={'ctx': to}, device_id_type=MESH)
    cp.wait()
    run()

    for j in range(2):
        q_far[j].wait_recv()
        q_diag[j].start()
    q_near.wait_recv()
    for c in q_diag:
        c.wait_recv()
    rest = pltpu.make_async_copy(qs.at[pl.ds(1, 3)], q_hbm.at[pl.ds(1, 3)], xsem)
    rest.start()
    for c in outs + [rest]:
        c.wait()
    for t in range(stages):
        for c in stores(t):
            c.wait()
    for c in [q_near] + q_far + q_diag:
        c.wait_send()


def _front(x, wq, wk, wv, kp, vp):
    rows, depth = x.shape
    cols = wq.shape[1]
    n, heads, d = kp.shape
    pos = n // (2 * depth // CHUNK)
    dma = pltpu.SemaphoreType.DMA
    blk = (heads, rows, d)
    return pl.pallas_call(
        _front_kernel,
        in_specs=[pl.BlockSpec(memory_space=pl.ANY)] * 6,
        out_specs=[pl.BlockSpec(memory_space=pl.ANY)] * 5,
        out_shape=[jax.ShapeDtypeStruct((4,) + blk, BF16)] + [jax.ShapeDtypeStruct(blk, BF16)] * 2
        + [jax.ShapeDtypeStruct((heads, n, d), BF16)] * 2,
        scratch_shapes=[
            VM((rows, depth), BF16), VM((RINGW, CHUNK, cols), BF16), VM((rows, cols), F32),
            VM((RINGW, 2, pos, heads, d), BF16), VM((heads, n, d), BF16), VM((heads, n, d), BF16),
            VM((4,) + blk, BF16), VM((2,) + blk, BF16),
            dma, dma((RINGW,)), dma((RINGW, 2)), dma((3,)), dma((2, 4)), dma((5,)), dma((5,))],
        compiler_params=pltpu.CompilerParams(vmem_limit_bytes=LIMIT, collective_id=0, has_side_effects=True),
        cost_estimate=_cost(2e10, 6 * depth * cols),
    )(x, wq, wk, wv, kp, vp)


def _back_kernel(scale, q_hbm, kt_hbm, vt_hbm, suf_hbm, x_hbm, w_hbm, y_ref,
                 qs, kt, vt, suf, x_ref, wo, ds, dr, ns, nr, fo, mo, xs, xr, xl, xlr, att, keep, ps, pr, sb, mb,
                 qsem, ksem, wsem, d_s, d_r, n_s, n_r, x_s, x_r, p_s, p_r, y_s, y_r):
    heads, n_pos, d = kt.shape
    rows = x_ref.shape[0]
    rh = rows // 2
    cols = x_ref.shape[1]
    half = cols // 2
    near, far = _peers()
    tp = lax.axis_index('tp')
    steps = 4
    group = heads // steps
    wide = ps.shape[-1]
    blocks = half // wide

    barrier = pltpu.get_barrier_semaphore()
    for to in ({'ctx': near}, {'ctx': far}, {'tp': 1 - tp}):
        pl.semaphore_signal(barrier, inc=1, device_id=to, device_id_type=MESH)
    q_cp = pltpu.make_async_copy(q_hbm, qs, qsem.at[0])
    q_cp.start()
    kv_cp = [[pltpu.make_async_copy(src.at[pl.ds(i * group, group)], dst.at[pl.ds(i * group, group)], ksem.at[j, i])
              for j, (src, dst) in enumerate(((kt_hbm, kt), (vt_hbm, vt)))] for i in range(steps)]
    for cs in kv_cp:
        for c in cs:
            c.start()
    suf_cp = pltpu.make_async_copy(suf_hbm, suf, qsem.at[1])
    x_cp = pltpu.make_async_copy(x_hbm, x_ref, qsem.at[2])
    wr = w_hbm.shape[0] // 4
    w_cp = [pltpu.make_async_copy(w_hbm.at[pl.ds(i * wr, wr)], wo.at[pl.ds(i * wr, wr)], wsem.at[i]) for i in range(4)]
    for c in [suf_cp, x_cp] + w_cp:
        c.start()

    lane = lax.broadcasted_iota(jnp.int32, (rh, d), 1)

    def d_copy(a, i):
        at = pl.ds(i * group, group)
        return _remote(ds.at[a, at], dr.at[a, at], d_s.at[a, i], d_r.at[a, i], ctx=near)

    def n_copy(a, i):
        at = pl.ds(i * group, group)
        return _remote(ns.at[a, at], nr.at[a, at], n_s.at[a, i], n_r.at[a, i], ctx=near)

    def x_copy(a, i):
        at = pl.ds(i * group, group)
        return _remote(xs.at[a, at], xr.at[a, at], x_s.at[a, i], x_r.at[a, i], ctx=far)

    def l_copy(a):
        return _remote(xl.at[a], xlr.at[a], x_s.at[a, steps], x_r.at[a, steps], ctx=far)

    def p_copy(a, j):
        return _remote(ps.at[a, j], pr.at[a, j], p_s.at[a, j], p_r.at[a, j], tp=1 - tp)

    def y_copy(a, j):
        at = (pl.ds(a * rh, rh), pl.ds(pl.multiple_of(tp * half + j * wide, wide), wide))
        return _remote(y_ref.at[at], y_ref.at[at], y_s.at[a, j], y_r.at[a, j], tp=1 - tp)

    def scores(a, h, q0, q1, slot):
        at = slice(a * rh, (a + 1) * rh)
        q = jnp.concatenate([qs[q0, h, at], qs[q1, h, at]], axis=0)
        s = _dot(q, kt[h], NT)
        sb[slot] = s
        mb[slot] = jnp.broadcast_to(jnp.max(s, axis=1, keepdims=True) * scale, (rows, d))

    def weigh(h, slot, dst0, dst1):
        m = mb[slot]
        es, l = [], None
        for k in range(0, n_pos, d):
            e = jnp.exp2(sb[slot, :, k:k + d] * scale - m)
            l = e if l is None else l + e
            es.append(e.astype(BF16))
        l = jnp.sum(l, axis=1, keepdims=True)
        o = _dot(jnp.concatenate(es, axis=1), vt[h]) / l
        lse = m + jnp.log2(l)
        dst0[h, 0], dst0[h, 1] = o[:rh], lse[:rh]
        dst1[h, 0], dst1[h, 1] = o[rh:], lse[rh:]

    def attend(a, i, q0, q1, dst0, dst1):
        for u in range(group):
            h = i * group + u
            scores(a, jnp.minimum(h + 1, heads - 1), q0, q1, (u + 1) % 2)
            weigh(h, u % 2, dst0, dst1)

    def merge_far(a, i):
        d_copy(a, i).wait_recv()
        for u in range(group):
            h = i * group + u
            l0, l1 = fo[h, 1], dr[a, h, 1]
            m = jnp.maximum(l0, l1)
            w0, w1 = jnp.exp2(l0 - m), jnp.exp2(l1 - m)
            t = w0 + w1
            xs[a, h] = ((w0 * fo[h, 0] + w1 * dr[a, h, 0]) / t).astype(BF16)
            xl[a] = jnp.where(lane == h, m + jnp.log2(t), xl[a])
        x_copy(a, i).start()

    def add_peer(a):
        for j in range(blocks):
            p_copy(a, j).wait_recv()
            y = (keep[a, j] + pr[a, j].astype(F32)).astype(BF16)
            y_ref[a * rh:(a + 1) * rh, pl.ds(pl.multiple_of(tp * half + j * wide, wide), wide)] = y
            y_copy(a, j).start()

    xl[...] = jnp.zeros_like(xl)
    q_cp.wait()
    for cp in kv_cp[0]:
        cp.wait()
    for a in range(2):
        def far_step(i, c):
            if a == 0:
                for k in range(steps - 1):
                    @pl.when(i == k)
                    def _():
                        for cp in kv_cp[k + 1]:
                            cp.wait()
            attend(a, i, 3, 2, ds.at[a], fo)
            if a == 0:
                @pl.when(i == 0)
                def _():
                    pl.semaphore_wait(barrier, 3)
            d_copy(a, i).start()

            @pl.when(i > 0)
            def _():
                merge_far(a, i - 1)
            return c
        scores(a, 0, 3, 2, 0)
        lax.fori_loop(0, steps, far_step, 0)

        def near_step(i, c):
            attend(a, i, 1, 0, ns.at[a], mo)
            n_copy(a, i).start()

            @pl.when(i == 0)
            def _():
                merge_far(a, steps - 1)
                l_copy(a).start()
                if a == 1:
                    add_peer(0)
            return c
        scores(a, 0, 1, 0, 0)
        lax.fori_loop(0, steps, near_step, 0)

        if a == 0:
            suf_cp.wait()
            x_cp.wait()
        at = slice(a * rh, (a + 1) * rh)
        l_copy(a).wait_recv()
        far_lse, suf_lse = xlr[a], suf[heads, at]
        for h in range(heads):
            if h % group == 0:
                n_copy(a, h // group).wait_recv()
                x_copy(a, h // group).wait_recv()
            ls = [mo[h, 1], nr[a, h, 1], jnp.broadcast_to(far_lse[:, h:h + 1], (rh, d)),
                  jnp.broadcast_to(suf_lse[:, h:h + 1], (rh, d))]
            m = functools.reduce(jnp.maximum, ls)
            ws = [jnp.exp2(l - m) for l in ls]
            o = ws[0] * mo[h, 0] + ws[1] * nr[a, h, 0] + ws[2] * xr[a, h].astype(F32) + ws[3] * suf[h, at]
            att[:, h * d:(h + 1) * d] = (o / functools.reduce(jnp.add, ws)).astype(BF16)
        if a == 0:
            for c in w_cp:
                c.wait()

        def send_block(j, c):
            cols_at = pl.ds(pl.multiple_of((1 - tp) * half + j * wide, wide), wide)
            ps[a, j] = _dot(att[...], wo[:, cols_at]).astype(BF16)
            p_copy(a, j).start()
            return c
        lax.fori_loop(0, blocks, send_block, 0)

        def keep_block(j, c):
            cols_at = pl.ds(pl.multiple_of(tp * half + j * wide, wide), wide)
            keep[a, j] = _dot(att[...], wo[:, cols_at]) + x_ref[at, cols_at].astype(F32)
            return c
        lax.fori_loop(0, blocks, keep_block, 0)

    add_peer(1)
    for a in range(2):
        for j in range(blocks):
            y_copy(a, j).wait_recv()
            y_copy(a, j).wait_send()
            p_copy(a, j).wait_send()
        for i in range(steps):
            d_copy(a, i).wait_send()
            n_copy(a, i).wait_send()
            x_copy(a, i).wait_send()
        l_copy(a).wait_send()


def _back(q, kt, vt, suf, x, w_o, scale):
    _, heads, rows, d = q.shape
    n = kt.shape[1]
    depth, cols = w_o.shape
    dma = pltpu.SemaphoreType.DMA
    rh, wide, steps = rows // 2, 512, 4
    blocks = cols // 2 // wide
    return pl.pallas_call(
        functools.partial(_back_kernel, scale),
        in_specs=[pl.BlockSpec(memory_space=pl.ANY)] * 6,
        out_specs=pl.BlockSpec(memory_space=VM),
        out_shape=jax.ShapeDtypeStruct((rows, cols), BF16),
        scratch_shapes=[
            VM(q.shape, BF16), VM(kt.shape, BF16), VM(vt.shape, BF16), VM(suf.shape, F32), VM((rows, cols), BF16),
            VM(w_o.shape, BF16)]
        + [VM((2, heads, 2, rh, d), F32)] * 4 + [VM((heads, 2, rh, d), F32)] * 2
        + [VM((2, heads, rh, d), BF16)] * 2 + [VM((2, rh, d), F32)] * 2
        + [VM((rh, depth), BF16), VM((2, blocks, rh, wide), F32)] + [VM((2, blocks, rh, wide), BF16)] * 2
        + [VM((2, rows, n), F32), VM((2, rows, d), F32)]
        + [dma((3,)), dma((2, steps)), dma((4,))]
        + [dma((2, steps))] * 4 + [dma((2, steps + 1))] * 2 + [dma((2, blocks))] * 4,
        compiler_params=pltpu.CompilerParams(vmem_limit_bytes=62 * 2**20, collective_id=1, has_side_effects=True),
        cost_estimate=_cost(5e10, 2 * depth * cols),
    )(q, kt, vt, suf, x, w_o)


def _suffix_kernel(scale, lens, q_hbm, kn_hbm, vn_hbm, k_hbm, v_hbm, o_ref,
                   new, newsem, items, qb, acc, m_s, l_s, kbuf, vbuf, sbuf, ksem, vsem):
    _, heads, rows, d = new.shape
    news = [pltpu.make_async_copy(src, new.at[j], newsem.at[j])
            for j, src in enumerate((q_hbm.at[0], kn_hbm, vn_hbm))]
    for c in news:
        c.start()
    per = k_hbm.shape[0] // rows
    wide = SLOTS * heads
    dummy = rows * per

    for g in range(BATCH):
        items[g] = dummy

    def listing(b, t):
        for j in range(per):
            items[BATCH + t + j] = b * per + j
        return t + (lens[b] + SLOTS - 1) // SLOTS
    total = lax.fori_loop(0, rows, listing, 0)
    for g in range(2 * BATCH):
        items[BATCH + total + g] = dummy
    batches = (total + BATCH - 1) // BATCH

    def fetch(i):
        slot = lax.rem(i, RING)
        for g in range(BATCH):
            it = jnp.minimum(items[BATCH + i * BATCH + g], dummy - 1)
            pltpu.make_async_copy(k_hbm.at[it], kbuf.at[slot, g], ksem.at[slot]).start()
            pltpu.make_async_copy(v_hbm.at[it], vbuf.at[slot, g], vsem.at[slot]).start()

    def prime(i, c):
        fetch(i)
        return c
    lax.fori_loop(0, jnp.minimum(batches, RING - 1), prime, 0)

    for c in news:
        c.wait()
    for c in range(rows // 16):
        q, kn, vn = [jnp.swapaxes(new[j, :, c * 16:c * 16 + 16, :], 0, 1) for j in range(3)]
        qb[c * 16:c * 16 + 16] = q
        s = jnp.sum(q.astype(F32) * kn.astype(F32), axis=-1, keepdims=True) * scale
        m_s[c * 16:c * 16 + 16] = jnp.broadcast_to(s, (16, heads, 128))
        l_s[c * 16:c * 16 + 16] = jnp.ones((16, heads, 128), F32)
        acc[c * 16:c * 16 + 16] = vn.astype(F32)

    row = lax.broadcasted_iota(jnp.int32, (heads, wide), 0)
    col = lax.broadcasted_iota(jnp.int32, (heads, wide), 1)
    slot_of = jnp.where(lax.rem(col, heads) == row, col // heads, 1 << 20)

    def step(i, c):
        slot = lax.rem(i, RING)
        last = lax.rem(i + RING - 1, RING)
        par = lax.rem(i, 2)

        @pl.when(i < batches)
        def _():
            pltpu.make_async_copy(k_hbm.at[pl.ds(0, BATCH)], kbuf.at[slot], ksem.at[slot]).wait()

        @pl.when(i > 0)
        def _():
            pltpu.make_async_copy(v_hbm.at[pl.ds(0, BATCH)], vbuf.at[last], vsem.at[last]).wait()

        for g in range(BATCH):
            it = items[BATCH + i * BATCH + g]
            b = it // per
            left = lens[jnp.minimum(b, rows - 1)] - lax.rem(it, per) * SLOTS
            s = _dot(qb[b], kbuf[slot, g], NT) * scale
            sbuf[par, g] = jnp.where(slot_of < left, s, -jnp.inf)

        parts = []
        for g in range(0, BATCH, 2):
            ps = []
            for u in range(2):
                s = sbuf[1 - par, g + u]
                m = jnp.max(s, axis=1, keepdims=True)
                p = jnp.exp2(s - m)
                parts.append([m, jnp.sum(p, axis=1, keepdims=True), None])
                ps.append(p.astype(BF16))
            o = _dot(jnp.concatenate(ps, axis=0),
                     jnp.concatenate([vbuf[last, g], vbuf[last, g + 1]], axis=1))
            parts[g][2] = o[:heads, :d]
            parts[g + 1][2] = o[heads:, d:]
        for g in range(BATCH):
            b = items[i * BATCH + g] // per
            m, l, o = parts[g]
            m_old = m_s[b]
            m_new = jnp.maximum(m_old, m)
            w_old = jnp.exp2(m_old - m_new)
            w = jnp.exp2(m - m_new)
            m_s[b] = m_new
            l_s[b] = l_s[b] * w_old + l * w
            acc[b] = acc[b] * w_old + o * w

        @pl.when(i + RING - 1 < batches)
        def _():
            fetch(i + RING - 1)
        return c

    lax.fori_loop(0, batches + 1, step, 0)

    lane = lax.broadcasted_iota(jnp.int32, (16, 128), 1)
    for c in range(rows // 16):
        l = l_s[c * 16:c * 16 + 16]
        o = acc[c * 16:c * 16 + 16] / l
        lse = m_s[c * 16:c * 16 + 16] + jnp.log2(l)
        o_ref[:heads, c * 16:c * 16 + 16, :] = jnp.swapaxes(o, 0, 1)
        lse = jnp.swapaxes(lse, 0, 1)
        out = jnp.zeros((16, 128), F32)
        for h in range(heads):
            out = jnp.where(lane == h, lse[h], out)
        o_ref[heads, c * 16:c * 16 + 16, :] = out


def _suffix(lens, q, kn, vn, k, v, scale):
    _, heads, rows, d = q.shape
    slots = k.shape[1]
    per = slots // SLOTS
    wide = SLOTS * heads
    k = k.reshape(rows * per, wide, d)
    v = v.reshape(rows * per, wide, d)
    return pl.pallas_call(
        functools.partial(_suffix_kernel, scale),
        in_specs=[pl.BlockSpec(memory_space=pltpu.SMEM)] + [pl.BlockSpec(memory_space=pl.ANY)] * 5,
        out_specs=pl.BlockSpec(memory_space=VM),
        out_shape=jax.ShapeDtypeStruct((heads + 1, rows, d), F32),
        scratch_shapes=[
            VM((3, heads, rows, d), BF16),
            pltpu.SemaphoreType.DMA((3,)),
            pltpu.SMEM((rows * per + 4 * BATCH,), jnp.int32),
            VM((rows + 1, heads, d), BF16),
            VM((rows + 1, heads, d), F32),
            VM((rows + 1, heads, 128), F32),
            VM((rows + 1, heads, 128), F32),
            VM((RING, BATCH, wide, d), BF16),
            VM((RING, BATCH, wide, d), BF16),
            VM((2, BATCH, heads, wide), F32),
            pltpu.SemaphoreType.DMA((RING,)),
            pltpu.SemaphoreType.DMA((RING,)),
        ],
        compiler_params=pltpu.CompilerParams(vmem_limit_bytes=LIMIT),
        cost_estimate=_cost(2e10, 4 * k.size),
    )(lens, q, kn, vn, k, v)


def solution(mesh):
    row_axes = ('dp', 'ctx')
    def device_step(hidden, w_q, w_k, w_v, w_o, k_prefix, v_prefix, k_suffix, v_suffix, seq_lens):
        scale = LOG2E * k_prefix.shape[2] ** -0.5
        q, kn, vn, kt, vt = _front(hidden, w_q, w_k, w_v, k_prefix, v_prefix)
        suf = _suffix(seq_lens, q, kn, vn, k_suffix, v_suffix, scale)
        return _back(q, kt, vt, suf, hidden, w_o, scale)

    spec_in = (P(row_axes, None), P(None, 'tp'), P(None, 'tp'), P(None, 'tp'), P('tp', None),
               P(row_axes, 'tp', None), P(row_axes, 'tp', None), P(row_axes, None, 'tp', None),
               P(row_axes, None, 'tp', None), P(row_axes))
    return jax.shard_map(device_step, mesh=mesh, in_specs=spec_in, out_specs=P(row_axes, None), check_vma=False)
```

```python
import functools

import jax
import jax.numpy as jnp
from jax import lax
from jax.experimental import pallas as pl
from jax.experimental.pallas import tpu as pltpu
from jax.sharding import PartitionSpec as P

F32 = jnp.float32
BF16 = jnp.bfloat16
VM = pltpu.VMEM
LOG2E = 1.4426950408889634
BATCH = 16
SLOTS = 16
RING = 5
CHUNK = 512
RINGW = 5
LIMIT = 56 * 2**20


def _cost(flops, nbytes):
    return pl.CostEstimate(flops=int(flops), bytes_accessed=int(nbytes), transcendentals=0)


def _dot(a, b, dims=(((1,), (0,)), ((), ()))):
    return lax.dot_general(a, b, dims, preferred_element_type=F32)


NT = (((1,), (1,)), ((), ()))


MESH = pl.DeviceIdType.MESH


def _stream(x_ref, ws, bufs, sem, acc, emit, extra_start=None, extra_body=None):
    ring, chunk, cols = bufs.shape
    n = ws[0].shape[0] // chunk
    total = n * len(ws)
    part = 512

    def start(g):
        slot = lax.rem(g, ring)
        for i, w in enumerate(ws):
            @pl.when((g >= i * n) & (g < (i + 1) * n))
            def _():
                at = pl.multiple_of((g - i * n) * chunk, chunk)
                pltpu.make_async_copy(w.at[pl.ds(at, chunk)], bufs.at[slot], sem.at[slot]).start()
        if extra_start is not None:
            extra_start(g)

    def prime():
        def body(g, c):
            start(g)
            return c
        lax.fori_loop(0, min(ring, total), body, 0)

    def run():
        for i, w in enumerate(ws):
            acc[...] = jnp.zeros_like(acc)

            def body(c, carry):
                g = i * n + c
                slot = lax.rem(g, ring)
                pltpu.make_async_copy(w.at[pl.ds(0, chunk)], bufs.at[slot], sem.at[slot]).wait()
                x = x_ref[:, pl.ds(pl.multiple_of(c * chunk, chunk), chunk)]
                for j in range(0, cols, part):
                    acc[:, j:j + part] += _dot(x, bufs[slot, :, j:j + part])
                if extra_body is not None:
                    extra_body(i, g)
                start(g + ring)
                return carry
            lax.fori_loop(0, n, body, 0)
            emit(i)
    return prime, run


def _peers():
    me = lax.axis_index('ctx')
    return me + 1 - 2 * lax.rem(me, 2), me + 2 - 4 * (me // 2)


def _remote(src, dst, s, r, **to):
    return pltpu.make_async_remote_copy(src_ref=src, dst_ref=dst, send_sem=s, recv_sem=r,
                                        device_id=to, device_id_type=MESH)


def _front_kernel(x_hbm, wq_hbm, wk_hbm, wv_hbm, q_hbm, kn_hbm, vn_hbm,
                  x_ref, bufs, acc, qs, kvn, xsem, sem, osem, q_s, q_r):
    _, heads, _, d = qs.shape
    near, far = _peers()
    cp = pltpu.make_async_copy(x_hbm, x_ref, xsem)
    cp.start()
    q_near = _remote(qs.at[0], qs.at[1], q_s.at[0], q_r.at[0], ctx=near)
    q_far = _remote(qs.at[0], qs.at[2], q_s.at[1], q_r.at[1], ctx=far)
    outs = [pltpu.make_async_copy(qs.at[0], q_hbm.at[0], osem.at[0]),
            pltpu.make_async_copy(kvn.at[0], kn_hbm, osem.at[1]),
            pltpu.make_async_copy(kvn.at[1], vn_hbm, osem.at[2])]
    rest = [pltpu.make_async_copy(qs.at[j], q_hbm.at[j], osem.at[2 + j]) for j in (1, 2)]

    def emit(i):
        dst = qs.at[0] if i == 0 else kvn.at[i - 1]
        for h in range(heads):
            dst[h] = acc[:, h * d:(h + 1) * d].astype(BF16)
        if i == 0:
            pl.semaphore_wait(barrier, 2)
            q_far.start()
            q_near.start()
        outs[i].start()

    prime, run = _stream(x_ref, [wq_hbm, wk_hbm, wv_hbm], bufs, sem, acc, emit)
    prime()
    barrier = pltpu.get_barrier_semaphore()
    for to in (near, far):
        pl.semaphore_signal(barrier, inc=1, device_id={'ctx': to}, device_id_type=MESH)
    cp.wait()
    run()
    for c, r in zip((q_near, q_far), rest):
        c.wait_recv()
        r.start()
    for c in outs + rest:
        c.wait()
    q_near.wait_send()
    q_far.wait_send()


def _front(x, wq, wk, wv, d):
    rows, depth = x.shape
    cols = wq.shape[1]
    dma = pltpu.SemaphoreType.DMA
    blk = (cols // d, rows, d)
    return pl.pallas_call(
        _front_kernel,
        in_specs=[pl.BlockSpec(memory_space=pl.ANY)] * 4,
        out_specs=[pl.BlockSpec(memory_space=pl.ANY)] * 3,
        out_shape=[jax.ShapeDtypeStruct((3,) + blk, BF16)] + [jax.ShapeDtypeStruct(blk, BF16)] * 2,
        scratch_shapes=[
            VM((rows, depth), BF16), VM((RINGW, CHUNK, cols), BF16), VM((rows, cols), F32),
            VM((3,) + blk, BF16), VM((2,) + blk, BF16),
            dma, dma((RINGW,)), dma((5,)), dma((2,)), dma((2,))],
        compiler_params=pltpu.CompilerParams(vmem_limit_bytes=LIMIT, collective_id=0, has_side_effects=True),
        cost_estimate=_cost(2e10, 6 * depth * cols),
    )(x, wq, wk, wv)


def _back_kernel(scale, q_hbm, kp_hbm, vp_hbm, suf_hbm, x_hbm, w_hbm, y_hbm,
                 y_ref, raw, qs, kt, vt, suf, x_ref, wo, ds, dr, ns, nr, fo, mo, xs, xr, xl, xlr, att, keep, ps, pr, sb, mb,
                 qsem, ksem, wsem, osem, q_s, q_r, d_s, d_r, n_s, n_r, x_s, x_r, p_s, p_r, y_s, y_r):
    heads, n_pos, d = kt.shape
    rows = x_ref.shape[0]
    rh = rows // 2
    cols = x_ref.shape[1]
    half = cols // 2
    near, far = _peers()
    tp = lax.axis_index('tp')
    steps = 4
    group = heads // steps
    wide = ps.shape[-1]
    blocks = half // wide

    barrier = pltpu.get_barrier_semaphore()
    for to in ({'ctx': near}, {'ctx': far}, {'tp': 1 - tp}):
        pl.semaphore_signal(barrier, inc=1, device_id=to, device_id_type=MESH)
    ring, _, pos = raw.shape[:3]
    q_cp = [pltpu.make_async_copy(q_hbm.at[j], qs.at[j], qsem.at[2 + j]) for j in range(3)]
    q_cp[2].start()

    def piece(g):
        slot = lax.rem(g, ring)
        return [pltpu.make_async_copy(src.at[pl.ds(g * pos, pos)], raw.at[slot, j], ksem.at[slot, j])
                for j, src in enumerate((kp_hbm, vp_hbm))]
    for g in range(ring):
        for c in piece(g):
            c.start()
    q_cp[0].start()
    q_cp[1].start()
    suf_cp = pltpu.make_async_copy(suf_hbm, suf, qsem.at[0])
    x_cp = pltpu.make_async_copy(x_hbm, x_ref, qsem.at[1])
    wr = w_hbm.shape[0] // 4
    w_cp = [pltpu.make_async_copy(w_hbm.at[pl.ds(i * wr, wr)], wo.at[pl.ds(i * wr, wr)], wsem.at[i]) for i in range(4)]
    q_diag = _remote(qs.at[2], qs.at[3], q_s.at[0], q_r.at[0], ctx=near)
    q_cp[2].wait()
    pl.semaphore_wait(barrier, 3)
    q_diag.start()

    def relayout(g, c):
        slot = lax.rem(g, ring)
        for cp in piece(g):
            cp.wait()
        for j, dst in enumerate((kt, vt)):
            for u in range(pos // 16):
                to = pl.multiple_of(g * pos + u * 16, 16)
                dst[:, pl.ds(to, 16), :] = jnp.swapaxes(raw[slot, j, u * 16:u * 16 + 16], 0, 1)

        @pl.when(g + ring < n_pos // pos)
        def _():
            for cp in piece(g + ring):
                cp.start()
        return c
    lax.fori_loop(0, n_pos // pos, relayout, 0)
    for c in [suf_cp, x_cp] + w_cp:
        c.start()

    lane = lax.broadcasted_iota(jnp.int32, (rh, d), 1)

    def d_copy(a, i):
        at = pl.ds(i * group, group)
        return _remote(ds.at[a, at], dr.at[a, at], d_s.at[a, i], d_r.at[a, i], ctx=near)

    def n_copy(a, i):
        at = pl.ds(i * group, group)
        return _remote(ns.at[a, at], nr.at[a, at], n_s.at[a, i], n_r.at[a, i], ctx=near)

    def x_copy(a, i):
        at = pl.ds(i * group, group)
        return _remote(xs.at[a, at], xr.at[a, at], x_s.at[a, i], x_r.at[a, i], ctx=far)

    def l_copy(a):
        return _remote(xl.at[a], xlr.at[a], x_s.at[a, steps], x_r.at[a, steps], ctx=far)

    def p_copy(a, j):
        return _remote(ps.at[a, j], pr.at[a, j], p_s.at[a, j], p_r.at[a, j], tp=1 - tp)

    def y_copy(a, j):
        at = (pl.ds(a * rh, rh), pl.ds(pl.multiple_of(tp * half + j * wide, wide), wide))
        return _remote(y_ref.at[at], y_ref.at[at], y_s.at[a, j], y_r.at[a, j], tp=1 - tp)

    def scores(a, h, q0, q1, slot):
        at = slice(a * rh, (a + 1) * rh)
        q = jnp.concatenate([qs[q0, h, at], qs[q1, h, at]], axis=0)
        s = _dot(q, kt[h], NT)
        sb[slot] = s
        mb[slot] = jnp.broadcast_to(jnp.max(s, axis=1, keepdims=True) * scale, (rows, d))

    def weigh(h, slot, dst0, dst1):
        m = mb[slot]
        es, l = [], None
        for k in range(0, n_pos, d):
            e = jnp.exp2(sb[slot, :, k:k + d] * scale - m)
            l = e if l is None else l + e
            es.append(e.astype(BF16))
        l = jnp.sum(l, axis=1, keepdims=True)
        o = _dot(jnp.concatenate(es, axis=1), vt[h]) / l
        lse = m + jnp.log2(l)
        dst0[h, 0], dst0[h, 1] = o[:rh], lse[:rh]
        dst1[h, 0], dst1[h, 1] = o[rh:], lse[rh:]

    def attend(a, i, q0, q1, dst0, dst1):
        for u in range(group):
            h = i * group + u
            scores(a, jnp.minimum(h + 1, heads - 1), q0, q1, (u + 1) % 4)
            weigh(h, u % 4, dst0, dst1)

    def merge_far(a, i):
        d_copy(a, i).wait_recv()
        for u in range(group):
            h = i * group + u
            l0, l1 = fo[h, 1], dr[a, h, 1]
            m = jnp.maximum(l0, l1)
            w0, w1 = jnp.exp2(l0 - m), jnp.exp2(l1 - m)
            t = w0 + w1
            xs[a, h] = ((w0 * fo[h, 0] + w1 * dr[a, h, 0]) / t).astype(BF16)
            xl[a] = jnp.where(lane == h, m + jnp.log2(t), xl[a])
        x_copy(a, i).start()

    def add_peer(a):
        for j in range(blocks):
            p_copy(a, j).wait_recv()
            y = (keep[a, j] + pr[a, j].astype(F32)).astype(BF16)
            y_ref[a * rh:(a + 1) * rh, pl.ds(pl.multiple_of(tp * half + j * wide, wide), wide)] = y
            y_copy(a, j).start()

    xl[...] = jnp.zeros_like(xl)
    q_cp[0].wait()
    q_cp[1].wait()
    q_diag.wait_recv()
    for a in range(2):
        def far_step(i, c):
            attend(a, i, 3, 2, ds.at[a], fo)
            d_copy(a, i).start()

            @pl.when(i > 0)
            def _():
                merge_far(a, i - 1)
            return c
        scores(a, 0, 3, 2, 0)
        lax.fori_loop(0, steps, far_step, 0)

        def near_step(i, c):
            attend(a, i, 1, 0, ns.at[a], mo)
            n_copy(a, i).start()

            @pl.when(i == 0)
            def _():
                merge_far(a, steps - 1)
                l_copy(a).start()
                if a == 1:
                    add_peer(0)
            return c
        scores(a, 0, 1, 0, 0)
        lax.fori_loop(0, steps, near_step, 0)

        if a == 0:
            suf_cp.wait()
            x_cp.wait()
        at = slice(a * rh, (a + 1) * rh)
        l_copy(a).wait_recv()
        far_lse, suf_lse = xlr[a], suf[heads, at]
        for h in range(heads):
            if h % group == 0:
                n_copy(a, h // group).wait_recv()
                x_copy(a, h // group).wait_recv()
            ls = [mo[h, 1], nr[a, h, 1], jnp.broadcast_to(far_lse[:, h:h + 1], (rh, d)),
                  jnp.broadcast_to(suf_lse[:, h:h + 1], (rh, d))]
            m = functools.reduce(jnp.maximum, ls)
            ws = [jnp.exp2(l - m) for l in ls]
            o = ws[0] * mo[h, 0] + ws[1] * nr[a, h, 0] + ws[2] * xr[a, h].astype(F32) + ws[3] * suf[h, at]
            att[:, h * d:(h + 1) * d] = (o / functools.reduce(jnp.add, ws)).astype(BF16)
        if a == 0:
            for c in w_cp:
                c.wait()

        def send_block(j, c):
            cols_at = pl.ds(pl.multiple_of((1 - tp) * half + j * wide, wide), wide)
            ps[a, j] = _dot(att[...], wo[:, cols_at]).astype(BF16)
            p_copy(a, j).start()
            return c
        lax.fori_loop(0, blocks, send_block, 0)

        def keep_block(j, c):
            cols_at = pl.ds(pl.multiple_of(tp * half + j * wide, wide), wide)
            keep[a, j] = _dot(att[...], wo[:, cols_at]) + x_ref[at, cols_at].astype(F32)
            return c
        lax.fori_loop(0, blocks, keep_block, 0)

    add_peer(1)
    outs = [pltpu.make_async_copy(y_ref.at[pl.ds(a * rh, rh)], y_hbm.at[pl.ds(a * rh, rh)], osem.at[a]) for a in range(2)]
    for a in range(2):
        for j in range(blocks):
            y_copy(a, j).wait_recv()
        outs[a].start()
    q_diag.wait_send()
    for a in range(2):
        for j in range(blocks):
            y_copy(a, j).wait_send()
            p_copy(a, j).wait_send()
        for i in range(steps):
            d_copy(a, i).wait_send()
            n_copy(a, i).wait_send()
            x_copy(a, i).wait_send()
        l_copy(a).wait_send()
        outs[a].wait()


def _back(q, kp, vp, suf, x, w_o, scale):
    _, heads, rows, d = q.shape
    n = kp.shape[0]
    depth, cols = w_o.shape
    dma = pltpu.SemaphoreType.DMA
    rh, wide, steps = rows // 2, 512, 4
    blocks = cols // 2 // wide
    return pl.pallas_call(
        functools.partial(_back_kernel, scale),
        in_specs=[pl.BlockSpec(memory_space=pl.ANY)] * 6,
        out_specs=pl.BlockSpec(memory_space=pl.ANY),
        out_shape=jax.ShapeDtypeStruct((rows, cols), BF16),
        scratch_shapes=[
            VM((rows, cols), BF16), VM((4, 2, 128, heads, d), BF16),
            VM((4, heads, rows, d), BF16), VM((heads, n, d), BF16), VM((heads, n, d), BF16), VM(suf.shape, F32), VM((rows, cols), BF16),
            VM(w_o.shape, BF16)]
        + [VM((2, heads, 2, rh, d), F32)] * 4 + [VM((heads, 2, rh, d), F32)] * 2
        + [VM((2, heads, rh, d), BF16)] * 2 + [VM((2, rh, d), F32)] * 2
        + [VM((rh, depth), BF16), VM((2, blocks, rh, wide), F32)] + [VM((2, blocks, rh, wide), BF16)] * 2
        + [VM((4, rows, n), F32), VM((4, rows, d), F32)]
        + [dma((5,)), dma((4, 2)), dma((4,)), dma((2,)), dma((1,)), dma((1,))]
        + [dma((2, steps))] * 4 + [dma((2, steps + 1))] * 2 + [dma((2, blocks))] * 4,
        compiler_params=pltpu.CompilerParams(vmem_limit_bytes=62 * 2**20, collective_id=1, has_side_effects=True),
        cost_estimate=_cost(5e10, 2 * depth * cols),
    )(q, kp, vp, suf, x, w_o)


def _suffix_kernel(scale, lens, q_hbm, kn_hbm, vn_hbm, k_hbm, v_hbm, o_ref,
                   new, newsem, items, qb, acc, m_s, l_s, kbuf, vbuf, sbuf, ksem, vsem):
    _, heads, rows, d = new.shape
    news = [pltpu.make_async_copy(src, new.at[j], newsem.at[j])
            for j, src in enumerate((q_hbm.at[0], kn_hbm, vn_hbm))]
    for c in news:
        c.start()
    per = k_hbm.shape[0] // rows
    wide = SLOTS * heads
    dummy = rows * per

    for g in range(BATCH):
        items[g] = dummy

    def listing(b, t):
        for j in range(per):
            items[BATCH + t + j] = b * per + j
        return t + (lens[b] + SLOTS - 1) // SLOTS
    total = lax.fori_loop(0, rows, listing, 0, unroll=4)
    for g in range(2 * BATCH):
        items[BATCH + total + g] = dummy
    batches = (total + BATCH - 1) // BATCH

    def fetch(i):
        slot = lax.rem(i, RING)
        for g in range(BATCH):
            it = jnp.minimum(items[BATCH + i * BATCH + g], dummy - 1)
            pltpu.make_async_copy(k_hbm.at[it], kbuf.at[slot, g], ksem.at[slot]).start()
            pltpu.make_async_copy(v_hbm.at[it], vbuf.at[slot, g], vsem.at[slot]).start()

    def prime(i, c):
        fetch(i)
        return c
    lax.fori_loop(0, jnp.minimum(batches, RING - 1), prime, 0)

    for c in news:
        c.wait()
    for c in range(rows // 16):
        q, kn, vn = [jnp.swapaxes(new[j, :, c * 16:c * 16 + 16, :], 0, 1) for j in range(3)]
        qb[c * 16:c * 16 + 16] = q
        s = jnp.sum(q.astype(F32) * kn.astype(F32), axis=-1, keepdims=True) * scale
        m_s[c * 16:c * 16 + 16] = jnp.broadcast_to(s, (16, heads, 128))
        l_s[c * 16:c * 16 + 16] = jnp.ones((16, heads, 128), F32)
        acc[c * 16:c * 16 + 16] = vn.astype(F32)

    row = lax.broadcasted_iota(jnp.int32, (heads, wide), 0)
    col = lax.broadcasted_iota(jnp.int32, (heads, wide), 1)
    slot_of = jnp.where(lax.rem(col, heads) == row, col // heads, 1 << 20)

    def step(i, c):
        slot = lax.rem(i, RING)
        last = lax.rem(i + RING - 1, RING)
        par = lax.rem(i, 2)

        @pl.when(i < batches)
        def _():
            pltpu.make_async_copy(k_hbm.at[pl.ds(0, BATCH)], kbuf.at[slot], ksem.at[slot]).wait()

        @pl.when(i > 0)
        def _():
            pltpu.make_async_copy(v_hbm.at[pl.ds(0, BATCH)], vbuf.at[last], vsem.at[last]).wait()

        for g in range(BATCH):
            it = items[BATCH + i * BATCH + g]
            b = it // per
            left = lens[jnp.minimum(b, rows - 1)] - lax.rem(it, per) * SLOTS
            s = _dot(qb[b], kbuf[slot, g], NT) * scale
            sbuf[par, g] = jnp.where(slot_of < left, s, -jnp.inf)

        parts = []
        for g in range(0, BATCH, 2):
            ps = []
            for u in range(2):
                s = sbuf[1 - par, g + u]
                m = jnp.max(s, axis=1, keepdims=True)
                p = jnp.exp2(s - m)
                parts.append([m, jnp.sum(p, axis=1, keepdims=True), None])
                ps.append(p.astype(BF16))
            o = _dot(jnp.concatenate(ps, axis=0),
                     jnp.concatenate([vbuf[last, g], vbuf[last, g + 1]], axis=1))
            parts[g][2] = o[:heads, :d]
            parts[g + 1][2] = o[heads:, d:]
        for g in range(BATCH):
            b = items[i * BATCH + g] // per
            m, l, o = parts[g]
            m_old = m_s[b]
            m_new = jnp.maximum(m_old, m)
            w_old = jnp.exp2(m_old - m_new)
            w = jnp.exp2(m - m_new)
            m_s[b] = m_new
            l_s[b] = l_s[b] * w_old + l * w
            acc[b] = acc[b] * w_old + o * w

        @pl.when(i + RING - 1 < batches)
        def _():
            fetch(i + RING - 1)
        return c

    lax.fori_loop(0, batches + 1, step, 0)

    lane = lax.broadcasted_iota(jnp.int32, (16, 128), 1)
    for c in range(rows // 16):
        l = l_s[c * 16:c * 16 + 16]
        o = acc[c * 16:c * 16 + 16] / l
        lse = m_s[c * 16:c * 16 + 16] + jnp.log2(l)
        o_ref[:heads, c * 16:c * 16 + 16, :] = jnp.swapaxes(o, 0, 1)
        lse = jnp.swapaxes(lse, 0, 1)
        out = jnp.zeros((16, 128), F32)
        for h in range(heads):
            out = jnp.where(lane == h, lse[h], out)
        o_ref[heads, c * 16:c * 16 + 16, :] = out


def _suffix(lens, q, kn, vn, k, v, scale):
    _, heads, rows, d = q.shape
    slots = k.shape[1]
    per = slots // SLOTS
    wide = SLOTS * heads
    k = k.reshape(rows * per, wide, d)
    v = v.reshape(rows * per, wide, d)
    return pl.pallas_call(
        functools.partial(_suffix_kernel, scale),
        in_specs=[pl.BlockSpec(memory_space=pltpu.SMEM)] + [pl.BlockSpec(memory_space=pl.ANY)] * 5,
        out_specs=pl.BlockSpec(memory_space=VM),
        out_shape=jax.ShapeDtypeStruct((heads + 1, rows, d), F32),
        scratch_shapes=[
            VM((3, heads, rows, d), BF16),
            pltpu.SemaphoreType.DMA((3,)),
            pltpu.SMEM((rows * per + 4 * BATCH,), jnp.int32),
            VM((rows + 1, heads, d), BF16),
            VM((rows + 1, heads, d), F32),
            VM((rows + 1, heads, 128), F32),
            VM((rows + 1, heads, 128), F32),
            VM((RING, BATCH, wide, d), BF16),
            VM((RING, BATCH, wide, d), BF16),
            VM((2, BATCH, heads, wide), F32),
            pltpu.SemaphoreType.DMA((RING,)),
            pltpu.SemaphoreType.DMA((RING,)),
        ],
        compiler_params=pltpu.CompilerParams(vmem_limit_bytes=LIMIT),
        cost_estimate=_cost(2e10, 4 * k.size),
    )(lens, q, kn, vn, k, v)


def solution(mesh):
    row_axes = ('dp', 'ctx')
    def device_step(hidden, w_q, w_k, w_v, w_o, k_prefix, v_prefix, k_suffix, v_suffix, seq_lens):
        scale = LOG2E * k_prefix.shape[2] ** -0.5
        q, kn, vn = _front(hidden, w_q, w_k, w_v, k_prefix.shape[2])
        suf = _suffix(seq_lens, q, kn, vn, k_suffix, v_suffix, scale)
        return _back(q, k_prefix, v_prefix, suf, hidden, w_o, scale)

    spec_in = (P(row_axes, None), P(None, 'tp'), P(None, 'tp'), P(None, 'tp'), P('tp', None),
               P(row_axes, 'tp', None), P(row_axes, 'tp', None), P(row_axes, None, 'tp', None),
               P(row_axes, None, 'tp', None), P(row_axes))
    return jax.shard_map(device_step, mesh=mesh, in_specs=spec_in, out_specs=P(row_axes, None), check_vma=False)
```

```python
import functools

import jax
import jax.numpy as jnp
from jax import lax
from jax.experimental import pallas as pl
from jax.experimental.pallas import tpu as pltpu
from jax.sharding import PartitionSpec as P

F32 = jnp.float32
BF16 = jnp.bfloat16
VM = pltpu.VMEM
LOG2E = 1.4426950408889634
BATCH = 16
SLOTS = 16
RING = 5
CHUNK = 512
RINGW = 6
LIMIT = 56 * 2**20


def _cost(flops, nbytes):
    return pl.CostEstimate(flops=int(flops), bytes_accessed=int(nbytes), transcendentals=0)


def _dot(a, b, dims=(((1,), (0,)), ((), ()))):
    return lax.dot_general(a, b, dims, preferred_element_type=F32)


NT = (((1,), (1,)), ((), ()))


MESH = pl.DeviceIdType.MESH


def _stream(x_ref, ws, bufs, sem, acc, emit, extra_start=None, extra_body=None):
    ring, chunk, _ = bufs.shape
    n = ws[0].shape[0] // chunk
    total = n * len(ws)
    part = 512

    def start(g):
        slot = lax.rem(g, ring)
        for i, w in enumerate(ws):
            @pl.when((g >= i * n) & (g < (i + 1) * n))
            def _():
                at = pl.multiple_of((g - i * n) * chunk, chunk)
                pltpu.make_async_copy(w.at[pl.ds(at, chunk)], bufs.at[slot, :, :w.shape[1]], sem.at[slot]).start()
        if extra_start is not None:
            extra_start(g)

    def prime():
        def body(g, c):
            start(g)
            return c
        lax.fori_loop(0, min(ring, total), body, 0)

    def run():
        for i, w in enumerate(ws):
            cols = w.shape[1]
            acc[...] = jnp.zeros_like(acc)

            def body(c, carry):
                g = i * n + c
                slot = lax.rem(g, ring)
                pltpu.make_async_copy(w.at[pl.ds(0, chunk)], bufs.at[slot, :, :cols], sem.at[slot]).wait()
                x = x_ref[:, pl.ds(pl.multiple_of(c * chunk, chunk), chunk)]
                for j in range(0, cols, part):
                    acc[:, j:j + part] += _dot(x, bufs[slot, :, j:j + part])
                if extra_body is not None:
                    extra_body(i, g)
                start(g + ring)
                return carry
            lax.fori_loop(0, n, body, 0)
            emit(i)
    return prime, run


def _peers():
    me = lax.axis_index('ctx')
    return me + 1 - 2 * lax.rem(me, 2), me + 2 - 4 * (me // 2)


def _remote(src, dst, s, r, **to):
    return pltpu.make_async_remote_copy(src_ref=src, dst_ref=dst, send_sem=s, recv_sem=r,
                                        device_id=to, device_id_type=MESH)


def _front_kernel(x_hbm, wq_hbm, wk_hbm, wv_hbm, q_hbm, kn_hbm, vn_hbm,
                  x_ref, bufs, acc, qs, kvn, xsem, sem, osem, q_s, q_r):
    _, heads, _, d = qs.shape
    near, far = _peers()
    cp = pltpu.make_async_copy(x_hbm, x_ref, xsem)
    cp.start()
    hh = heads // 2
    half = [pl.ds(j * hh, hh) for j in range(2)]
    q_near = [_remote(qs.at[0, at], qs.at[1, at], q_s.at[0, j], q_r.at[0, j], ctx=near) for j, at in enumerate(half)]
    q_far = [_remote(qs.at[0, at], qs.at[2, at], q_s.at[1, j], q_r.at[1, j], ctx=far) for j, at in enumerate(half)]
    outs = [pltpu.make_async_copy(qs.at[0], q_hbm.at[0], osem.at[0]),
            pltpu.make_async_copy(kvn.at[0], kn_hbm, osem.at[1]),
            pltpu.make_async_copy(kvn.at[1], vn_hbm, osem.at[2])]
    rest = [pltpu.make_async_copy(qs.at[j], q_hbm.at[j], osem.at[2 + j]) for j in (1, 2)]

    def emit(i):
        if i < 2:
            for h in range(hh):
                qs[0, i * hh + h] = acc[:, h * d:(h + 1) * d].astype(BF16)
            if i == 0:
                pl.semaphore_wait(barrier, 2)
            q_far[i].start()
            q_near[i].start()
        else:
            for h in range(heads):
                kvn[i - 2, h] = acc[:, h * d:(h + 1) * d].astype(BF16)
        if i > 0:
            outs[i - 1].start()

    wq_half = [wq_hbm.at[:, pl.ds(j * hh * d, hh * d)] for j in range(2)]
    prime, run = _stream(x_ref, wq_half + [wk_hbm, wv_hbm], bufs, sem, acc, emit)
    prime()
    barrier = pltpu.get_barrier_semaphore()
    for to in (near, far):
        pl.semaphore_signal(barrier, inc=1, device_id={'ctx': to}, device_id_type=MESH)
    cp.wait()
    run()
    for cs, r in zip((q_near, q_far), rest):
        for c in cs:
            c.wait_recv()
        r.start()
    for c in outs + rest:
        c.wait()
    for c in q_near + q_far:
        c.wait_send()


def _front(x, wq, wk, wv, d):
    rows, depth = x.shape
    cols = wq.shape[1]
    dma = pltpu.SemaphoreType.DMA
    blk = (cols // d, rows, d)
    return pl.pallas_call(
        _front_kernel,
        in_specs=[pl.BlockSpec(memory_space=pl.ANY)] * 4,
        out_specs=[pl.BlockSpec(memory_space=pl.ANY)] * 3,
        out_shape=[jax.ShapeDtypeStruct((3,) + blk, BF16)] + [jax.ShapeDtypeStruct(blk, BF16)] * 2,
        scratch_shapes=[
            VM((rows, depth), BF16), VM((RINGW, CHUNK, cols), BF16), VM((rows, cols), F32),
            VM((3,) + blk, BF16), VM((2,) + blk, BF16),
            dma, dma((RINGW,)), dma((5,)), dma((2, 2)), dma((2, 2))],
        compiler_params=pltpu.CompilerParams(vmem_limit_bytes=LIMIT, collective_id=0, has_side_effects=True),
        cost_estimate=_cost(2e10, 6 * depth * cols),
    )(x, wq, wk, wv)


def _back_kernel(scale, q_hbm, kp_hbm, vp_hbm, suf_hbm, x_hbm, w_hbm, mine_hbm, other_hbm,
                 mine, other, raw, qs, kt, vt, suf, x_ref, wo, ds, dr, ns, nr, fo, mo, xs, xr, xl, xlr, att, keep, ps, pr, sb, mb,
                 qsem, ksem, wsem, osem, q_s, q_r, d_s, d_r, n_s, n_r, x_s, x_r, p_s, p_r, y_s, y_r):
    heads, n_pos, d = kt.shape
    rows = x_ref.shape[0]
    rh = rows // 2
    half = x_ref.shape[1] // 2
    near, far = _peers()
    tp = lax.axis_index('tp')
    steps = 4
    group = heads // steps
    wide = ps.shape[-1]
    blocks = half // wide

    barrier = pltpu.get_barrier_semaphore()
    for to in ({'ctx': near}, {'ctx': far}, {'tp': 1 - tp}):
        pl.semaphore_signal(barrier, inc=1, device_id=to, device_id_type=MESH)
    ring, _, pos = raw.shape[:3]
    q_cp = [pltpu.make_async_copy(q_hbm.at[j], qs.at[j], qsem.at[2 + j]) for j in range(3)]
    q_cp[2].start()

    def piece(g):
        slot = lax.rem(g, ring)
        return [pltpu.make_async_copy(src.at[pl.ds(g * pos, pos)], raw.at[slot, j], ksem.at[slot, j])
                for j, src in enumerate((kp_hbm, vp_hbm))]
    for g in range(ring):
        for c in piece(g):
            c.start()
    q_cp[0].start()
    q_cp[1].start()
    suf_cp = pltpu.make_async_copy(suf_hbm, suf, qsem.at[0])
    x_cp = pltpu.make_async_copy(x_hbm, x_ref, qsem.at[1])
    wr = w_hbm.shape[0] // 4
    w_cp = [pltpu.make_async_copy(w_hbm.at[pl.ds(i * wr, wr)], wo.at[pl.ds(i * wr, wr)], wsem.at[i]) for i in range(4)]
    q_diag = _remote(qs.at[2], qs.at[3], q_s.at[0], q_r.at[0], ctx=near)
    q_cp[2].wait()
    pl.semaphore_wait(barrier, 3)
    q_diag.start()

    def relayout(g, c):
        slot = lax.rem(g, ring)
        for cp in piece(g):
            cp.wait()
        for j, dst in enumerate((kt, vt)):
            for u in range(pos // 16):
                to = pl.multiple_of(g * pos + u * 16, 16)
                dst[:, pl.ds(to, 16), :] = jnp.swapaxes(raw[slot, j, u * 16:u * 16 + 16], 0, 1)

        @pl.when(g + ring < n_pos // pos)
        def _():
            for cp in piece(g + ring):
                cp.start()
        return c
    lax.fori_loop(0, n_pos // pos, relayout, 0)
    for c in [suf_cp, x_cp] + w_cp:
        c.start()

    lane = lax.broadcasted_iota(jnp.int32, (rh, d), 1)

    def d_copy(a, i):
        at = pl.ds(i * group, group)
        return _remote(ds.at[a, at], dr.at[a, at], d_s.at[a, i], d_r.at[a, i], ctx=near)

    def n_copy(a, i):
        at = pl.ds(i * group, group)
        return _remote(ns.at[a, at], nr.at[a, at], n_s.at[a, i], n_r.at[a, i], ctx=near)

    def x_copy(a, i):
        at = pl.ds(i * group, group)
        return _remote(xs.at[a, at], xr.at[a, at], x_s.at[a, i], x_r.at[a, i], ctx=far)

    def l_copy(a):
        return _remote(xl.at[a], xlr.at[a], x_s.at[a, steps], x_r.at[a, steps], ctx=far)

    def p_copy(a, j):
        return _remote(ps.at[a, j], pr.at[a, j], p_s.at[a, j], p_r.at[a, j], tp=1 - tp)

    def y_copy(a, j):
        at = (pl.ds(a * rh, rh), pl.ds(j * wide, wide))
        return _remote(mine.at[at], other.at[at], y_s.at[a, j], y_r.at[a, j], tp=1 - tp)

    def scores(a, h, q0, q1, slot):
        at = slice(a * rh, (a + 1) * rh)
        q = jnp.concatenate([qs[q0, h, at], qs[q1, h, at]], axis=0)
        s = _dot(q, kt[h], NT)
        sb[slot] = s
        mb[slot] = jnp.broadcast_to(jnp.max(s, axis=1, keepdims=True) * scale, (rows, d))

    def weigh(h, slot, dst0, dst1):
        m = mb[slot]
        es, l = [], None
        for k in range(0, n_pos, d):
            e = jnp.exp2(sb[slot, :, k:k + d] * scale - m)
            l = e if l is None else l + e
            es.append(e.astype(BF16))
        l = jnp.sum(l, axis=1, keepdims=True)
        o = _dot(jnp.concatenate(es, axis=1), vt[h]) / l
        lse = m + jnp.log2(l)
        dst0[h, 0], dst0[h, 1] = o[:rh], lse[:rh]
        dst1[h, 0], dst1[h, 1] = o[rh:], lse[rh:]

    def attend(a, i, q0, q1, dst0, dst1):
        for u in range(group):
            h = i * group + u
            scores(a, jnp.minimum(h + 1, heads - 1), q0, q1, (u + 1) % 4)
            weigh(h, u % 4, dst0, dst1)

    def merge_far(a, i):
        d_copy(a, i).wait_recv()
        for u in range(group):
            h = i * group + u
            l0, l1 = fo[h, 1], dr[a, h, 1]
            m = jnp.maximum(l0, l1)
            w0, w1 = jnp.exp2(l0 - m), jnp.exp2(l1 - m)
            t = w0 + w1
            xs[a, h] = ((w0 * fo[h, 0] + w1 * dr[a, h, 0]) / t).astype(BF16)
            xl[a] = jnp.where(lane == h, m + jnp.log2(t), xl[a])
        x_copy(a, i).start()

    def add_peer(a):
        for j in range(blocks):
            p_copy(a, j).wait_recv()
            y = (keep[a, j] + pr[a, j].astype(F32)).astype(BF16)
            mine[a * rh:(a + 1) * rh, j * wide:(j + 1) * wide] = y
            y_copy(a, j).start()

    xl[...] = jnp.zeros_like(xl)
    q_cp[0].wait()
    q_cp[1].wait()
    q_diag.wait_recv()
    for a in range(2):
        def far_step(i, c):
            attend(a, i, 3, 2, ds.at[a], fo)
            d_copy(a, i).start()

            @pl.when(i > 0)
            def _():
                merge_far(a, i - 1)
            return c
        scores(a, 0, 3, 2, 0)
        lax.fori_loop(0, steps, far_step, 0)

        def near_step(i, c):
            attend(a, i, 1, 0, ns.at[a], mo)
            n_copy(a, i).start()

            @pl.when(i == 0)
            def _():
                merge_far(a, steps - 1)
                l_copy(a).start()
                if a == 1:
                    add_peer(0)
            return c
        scores(a, 0, 1, 0, 0)
        lax.fori_loop(0, steps, near_step, 0)

        if a == 0:
            suf_cp.wait()
            x_cp.wait()
        at = slice(a * rh, (a + 1) * rh)
        l_copy(a).wait_recv()
        far_lse, suf_lse = xlr[a], suf[heads, at]
        for h in range(heads):
            if h % group == 0:
                n_copy(a, h // group).wait_recv()
                x_copy(a, h // group).wait_recv()
            ls = [mo[h, 1], nr[a, h, 1], jnp.broadcast_to(far_lse[:, h:h + 1], (rh, d)),
                  jnp.broadcast_to(suf_lse[:, h:h + 1], (rh, d))]
            m = functools.reduce(jnp.maximum, ls)
            ws = [jnp.exp2(l - m) for l in ls]
            o = ws[0] * mo[h, 0] + ws[1] * nr[a, h, 0] + ws[2] * xr[a, h].astype(F32) + ws[3] * suf[h, at]
            att[:, h * d:(h + 1) * d] = (o / functools.reduce(jnp.add, ws)).astype(BF16)
        if a == 0:
            for c in w_cp:
                c.wait()

        def send_block(j, c):
            cols_at = pl.ds(pl.multiple_of((1 - tp) * half + j * wide, wide), wide)
            ps[a, j] = _dot(att[...], wo[:, cols_at]).astype(BF16)
            p_copy(a, j).start()
            return c
        lax.fori_loop(0, blocks, send_block, 0)

        def keep_block(j, c):
            cols_at = pl.ds(pl.multiple_of(tp * half + j * wide, wide), wide)
            keep[a, j] = _dot(att[...], wo[:, cols_at]) + x_ref[at, cols_at].astype(F32)
            return c
        lax.fori_loop(0, blocks, keep_block, 0)

    add_peer(1)
    outs = [pltpu.make_async_copy(mine, mine_hbm, osem.at[2])]
    outs[0].start()
    for a in range(2):
        for j in range(blocks):
            y_copy(a, j).wait_recv()
        at = pl.ds(a * rh, rh)
        outs.append(pltpu.make_async_copy(other.at[at], other_hbm.at[at], osem.at[a]))
        outs[-1].start()
    q_diag.wait_send()
    for a in range(2):
        for j in range(blocks):
            y_copy(a, j).wait_send()
            p_copy(a, j).wait_send()
        for i in range(steps):
            d_copy(a, i).wait_send()
            n_copy(a, i).wait_send()
            x_copy(a, i).wait_send()
        l_copy(a).wait_send()
    for c in outs:
        c.wait()


def _back(q, kp, vp, suf, x, w_o, scale):
    _, heads, rows, d = q.shape
    n = kp.shape[0]
    depth, cols = w_o.shape
    dma = pltpu.SemaphoreType.DMA
    rh, wide, steps = rows // 2, 512, 4
    blocks = cols // 2 // wide
    return pl.pallas_call(
        functools.partial(_back_kernel, scale),
        in_specs=[pl.BlockSpec(memory_space=pl.ANY)] * 6,
        out_specs=[pl.BlockSpec(memory_space=pl.ANY)] * 2,
        out_shape=[jax.ShapeDtypeStruct((rows, cols // 2), BF16)] * 2,
        scratch_shapes=[
            VM((rows, cols // 2), BF16), VM((rows, cols // 2), BF16), VM((4, 2, 128, heads, d), BF16),
            VM((4, heads, rows, d), BF16), VM((heads, n, d), BF16), VM((heads, n, d), BF16), VM(suf.shape, F32), VM((rows, cols), BF16),
            VM(w_o.shape, BF16)]
        + [VM((2, heads, 2, rh, d), F32)] * 4 + [VM((heads, 2, rh, d), F32)] * 2
        + [VM((2, heads, rh, d), BF16)] * 2 + [VM((2, rh, d), F32)] * 2
        + [VM((rh, depth), BF16), VM((2, blocks, rh, wide), F32)] + [VM((2, blocks, rh, wide), BF16)] * 2
        + [VM((4, rows, n), F32), VM((4, rows, d), F32)]
        + [dma((5,)), dma((4, 2)), dma((4,)), dma((3,)), dma((1,)), dma((1,))]
        + [dma((2, steps))] * 4 + [dma((2, steps + 1))] * 2 + [dma((2, blocks))] * 4,
        compiler_params=pltpu.CompilerParams(vmem_limit_bytes=62 * 2**20, collective_id=1, has_side_effects=True),
        cost_estimate=_cost(5e10, 2 * depth * cols),
    )(q, kp, vp, suf, x, w_o)


def _suffix_kernel(scale, lens, q_hbm, kn_hbm, vn_hbm, k_hbm, v_hbm, o_ref,
                   new, newsem, items, qb, acc, m_s, l_s, kbuf, vbuf, sbuf, ksem, vsem):
    _, heads, rows, d = new.shape
    news = [pltpu.make_async_copy(src, new.at[j], newsem.at[j])
            for j, src in enumerate((q_hbm.at[0], kn_hbm, vn_hbm))]
    for c in news:
        c.start()
    per = k_hbm.shape[0] // rows
    shift = per.bit_length() - 1
    wide = SLOTS * heads
    dummy = rows * per

    for g in range(BATCH):
        items[g] = dummy

    def listing(b, t):
        for j in range(per):
            items[BATCH + t + j] = b * per + j
        return t + (lens[b] + SLOTS - 1) // SLOTS
    total = lax.fori_loop(0, rows, listing, 0, unroll=4)
    for g in range(2 * BATCH):
        items[BATCH + total + g] = dummy
    batches = (total + BATCH - 1) // BATCH

    def fetch(i):
        slot = lax.rem(i, RING)
        for g in range(BATCH):
            it = jnp.minimum(items[BATCH + i * BATCH + g], dummy - 1)
            pltpu.make_async_copy(k_hbm.at[it], kbuf.at[slot, g], ksem.at[slot]).start()
            pltpu.make_async_copy(v_hbm.at[it], vbuf.at[slot, g], vsem.at[slot]).start()

    def prime(i, c):
        fetch(i)
        return c
    lax.fori_loop(0, jnp.minimum(batches, RING - 1), prime, 0)

    for c in news:
        c.wait()
    for c in range(rows // 16):
        q, kn, vn = [jnp.swapaxes(new[j, :, c * 16:c * 16 + 16, :], 0, 1) for j in range(3)]
        qb[c * 16:c * 16 + 16] = q
        s = jnp.sum(q.astype(F32) * kn.astype(F32), axis=-1, keepdims=True) * scale
        m_s[c * 16:c * 16 + 16] = jnp.broadcast_to(s, (16, heads, 128))
        l_s[c * 16:c * 16 + 16] = jnp.ones((16, heads, 128), F32)
        acc[c * 16:c * 16 + 16] = vn.astype(F32)

    row = lax.broadcasted_iota(jnp.int32, (heads, wide), 0)
    col = lax.broadcasted_iota(jnp.int32, (heads, wide), 1)
    slot_of = jnp.where(lax.rem(col, heads) == row, col // heads, 1 << 20)

    def step(i, c):
        slot = lax.rem(i, RING)
        last = lax.rem(i + RING - 1, RING)
        par = lax.rem(i, 2)

        @pl.when(i < batches)
        def _():
            pltpu.make_async_copy(k_hbm.at[pl.ds(0, BATCH)], kbuf.at[slot], ksem.at[slot]).wait()

        @pl.when(i > 0)
        def _():
            pltpu.make_async_copy(v_hbm.at[pl.ds(0, BATCH)], vbuf.at[last], vsem.at[last]).wait()

        for g in range(BATCH):
            it = items[BATCH + i * BATCH + g]
            b = lax.shift_right_logical(it, shift)
            left = lens[jnp.minimum(b, rows - 1)] - (it & (per - 1)) * SLOTS
            s = _dot(qb[b], kbuf[slot, g], NT) * scale
            sbuf[par, g] = jnp.where(slot_of < left, s, -jnp.inf)

        parts = []
        for g in range(0, BATCH, 2):
            ps = []
            for u in range(2):
                s = sbuf[1 - par, g + u]
                m = jnp.max(s, axis=1, keepdims=True)
                p = jnp.exp2(s - m)
                parts.append([m, jnp.sum(p, axis=1, keepdims=True), None])
                ps.append(p.astype(BF16))
            o = _dot(jnp.concatenate(ps, axis=0),
                     jnp.concatenate([vbuf[last, g], vbuf[last, g + 1]], axis=1))
            parts[g][2] = o[:heads, :d]
            parts[g + 1][2] = o[heads:, d:]
        for g in range(BATCH):
            b = lax.shift_right_logical(items[i * BATCH + g], shift)
            m, l, o = parts[g]
            m_old = m_s[b]
            m_new = jnp.maximum(m_old, m)
            w_old = jnp.exp2(m_old - m_new)
            w = jnp.exp2(m - m_new)
            m_s[b] = m_new
            l_s[b] = l_s[b] * w_old + l * w
            acc[b] = acc[b] * w_old + o * w

        @pl.when(i + RING - 1 < batches)
        def _():
            fetch(i + RING - 1)
        return c

    lax.fori_loop(0, batches + 1, step, 0)

    lane = lax.broadcasted_iota(jnp.int32, (16, 128), 1)
    for c in range(rows // 16):
        l = l_s[c * 16:c * 16 + 16]
        o = acc[c * 16:c * 16 + 16] / l
        lse = m_s[c * 16:c * 16 + 16] + jnp.log2(l)
        o_ref[:heads, c * 16:c * 16 + 16, :] = jnp.swapaxes(o, 0, 1)
        lse = jnp.swapaxes(lse, 0, 1)
        out = jnp.zeros((16, 128), F32)
        for h in range(heads):
            out = jnp.where(lane == h, lse[h], out)
        o_ref[heads, c * 16:c * 16 + 16, :] = out


def _suffix(lens, q, kn, vn, k, v, scale):
    _, heads, rows, d = q.shape
    slots = k.shape[1]
    per = slots // SLOTS
    wide = SLOTS * heads
    k = k.reshape(rows * per, wide, d)
    v = v.reshape(rows * per, wide, d)
    return pl.pallas_call(
        functools.partial(_suffix_kernel, scale),
        in_specs=[pl.BlockSpec(memory_space=pltpu.SMEM)] + [pl.BlockSpec(memory_space=pl.ANY)] * 5,
        out_specs=pl.BlockSpec(memory_space=VM),
        out_shape=jax.ShapeDtypeStruct((heads + 1, rows, d), F32),
        scratch_shapes=[
            VM((3, heads, rows, d), BF16),
            pltpu.SemaphoreType.DMA((3,)),
            pltpu.SMEM((rows * per + 4 * BATCH,), jnp.int32),
            VM((rows + 1, heads, d), BF16),
            VM((rows + 1, heads, d), F32),
            VM((rows + 1, heads, 128), F32),
            VM((rows + 1, heads, 128), F32),
            VM((RING, BATCH, wide, d), BF16),
            VM((RING, BATCH, wide, d), BF16),
            VM((2, BATCH, heads, wide), F32),
            pltpu.SemaphoreType.DMA((RING,)),
            pltpu.SemaphoreType.DMA((RING,)),
        ],
        compiler_params=pltpu.CompilerParams(vmem_limit_bytes=LIMIT),
        cost_estimate=_cost(2e10, 4 * k.size),
    )(lens, q, kn, vn, k, v)


def solution(mesh):
    row_axes = ('dp', 'ctx')
    def device_step(hidden, w_q, w_k, w_v, w_o, k_prefix, v_prefix, k_suffix, v_suffix, seq_lens):
        scale = LOG2E * k_prefix.shape[2] ** -0.5
        q, kn, vn = _front(hidden, w_q, w_k, w_v, k_prefix.shape[2])
        suf = _suffix(seq_lens, q, kn, vn, k_suffix, v_suffix, scale)
        mine, other = _back(q, k_prefix, v_prefix, suf, hidden, w_o, scale)
        return jnp.where(lax.axis_index('tp') == 0, jnp.concatenate([mine, other], axis=1),
                         jnp.concatenate([other, mine], axis=1))

    spec_in = (P(row_axes, None), P(None, 'tp'), P(None, 'tp'), P(None, 'tp'), P('tp', None),
               P(row_axes, 'tp', None), P(row_axes, 'tp', None), P(row_axes, None, 'tp', None),
               P(row_axes, None, 'tp', None), P(row_axes))
    return jax.shard_map(device_step, mesh=mesh, in_specs=spec_in, out_specs=P(row_axes, None), check_vma=False)
```

```python
import functools

import jax
import jax.numpy as jnp
from jax import lax
from jax.experimental import pallas as pl
from jax.experimental.pallas import tpu as pltpu
from jax.sharding import PartitionSpec as P

F32 = jnp.float32
BF16 = jnp.bfloat16
VM = pltpu.VMEM
LOG2E = 1.4426950408889634
BATCH = 16
SLOTS = 16
RING = 5
CHUNK = 512
RINGW = 6
LIMIT = 56 * 2**20


def _cost(flops, nbytes):
    return pl.CostEstimate(flops=int(flops), bytes_accessed=int(nbytes), transcendentals=0)


def _dot(a, b, dims=(((1,), (0,)), ((), ()))):
    return lax.dot_general(a, b, dims, preferred_element_type=F32)


NT = (((1,), (1,)), ((), ()))


MESH = pl.DeviceIdType.MESH


def _stream(x_ref, ws, bufs, sem, acc, emit, extra_start=None, extra_body=None):
    ring, chunk, _ = bufs.shape
    n = ws[0].shape[0] // chunk
    total = n * len(ws)
    part = 512

    def start(g):
        slot = lax.rem(g, ring)
        for i, w in enumerate(ws):
            @pl.when((g >= i * n) & (g < (i + 1) * n))
            def _():
                at = pl.multiple_of((g - i * n) * chunk, chunk)
                pltpu.make_async_copy(w.at[pl.ds(at, chunk)], bufs.at[slot, :, :w.shape[1]], sem.at[slot]).start()
        if extra_start is not None:
            extra_start(g)

    def prime():
        def body(g, c):
            start(g)
            return c
        lax.fori_loop(0, min(ring, total), body, 0)

    def run():
        for i, w in enumerate(ws):
            cols = w.shape[1]
            acc[...] = jnp.zeros_like(acc)

            def body(c, carry):
                g = i * n + c
                slot = lax.rem(g, ring)
                pltpu.make_async_copy(w.at[pl.ds(0, chunk)], bufs.at[slot, :, :cols], sem.at[slot]).wait()
                x = x_ref[:, pl.ds(pl.multiple_of(c * chunk, chunk), chunk)]
                for j in range(0, cols, part):
                    acc[:, j:j + part] += _dot(x, bufs[slot, :, j:j + part])
                if extra_body is not None:
                    extra_body(i, g)
                start(g + ring)
                return carry
            lax.fori_loop(0, n, body, 0)
            emit(i)
    return prime, run


def _peers():
    me = lax.axis_index('ctx')
    return me + 1 - 2 * lax.rem(me, 2), me + 2 - 4 * (me // 2)


def _remote(src, dst, s, r, **to):
    return pltpu.make_async_remote_copy(src_ref=src, dst_ref=dst, send_sem=s, recv_sem=r,
                                        device_id=to, device_id_type=MESH)


def _front_kernel(x_hbm, wq_hbm, wk_hbm, wv_hbm, q_hbm, kn_hbm, vn_hbm,
                  x_ref, bufs, acc, qs, kvn, xsem, sem, osem, q_s, q_r):
    _, heads, _, d = qs.shape
    near, far = _peers()
    cp = pltpu.make_async_copy(x_hbm, x_ref, xsem)
    cp.start()
    hh = heads // 2
    half = [pl.ds(j * hh, hh) for j in range(2)]
    q_near = [_remote(qs.at[0, at], qs.at[1, at], q_s.at[0, j], q_r.at[0, j], ctx=near) for j, at in enumerate(half)]
    q_far = [_remote(qs.at[0, at], qs.at[2, at], q_s.at[1, j], q_r.at[1, j], ctx=far) for j, at in enumerate(half)]
    outs = [pltpu.make_async_copy(qs.at[0], q_hbm.at[0], osem.at[0]),
            pltpu.make_async_copy(kvn.at[0], kn_hbm, osem.at[1]),
            pltpu.make_async_copy(kvn.at[1], vn_hbm, osem.at[2])]
    rest = [pltpu.make_async_copy(qs.at[j], q_hbm.at[j], osem.at[2 + j]) for j in (1, 2)]

    def emit(i):
        if i < 2:
            for h in range(hh):
                qs[0, i * hh + h] = acc[:, h * d:(h + 1) * d].astype(BF16)
            if i == 0:
                pl.semaphore_wait(barrier, 2)
            q_far[i].start()
            q_near[i].start()
        else:
            for h in range(heads):
                kvn[i - 2, h] = acc[:, h * d:(h + 1) * d].astype(BF16)
        if i > 0:
            outs[i - 1].start()

    wq_half = [wq_hbm.at[:, pl.ds(j * hh * d, hh * d)] for j in range(2)]
    prime, run = _stream(x_ref, wq_half + [wk_hbm, wv_hbm], bufs, sem, acc, emit)
    prime()
    barrier = pltpu.get_barrier_semaphore()
    for to in (near, far):
        pl.semaphore_signal(barrier, inc=1, device_id={'ctx': to}, device_id_type=MESH)
    cp.wait()
    run()
    for cs, r in zip((q_near, q_far), rest):
        for c in cs:
            c.wait_recv()
        r.start()
    for c in outs + rest:
        c.wait()
    for c in q_near + q_far:
        c.wait_send()


def _front(x, wq, wk, wv, d):
    rows, depth = x.shape
    cols = wq.shape[1]
    dma = pltpu.SemaphoreType.DMA
    blk = (cols // d, rows, d)
    return pl.pallas_call(
        _front_kernel,
        in_specs=[pl.BlockSpec(memory_space=pl.ANY)] * 4,
        out_specs=[pl.BlockSpec(memory_space=pl.ANY)] * 3,
        out_shape=[jax.ShapeDtypeStruct((3,) + blk, BF16)] + [jax.ShapeDtypeStruct(blk, BF16)] * 2,
        scratch_shapes=[
            VM((rows, depth), BF16), VM((RINGW, CHUNK, cols), BF16), VM((rows, cols), F32),
            VM((3,) + blk, BF16), VM((2,) + blk, BF16),
            dma, dma((RINGW,)), dma((5,)), dma((2, 2)), dma((2, 2))],
        compiler_params=pltpu.CompilerParams(vmem_limit_bytes=LIMIT, collective_id=0, has_side_effects=True),
        cost_estimate=_cost(2e10, 6 * depth * cols),
    )(x, wq, wk, wv)


def _back_kernel(scale, q_hbm, kp_hbm, vp_hbm, suf_hbm, x_hbm, w_hbm, y_hbm,
                 y_ref, raw, qs, kt, vt, suf, x_ref, wo, ds, dr, ns, nr, fo, mo, xs, xr, xl, xlr, att, keep, ps, pr, sb, mb,
                 qsem, ksem, wsem, osem, q_s, q_r, d_s, d_r, n_s, n_r, x_s, x_r, p_s, p_r, y_s, y_r):
    heads, n_pos, d = kt.shape
    rows = x_ref.shape[0]
    rh = rows // 2
    half = x_ref.shape[1] // 2
    near, far = _peers()
    tp = lax.axis_index('tp')
    steps = 4
    group = heads // steps
    wide = ps.shape[-1]
    blocks = half // wide

    barrier = pltpu.get_barrier_semaphore()
    for to in ({'ctx': near}, {'ctx': far}, {'tp': 1 - tp}):
        pl.semaphore_signal(barrier, inc=1, device_id=to, device_id_type=MESH)
    ring, _, pos = raw.shape[:3]
    q_cp = [pltpu.make_async_copy(q_hbm.at[j], qs.at[j], qsem.at[2 + j]) for j in range(3)]
    q_cp[2].start()

    def piece(g):
        slot = lax.rem(g, ring)
        return [pltpu.make_async_copy(src.at[pl.ds(g * pos, pos)], raw.at[slot, j], ksem.at[slot, j])
                for j, src in enumerate((kp_hbm, vp_hbm))]
    for g in range(ring):
        for c in piece(g):
            c.start()
    q_cp[0].start()
    q_cp[1].start()
    suf_cp = pltpu.make_async_copy(suf_hbm, suf, qsem.at[0])
    x_cp = pltpu.make_async_copy(x_hbm, x_ref, qsem.at[1])
    wr = w_hbm.shape[0] // 4
    w_cp = [pltpu.make_async_copy(w_hbm.at[pl.ds(i * wr, wr)], wo.at[pl.ds(i * wr, wr)], wsem.at[i]) for i in range(4)]
    q_diag = _remote(qs.at[2], qs.at[3], q_s.at[0], q_r.at[0], ctx=near)

    def relayout(g, c):
        slot = lax.rem(g, ring)
        for cp in piece(g):
            cp.wait()
        for j, dst in enumerate((kt, vt)):
            for u in range(pos // 16):
                to = pl.multiple_of(g * pos + u * 16, 16)
                dst[:, pl.ds(to, 16), :] = jnp.swapaxes(raw[slot, j, u * 16:u * 16 + 16], 0, 1)

        @pl.when(g + ring < n_pos // pos)
        def _():
            for cp in piece(g + ring):
                cp.start()
        return c
    lax.fori_loop(0, ring, relayout, 0)
    q_cp[2].wait()
    pl.semaphore_wait(barrier, 3)
    q_diag.start()
    lax.fori_loop(ring, n_pos // pos, relayout, 0)
    for c in [suf_cp, x_cp] + w_cp:
        c.start()

    lane = lax.broadcasted_iota(jnp.int32, (rh, d), 1)

    def d_copy(a, i):
        at = pl.ds(i * group, group)
        return _remote(ds.at[a, at], dr.at[a, at], d_s.at[a, i], d_r.at[a, i], ctx=near)

    def n_copy(a, i):
        at = pl.ds(i * group, group)
        return _remote(ns.at[a, at], nr.at[a, at], n_s.at[a, i], n_r.at[a, i], ctx=near)

    def x_copy(a, i):
        at = pl.ds(i * group, group)
        return _remote(xs.at[a, at], xr.at[a, at], x_s.at[a, i], x_r.at[a, i], ctx=far)

    def l_copy(a):
        return _remote(xl.at[a], xlr.at[a], x_s.at[a, steps], x_r.at[a, steps], ctx=far)

    def p_copy(a, j):
        return _remote(ps.at[a, j], pr.at[a, j], p_s.at[a, j], p_r.at[a, j], tp=1 - tp)

    def y_copy(a, j):
        at = (pl.ds(a * rh, rh), pl.ds(pl.multiple_of(tp * half + j * wide, wide), wide))
        return _remote(y_ref.at[at], y_ref.at[at], y_s.at[a, j], y_r.at[a, j], tp=1 - tp)

    def scores(a, h, q0, q1, slot):
        at = slice(a * rh, (a + 1) * rh)
        q = jnp.concatenate([qs[q0, h, at], qs[q1, h, at]], axis=0)
        s = _dot(q, kt[h], NT)
        sb[slot] = s
        mb[slot] = jnp.broadcast_to(jnp.max(s, axis=1, keepdims=True) * scale, (rows, d))

    def weigh(h, slot, dst0, dst1):
        m = mb[slot]
        es, l = [], None
        for k in range(0, n_pos, d):
            e = jnp.exp2(sb[slot, :, k:k + d] * scale - m)
            l = e if l is None else l + e
            es.append(e.astype(BF16))
        l = jnp.sum(l, axis=1, keepdims=True)
        o = _dot(jnp.concatenate(es, axis=1), vt[h]) / l
        lse = m + jnp.log2(l)
        dst0[h, 0], dst0[h, 1] = o[:rh], lse[:rh]
        dst1[h, 0], dst1[h, 1] = o[rh:], lse[rh:]

    def attend(a, i, q0, q1, dst0, dst1):
        for u in range(group):
            h = i * group + u
            scores(a, jnp.minimum(h + 1, heads - 1), q0, q1, (u + 1) % 4)
            weigh(h, u % 4, dst0, dst1)

    def merge_far(a, i):
        d_copy(a, i).wait_recv()
        for u in range(group):
            h = i * group + u
            l0, l1 = fo[h, 1], dr[a, h, 1]
            m = jnp.maximum(l0, l1)
            w0, w1 = jnp.exp2(l0 - m), jnp.exp2(l1 - m)
            t = w0 + w1
            xs[a, h] = ((w0 * fo[h, 0] + w1 * dr[a, h, 0]) / t).astype(BF16)
            xl[a] = jnp.where(lane == h, m + jnp.log2(t), xl[a])
        x_copy(a, i).start()

    def add_peer(a):
        for j in range(blocks):
            p_copy(a, j).wait_recv()
            y = (keep[a, j] + pr[a, j].astype(F32)).astype(BF16)
            y_ref[a * rh:(a + 1) * rh, pl.ds(pl.multiple_of(tp * half + j * wide, wide), wide)] = y
            y_copy(a, j).start()

    xl[...] = jnp.zeros_like(xl)
    q_cp[0].wait()
    q_cp[1].wait()
    q_diag.wait_recv()
    for a in range(2):
        def far_step(i, c):
            attend(a, i, 3, 2, ds.at[a], fo)
            d_copy(a, i).start()

            @pl.when(i > 0)
            def _():
                merge_far(a, i - 1)
            return c
        scores(a, 0, 3, 2, 0)
        lax.fori_loop(0, steps, far_step, 0)

        def near_step(i, c):
            attend(a, i, 1, 0, ns.at[a], mo)
            n_copy(a, i).start()

            @pl.when(i == 0)
            def _():
                merge_far(a, steps - 1)
                l_copy(a).start()
                if a == 1:
                    add_peer(0)
            return c
        scores(a, 0, 1, 0, 0)
        lax.fori_loop(0, steps, near_step, 0)

        if a == 0:
            suf_cp.wait()
            x_cp.wait()
        at = slice(a * rh, (a + 1) * rh)
        l_copy(a).wait_recv()
        far_lse, suf_lse = xlr[a], suf[heads, at]
        for h in range(heads):
            if h % group == 0:
                n_copy(a, h // group).wait_recv()
                x_copy(a, h // group).wait_recv()
            ls = [mo[h, 1], nr[a, h, 1], jnp.broadcast_to(far_lse[:, h:h + 1], (rh, d)),
                  jnp.broadcast_to(suf_lse[:, h:h + 1], (rh, d))]
            m = functools.reduce(jnp.maximum, ls)
            ws = [jnp.exp2(l - m) for l in ls]
            o = ws[0] * mo[h, 0] + ws[1] * nr[a, h, 0] + ws[2] * xr[a, h].astype(F32) + ws[3] * suf[h, at]
            att[:, h * d:(h + 1) * d] = (o / functools.reduce(jnp.add, ws)).astype(BF16)
        if a == 0:
            for c in w_cp:
                c.wait()

        def send_block(j, c):
            cols_at = pl.ds(pl.multiple_of((1 - tp) * half + j * wide, wide), wide)
            ps[a, j] = _dot(att[...], wo[:, cols_at]).astype(BF16)
            p_copy(a, j).start()
            return c
        lax.fori_loop(0, blocks, send_block, 0)

        def keep_block(j, c):
            cols_at = pl.ds(pl.multiple_of(tp * half + j * wide, wide), wide)
            keep[a, j] = _dot(att[...], wo[:, cols_at]) + x_ref[at, cols_at].astype(F32)
            return c
        lax.fori_loop(0, blocks, keep_block, 0)

    add_peer(1)
    outs = []
    for a in range(2):
        for j in range(blocks):
            y_copy(a, j).wait_recv()
        at = pl.ds(a * rh, rh)
        outs.append(pltpu.make_async_copy(y_ref.at[at], y_hbm.at[at], osem.at[a]))
        outs[-1].start()
    q_diag.wait_send()
    for a in range(2):
        for j in range(blocks):
            y_copy(a, j).wait_send()
            p_copy(a, j).wait_send()
        for i in range(steps):
            d_copy(a, i).wait_send()
            n_copy(a, i).wait_send()
            x_copy(a, i).wait_send()
        l_copy(a).wait_send()
    for c in outs:
        c.wait()


def _back(q, kp, vp, suf, x, w_o, scale):
    _, heads, rows, d = q.shape
    n = kp.shape[0]
    depth, cols = w_o.shape
    dma = pltpu.SemaphoreType.DMA
    rh, wide, steps = rows // 2, 512, 4
    blocks = cols // 2 // wide
    return pl.pallas_call(
        functools.partial(_back_kernel, scale),
        in_specs=[pl.BlockSpec(memory_space=pl.ANY)] * 6,
        out_specs=pl.BlockSpec(memory_space=pl.ANY),
        out_shape=jax.ShapeDtypeStruct((rows, cols), BF16),
        scratch_shapes=[
            VM((rows, cols), BF16), VM((4, 2, 128, heads, d), BF16),
            VM((4, heads, rows, d), BF16), VM((heads, n, d), BF16), VM((heads, n, d), BF16), VM(suf.shape, F32), VM((rows, cols), BF16),
            VM(w_o.shape, BF16)]
        + [VM((2, heads, 2, rh, d), F32)] * 4 + [VM((heads, 2, rh, d), F32)] * 2
        + [VM((2, heads, rh, d), BF16)] * 2 + [VM((2, rh, d), F32)] * 2
        + [VM((rh, depth), BF16), VM((2, blocks, rh, wide), F32)] + [VM((2, blocks, rh, wide), BF16)] * 2
        + [VM((4, rows, n), F32), VM((4, rows, d), F32)]
        + [dma((5,)), dma((4, 2)), dma((4,)), dma((2,)), dma((1,)), dma((1,))]
        + [dma((2, steps))] * 4 + [dma((2, steps + 1))] * 2 + [dma((2, blocks))] * 4,
        compiler_params=pltpu.CompilerParams(vmem_limit_bytes=62 * 2**20, collective_id=1, has_side_effects=True),
        cost_estimate=_cost(5e10, 2 * depth * cols),
    )(q, kp, vp, suf, x, w_o)


def _suffix_kernel(scale, lens, q_hbm, kn_hbm, vn_hbm, k_hbm, v_hbm, o_hbm,
                   o_ref, osem, new, newsem, items, qb, acc, m_s, l_s, kbuf, vbuf, sbuf, ksem, vsem):
    _, heads, rows, d = new.shape
    news = [pltpu.make_async_copy(src, new.at[j], newsem.at[j])
            for j, src in enumerate((q_hbm.at[0], kn_hbm, vn_hbm))]
    for c in news:
        c.start()
    per = k_hbm.shape[0] // rows
    shift = per.bit_length() - 1
    wide = SLOTS * heads
    dummy = rows * per

    for g in range(BATCH):
        items[g] = dummy

    def listing(b, t):
        for j in range(per):
            items[BATCH + t + j] = b * per + j
        return t + (lens[b] + SLOTS - 1) // SLOTS
    def fetch(i):
        slot = lax.rem(i, RING)
        for g in range(BATCH):
            it = jnp.minimum(items[BATCH + i * BATCH + g], dummy - 1)
            pltpu.make_async_copy(k_hbm.at[it], kbuf.at[slot, g], ksem.at[slot]).start()
            pltpu.make_async_copy(v_hbm.at[it], vbuf.at[slot, g], vsem.at[slot]).start()

    def prime(i, c):
        fetch(i)
        return c
    some = lax.fori_loop(0, rows // 4, listing, 0, unroll=4)
    early = jnp.minimum(some // BATCH, RING - 1)
    lax.fori_loop(0, early, prime, 0)
    total = lax.fori_loop(rows // 4, rows, listing, some, unroll=4)
    for g in range(2 * BATCH):
        items[BATCH + total + g] = dummy
    batches = (total + BATCH - 1) // BATCH
    lax.fori_loop(early, jnp.minimum(batches, RING - 1), prime, 0)

    for c in news:
        c.wait()
    for c in range(rows // 16):
        q, kn, vn = [jnp.swapaxes(new[j, :, c * 16:c * 16 + 16, :], 0, 1) for j in range(3)]
        qb[c * 16:c * 16 + 16] = q
        s = jnp.sum(q.astype(F32) * kn.astype(F32), axis=-1, keepdims=True) * scale
        m_s[c * 16:c * 16 + 16] = jnp.broadcast_to(s, (16, heads, 128))
        l_s[c * 16:c * 16 + 16] = jnp.ones((16, heads, 128), F32)
        acc[c * 16:c * 16 + 16] = vn.astype(F32)

    row = lax.broadcasted_iota(jnp.int32, (heads, wide), 0)
    col = lax.broadcasted_iota(jnp.int32, (heads, wide), 1)
    slot_of = jnp.where(lax.rem(col, heads) == row, col // heads, 1 << 20)

    def step(i, c):
        slot = lax.rem(i, RING)
        last = lax.rem(i + RING - 1, RING)
        par = lax.rem(i, 2)

        @pl.when(i < batches)
        def _():
            pltpu.make_async_copy(k_hbm.at[pl.ds(0, BATCH)], kbuf.at[slot], ksem.at[slot]).wait()

        @pl.when(i > 0)
        def _():
            pltpu.make_async_copy(v_hbm.at[pl.ds(0, BATCH)], vbuf.at[last], vsem.at[last]).wait()

        for g in range(BATCH):
            it = items[BATCH + i * BATCH + g]
            b = lax.shift_right_logical(it, shift)
            left = lens[jnp.minimum(b, rows - 1)] - (it & (per - 1)) * SLOTS
            s = _dot(qb[b], kbuf[slot, g], NT) * scale
            sbuf[par, g] = jnp.where(slot_of < left, s, -jnp.inf)

        parts = []
        for g in range(0, BATCH, 2):
            ps = []
            for u in range(2):
                s = sbuf[1 - par, g + u]
                m = jnp.max(s, axis=1, keepdims=True)
                p = jnp.exp2(s - m)
                parts.append([m, jnp.sum(p, axis=1, keepdims=True), None])
                ps.append(p.astype(BF16))
            o = _dot(jnp.concatenate(ps, axis=0),
                     jnp.concatenate([vbuf[last, g], vbuf[last, g + 1]], axis=1))
            parts[g][2] = o[:heads, :d]
            parts[g + 1][2] = o[heads:, d:]
        for g in range(BATCH):
            b = lax.shift_right_logical(items[i * BATCH + g], shift)
            m, l, o = parts[g]
            m_old = m_s[b]
            m_new = jnp.maximum(m_old, m)
            w_old = jnp.exp2(m_old - m_new)
            w = jnp.exp2(m - m_new)
            m_s[b] = m_new
            l_s[b] = l_s[b] * w_old + l * w
            acc[b] = acc[b] * w_old + o * w

        @pl.when(i + RING - 1 < batches)
        def _():
            fetch(i + RING - 1)
        return c

    lax.fori_loop(0, batches + 1, step, 0)

    def leave(c):
        at = pl.ds(c * 16, 16)
        return pltpu.make_async_copy(o_ref.at[:, at], o_hbm.at[:, at], osem.at[c])

    lane = lax.broadcasted_iota(jnp.int32, (16, 128), 1)
    for c in range(rows // 16):
        l = l_s[c * 16:c * 16 + 16]
        o = acc[c * 16:c * 16 + 16] / l
        lse = m_s[c * 16:c * 16 + 16] + jnp.log2(l)
        o_ref[:heads, c * 16:c * 16 + 16, :] = jnp.swapaxes(o, 0, 1)
        lse = jnp.swapaxes(lse, 0, 1)
        out = jnp.zeros((16, 128), F32)
        for h in range(heads):
            out = jnp.where(lane == h, lse[h], out)
        o_ref[heads, c * 16:c * 16 + 16, :] = out
        leave(c).start()
    for c in range(rows // 16):
        leave(c).wait()


def _suffix(lens, q, kn, vn, k, v, scale):
    _, heads, rows, d = q.shape
    slots = k.shape[1]
    per = slots // SLOTS
    wide = SLOTS * heads
    k = k.reshape(rows * per, wide, d)
    v = v.reshape(rows * per, wide, d)
    return pl.pallas_call(
        functools.partial(_suffix_kernel, scale),
        in_specs=[pl.BlockSpec(memory_space=pltpu.SMEM)] + [pl.BlockSpec(memory_space=pl.ANY)] * 5,
        out_specs=pl.BlockSpec(memory_space=pl.ANY),
        out_shape=jax.ShapeDtypeStruct((heads + 1, rows, d), F32),
        scratch_shapes=[
            VM((heads + 1, rows, d), F32),
            pltpu.SemaphoreType.DMA((rows // 16,)),
            VM((3, heads, rows, d), BF16),
            pltpu.SemaphoreType.DMA((3,)),
            pltpu.SMEM((rows * per + 4 * BATCH,), jnp.int32),
            VM((rows + 1, heads, d), BF16),
            VM((rows + 1, heads, d), F32),
            VM((rows + 1, heads, 128), F32),
            VM((rows + 1, heads, 128), F32),
            VM((RING, BATCH, wide, d), BF16),
            VM((RING, BATCH, wide, d), BF16),
            VM((2, BATCH, heads, wide), F32),
            pltpu.SemaphoreType.DMA((RING,)),
            pltpu.SemaphoreType.DMA((RING,)),
        ],
        compiler_params=pltpu.CompilerParams(vmem_limit_bytes=LIMIT),
        cost_estimate=_cost(2e10, 4 * k.size),
    )(lens, q, kn, vn, k, v)


def solution(mesh):
    row_axes = ('dp', 'ctx')
    def device_step(hidden, w_q, w_k, w_v, w_o, k_prefix, v_prefix, k_suffix, v_suffix, seq_lens):
        scale = LOG2E * k_prefix.shape[2] ** -0.5
        q, kn, vn = _front(hidden, w_q, w_k, w_v, k_prefix.shape[2])
        suf = _suffix(seq_lens, q, kn, vn, k_suffix, v_suffix, scale)
        return _back(q, k_prefix, v_prefix, suf, hidden, w_o, scale)

    spec_in = (P(row_axes, None), P(None, 'tp'), P(None, 'tp'), P(None, 'tp'), P('tp', None),
               P(row_axes, 'tp', None), P(row_axes, 'tp', None), P(row_axes, None, 'tp', None),
               P(row_axes, None, 'tp', None), P(row_axes))
    return jax.shard_map(device_step, mesh=mesh, in_specs=spec_in, out_specs=P(row_axes, None), check_vma=False)
```

```python
import functools

import jax
import jax.numpy as jnp
from jax import lax
from jax.experimental import pallas as pl
from jax.experimental.pallas import tpu as pltpu
from jax.sharding import PartitionSpec as P

F32 = jnp.float32
BF16 = jnp.bfloat16
VM = pltpu.VMEM
LOG2E = 1.4426950408889634
BATCH = 16
SLOTS = 16
RING = 5
CHUNK = 512
RINGW = 6
LIMIT = 56 * 2**20


def _cost(flops, nbytes):
    return pl.CostEstimate(flops=int(flops), bytes_accessed=int(nbytes), transcendentals=0)


def _dot(a, b, dims=(((1,), (0,)), ((), ()))):
    return lax.dot_general(a, b, dims, preferred_element_type=F32)


NT = (((1,), (1,)), ((), ()))


MESH = pl.DeviceIdType.MESH


def _stream(x_ref, ws, bufs, sem, acc, emit, extra_start=None, extra_body=None):
    ring, chunk, _ = bufs.shape
    n = ws[0].shape[0] // chunk
    total = n * len(ws)
    part = 512

    def start(g):
        slot = lax.rem(g, ring)
        for i, w in enumerate(ws):
            @pl.when((g >= i * n) & (g < (i + 1) * n))
            def _():
                at = pl.multiple_of((g - i * n) * chunk, chunk)
                pltpu.make_async_copy(w.at[pl.ds(at, chunk)], bufs.at[slot, :, :w.shape[1]], sem.at[slot]).start()
        if extra_start is not None:
            extra_start(g)

    def prime():
        def body(g, c):
            start(g)
            return c
        lax.fori_loop(0, min(ring, total), body, 0)

    def run():
        for i, w in enumerate(ws):
            cols = w.shape[1]
            acc[...] = jnp.zeros_like(acc)

            def body(c, carry):
                g = i * n + c
                slot = lax.rem(g, ring)
                pltpu.make_async_copy(w.at[pl.ds(0, chunk)], bufs.at[slot, :, :cols], sem.at[slot]).wait()
                x = x_ref[:, pl.ds(pl.multiple_of(c * chunk, chunk), chunk)]
                for j in range(0, cols, part):
                    acc[:, j:j + part] += _dot(x, bufs[slot, :, j:j + part])
                if extra_body is not None:
                    extra_body(i, g)
                start(g + ring)
                return carry
            lax.fori_loop(0, n, body, 0)
            emit(i)
    return prime, run


def _peers():
    me = lax.axis_index('ctx')
    return me + 1 - 2 * lax.rem(me, 2), me + 2 - 4 * (me // 2)


def _remote(src, dst, s, r, **to):
    return pltpu.make_async_remote_copy(src_ref=src, dst_ref=dst, send_sem=s, recv_sem=r,
                                        device_id=to, device_id_type=MESH)


def _front_kernel(x_hbm, wq_hbm, wk_hbm, wv_hbm, q_hbm, kn_hbm, vn_hbm,
                  x_ref, bufs, acc, qs, kvn, xsem, sem, osem, q_s, q_r):
    _, heads, _, d = qs.shape
    near, far = _peers()
    cp = pltpu.make_async_copy(x_hbm, x_ref, xsem)
    cp.start()
    hh = heads // 2
    half = [pl.ds(j * hh, hh) for j in range(2)]
    q_near = [_remote(qs.at[0, at], qs.at[1, at], q_s.at[0, j], q_r.at[0, j], ctx=near) for j, at in enumerate(half)]
    q_far = [_remote(qs.at[0, at], qs.at[2, at], q_s.at[1, j], q_r.at[1, j], ctx=far) for j, at in enumerate(half)]
    outs = [pltpu.make_async_copy(qs.at[0], q_hbm.at[0], osem.at[0]),
            pltpu.make_async_copy(kvn.at[0], kn_hbm, osem.at[1]),
            pltpu.make_async_copy(kvn.at[1], vn_hbm, osem.at[2])]
    rest = [pltpu.make_async_copy(qs.at[j], q_hbm.at[j], osem.at[2 + j]) for j in (1, 2)]

    def emit(i):
        if i < 2:
            for h in range(hh):
                qs[0, i * hh + h] = acc[:, h * d:(h + 1) * d].astype(BF16)
            if i == 0:
                pl.semaphore_wait(barrier, 2)
            q_far[i].start()
            q_near[i].start()
        else:
            for h in range(heads):
                kvn[i - 2, h] = acc[:, h * d:(h + 1) * d].astype(BF16)
        if i > 0:
            outs[i - 1].start()

    wq_half = [wq_hbm.at[:, pl.ds(j * hh * d, hh * d)] for j in range(2)]
    prime, run = _stream(x_ref, wq_half + [wk_hbm, wv_hbm], bufs, sem, acc, emit)
    prime()
    barrier = pltpu.get_barrier_semaphore()
    for to in (near, far):
        pl.semaphore_signal(barrier, inc=1, device_id={'ctx': to}, device_id_type=MESH)
    cp.wait()
    run()
    for cs, r in zip((q_near, q_far), rest):
        for c in cs:
            c.wait_recv()
        r.start()
    for c in outs + rest:
        c.wait()
    for c in q_near + q_far:
        c.wait_send()


def _front(x, wq, wk, wv, d):
    rows, depth = x.shape
    cols = wq.shape[1]
    dma = pltpu.SemaphoreType.DMA
    blk = (cols // d, rows, d)
    return pl.pallas_call(
        _front_kernel,
        in_specs=[pl.BlockSpec(memory_space=pl.ANY)] * 4,
        out_specs=[pl.BlockSpec(memory_space=pl.ANY)] * 3,
        out_shape=[jax.ShapeDtypeStruct((3,) + blk, BF16)] + [jax.ShapeDtypeStruct(blk, BF16)] * 2,
        scratch_shapes=[
            VM((rows, depth), BF16), VM((RINGW, CHUNK, cols), BF16), VM((rows, cols), F32),
            VM((3,) + blk, BF16), VM((2,) + blk, BF16),
            dma, dma((RINGW,)), dma((5,)), dma((2, 2)), dma((2, 2))],
        compiler_params=pltpu.CompilerParams(vmem_limit_bytes=LIMIT, collective_id=0, has_side_effects=True),
        cost_estimate=_cost(2e10, 6 * depth * cols),
    )(x, wq, wk, wv)


def _back_kernel(scale, q_hbm, kp_hbm, vp_hbm, suf_hbm, x_hbm, w_hbm, y_hbm,
                 y_ref, raw, qs, kt, vt, suf, x_ref, wo, ds, dr, ns, nr, fo, mo, xs, xr, xl, xlr, att, keep, ps, pr, sb, mb,
                 qsem, ksem, wsem, osem, q_s, q_r, d_s, d_r, n_s, n_r, x_s, x_r, p_s, p_r, y_s, y_r):
    heads, n_pos, d = kt.shape
    rows = x_ref.shape[0]
    rh = rows // 2
    half = x_ref.shape[1] // 2
    near, far = _peers()
    tp = lax.axis_index('tp')
    steps = 4
    group = heads // steps
    wide = ps.shape[-1]
    blocks = half // wide

    barrier = pltpu.get_barrier_semaphore()
    for to in ({'ctx': near}, {'ctx': far}, {'tp': 1 - tp}):
        pl.semaphore_signal(barrier, inc=1, device_id=to, device_id_type=MESH)
    ring, _, pos = raw.shape[:3]
    q_cp = [pltpu.make_async_copy(q_hbm.at[j], qs.at[j], qsem.at[2 + j]) for j in range(3)]
    q_cp[2].start()

    def piece(g):
        slot = lax.rem(g, ring)
        return [pltpu.make_async_copy(src.at[pl.ds(g * pos, pos)], raw.at[slot, j], ksem.at[slot, j])
                for j, src in enumerate((kp_hbm, vp_hbm))]
    for g in range(ring):
        for c in piece(g):
            c.start()
    q_cp[0].start()
    q_cp[1].start()
    suf_cp = pltpu.make_async_copy(suf_hbm, suf, qsem.at[0])
    x_cp = pltpu.make_async_copy(x_hbm, x_ref, qsem.at[1])
    wr = w_hbm.shape[0] // 4
    w_cp = [pltpu.make_async_copy(w_hbm.at[pl.ds(i * wr, wr)], wo.at[pl.ds(i * wr, wr)], wsem.at[i]) for i in range(4)]
    q_diag = _remote(qs.at[2], qs.at[3], q_s.at[0], q_r.at[0], ctx=near)

    def relayout(g, c):
        slot = lax.rem(g, ring)
        for cp in piece(g):
            cp.wait()
        for j, dst in enumerate((kt, vt)):
            for u in range(pos // 16):
                to = pl.multiple_of(g * pos + u * 16, 16)
                dst[:, pl.ds(to, 16), :] = jnp.swapaxes(raw[slot, j, u * 16:u * 16 + 16], 0, 1)

        @pl.when(g + ring < n_pos // pos)
        def _():
            for cp in piece(g + ring):
                cp.start()
        return c
    lax.fori_loop(0, ring, relayout, 0)
    q_cp[2].wait()
    pl.semaphore_wait(barrier, 3)
    q_diag.start()
    lax.fori_loop(ring, n_pos // pos, relayout, 0)
    for c in [suf_cp, x_cp] + w_cp:
        c.start()

    lane = lax.broadcasted_iota(jnp.int32, (rh, d), 1)

    def d_copy(a, i):
        at = pl.ds(i * group, group)
        return _remote(ds.at[a, at], dr.at[a, at], d_s.at[a, i], d_r.at[a, i], ctx=near)

    def n_copy(a, i):
        at = pl.ds(i * group, group)
        return _remote(ns.at[a, at], nr.at[a, at], n_s.at[a, i], n_r.at[a, i], ctx=near)

    def x_copy(a, i):
        at = pl.ds(i * group, group)
        return _remote(xs.at[a, at], xr.at[a, at], x_s.at[a, i], x_r.at[a, i], ctx=far)

    def l_copy(a):
        return _remote(xl.at[a], xlr.at[a], x_s.at[a, steps], x_r.at[a, steps], ctx=far)

    def p_copy(a, j):
        return _remote(ps.at[a, j], pr.at[a, j], p_s.at[a, j], p_r.at[a, j], tp=1 - tp)

    def y_copy(a, j):
        at = (pl.ds(a * rh, rh), pl.ds(pl.multiple_of(tp * half + j * wide, wide), wide))
        return _remote(y_ref.at[at], y_ref.at[at], y_s.at[a, j], y_r.at[a, j], tp=1 - tp)

    def scores(a, h, q0, q1, slot):
        at = pl.ds(pl.multiple_of(a * rh, rh), rh)
        q = jnp.concatenate([qs[q0, h, at], qs[q1, h, at]], axis=0)
        s = _dot(q, kt[h], NT)
        sb[slot] = s
        mb[slot] = jnp.broadcast_to(jnp.max(s, axis=1, keepdims=True) * scale, (rows, d))

    def weigh(h, slot, dst0, dst1):
        m = mb[slot]
        es, l = [], None
        for k in range(0, n_pos, d):
            e = jnp.exp2(sb[slot, :, k:k + d] * scale - m)
            l = e if l is None else l + e
            es.append(e.astype(BF16))
        l = jnp.sum(l, axis=1, keepdims=True)
        o = _dot(jnp.concatenate(es, axis=1), vt[h]) / l
        lse = m + jnp.log2(l)
        dst0[h, 0], dst0[h, 1] = o[:rh], lse[:rh]
        dst1[h, 0], dst1[h, 1] = o[rh:], lse[rh:]

    def attend(i, this, after, dst0, dst1):
        over = (i + 1) // steps
        for u in range(group):
            h = i * group + u
            if u < group - 1:
                scores(this[0], h + 1, this[1], this[2], (u + 1) % 4)
            else:
                to = [t + over * (n - t) for t, n in zip(this, after)]
                scores(to[0], lax.rem(h + 1, heads), to[1], to[2], (u + 1) % 4)
            weigh(h, u % 4, dst0, dst1)

    def merge_far(a, i):
        d_copy(a, i).wait_recv()
        for u in range(group):
            h = i * group + u
            l0, l1 = fo[h, 1], dr[a, h, 1]
            m = jnp.maximum(l0, l1)
            w0, w1 = jnp.exp2(l0 - m), jnp.exp2(l1 - m)
            t = w0 + w1
            xs[a, h] = ((w0 * fo[h, 0] + w1 * dr[a, h, 0]) / t).astype(BF16)
            xl[a] = jnp.where(lane == h, m + jnp.log2(t), xl[a])
        x_copy(a, i).start()

    def add_peer(a, js):
        for j in js:
            p_copy(a, j).wait_recv()
            y = (keep[a, j] + pr[a, j].astype(F32)).astype(BF16)
            y_ref[a * rh:(a + 1) * rh, pl.ds(pl.multiple_of(tp * half + j * wide, wide), wide)] = y
            y_copy(a, j).start()

    xl[...] = jnp.zeros_like(xl)
    q_cp[0].wait()
    q_cp[1].wait()
    q_diag.wait_recv()
    for a in range(2):
        def far_step(i, c):
            attend(i, (a, 3, 2), (a, 1, 0), ds.at[a], fo)
            d_copy(a, i).start()
            if a == 1:
                for j in range(2):
                    @pl.when(i == 2 + j)
                    def _():
                        add_peer(0, [j])

            @pl.when(i > 0)
            def _():
                merge_far(a, i - 1)
            return c
        if a == 0:
            scores(a, 0, 3, 2, 0)
        lax.fori_loop(0, steps, far_step, 0)

        def near_step(i, c):
            attend(i, (a, 1, 0), (1, 3, 2), ns.at[a], mo)
            n_copy(a, i).start()

            @pl.when(i == 0)
            def _():
                merge_far(a, steps - 1)
                l_copy(a).start()
            if a == 1:
                for j in range(2):
                    @pl.when(i == j)
                    def _():
                        add_peer(0, range(2 + j, blocks, 2))
            return c
        lax.fori_loop(0, steps, near_step, 0)

        if a == 0:
            suf_cp.wait()
            x_cp.wait()
        at = slice(a * rh, (a + 1) * rh)
        l_copy(a).wait_recv()
        far_lse, suf_lse = xlr[a], suf[heads, at]
        for h in range(heads):
            if h % group == 0:
                n_copy(a, h // group).wait_recv()
                x_copy(a, h // group).wait_recv()
            ls = [mo[h, 1], nr[a, h, 1], jnp.broadcast_to(far_lse[:, h:h + 1], (rh, d)),
                  jnp.broadcast_to(suf_lse[:, h:h + 1], (rh, d))]
            m = functools.reduce(jnp.maximum, ls)
            ws = [jnp.exp2(l - m) for l in ls]
            o = ws[0] * mo[h, 0] + ws[1] * nr[a, h, 0] + ws[2] * xr[a, h].astype(F32) + ws[3] * suf[h, at]
            att[:, h * d:(h + 1) * d] = (o / functools.reduce(jnp.add, ws)).astype(BF16)
        if a == 0:
            for c in w_cp:
                c.wait()

        def send_block(j, c):
            cols_at = pl.ds(pl.multiple_of((1 - tp) * half + j * wide, wide), wide)
            ps[a, j] = _dot(att[...], wo[:, cols_at]).astype(BF16)
            p_copy(a, j).start()
            return c
        lax.fori_loop(0, blocks, send_block, 0)

        def keep_block(j, c):
            cols_at = pl.ds(pl.multiple_of(tp * half + j * wide, wide), wide)
            keep[a, j] = _dot(att[...], wo[:, cols_at]) + x_ref[at, cols_at].astype(F32)
            return c
        lax.fori_loop(0, blocks, keep_block, 0)

    add_peer(1, range(blocks))
    outs = []
    for a in range(2):
        for j in range(blocks):
            y_copy(a, j).wait_recv()
        at = pl.ds(a * rh, rh)
        outs.append(pltpu.make_async_copy(y_ref.at[at], y_hbm.at[at], osem.at[a]))
        outs[-1].start()
    q_diag.wait_send()
    for a in range(2):
        for j in range(blocks):
            y_copy(a, j).wait_send()
            p_copy(a, j).wait_send()
        for i in range(steps):
            d_copy(a, i).wait_send()
            n_copy(a, i).wait_send()
            x_copy(a, i).wait_send()
        l_copy(a).wait_send()
    for c in outs:
        c.wait()


def _back(q, kp, vp, suf, x, w_o, scale):
    _, heads, rows, d = q.shape
    n = kp.shape[0]
    depth, cols = w_o.shape
    dma = pltpu.SemaphoreType.DMA
    rh, wide, steps = rows // 2, 512, 4
    blocks = cols // 2 // wide
    return pl.pallas_call(
        functools.partial(_back_kernel, scale),
        in_specs=[pl.BlockSpec(memory_space=pl.ANY)] * 6,
        out_specs=pl.BlockSpec(memory_space=pl.ANY),
        out_shape=jax.ShapeDtypeStruct((rows, cols), BF16),
        scratch_shapes=[
            VM((rows, cols), BF16), VM((4, 2, 128, heads, d), BF16),
            VM((4, heads, rows, d), BF16), VM((heads, n, d), BF16), VM((heads, n, d), BF16), VM(suf.shape, F32), VM((rows, cols), BF16),
            VM(w_o.shape, BF16)]
        + [VM((2, heads, 2, rh, d), F32)] * 4 + [VM((heads, 2, rh, d), F32)] * 2
        + [VM((2, heads, rh, d), BF16)] * 2 + [VM((2, rh, d), F32)] * 2
        + [VM((rh, depth), BF16), VM((2, blocks, rh, wide), F32)] + [VM((2, blocks, rh, wide), BF16)] * 2
        + [VM((4, rows, n), F32), VM((4, rows, d), F32)]
        + [dma((5,)), dma((4, 2)), dma((4,)), dma((2,)), dma((1,)), dma((1,))]
        + [dma((2, steps))] * 4 + [dma((2, steps + 1))] * 2 + [dma((2, blocks))] * 4,
        compiler_params=pltpu.CompilerParams(vmem_limit_bytes=62 * 2**20, collective_id=1, has_side_effects=True),
        cost_estimate=_cost(5e10, 2 * depth * cols),
    )(q, kp, vp, suf, x, w_o)


def _suffix_kernel(scale, lens, q_hbm, kn_hbm, vn_hbm, k_hbm, v_hbm, o_hbm,
                   o_ref, osem, new, newsem, items, qb, acc, m_s, l_s, kbuf, vbuf, sbuf, ksem, vsem):
    _, heads, rows, d = new.shape
    news = [pltpu.make_async_copy(src, new.at[j], newsem.at[j])
            for j, src in enumerate((q_hbm.at[0], kn_hbm, vn_hbm))]
    for c in news:
        c.start()
    per = k_hbm.shape[0] // rows
    shift = per.bit_length() - 1
    wide = SLOTS * heads
    dummy = rows * per

    for g in range(BATCH):
        items[g] = dummy

    def listing(b, t):
        for j in range(per):
            items[BATCH + t + j] = b * per + j
        return t + (lens[b] + SLOTS - 1) // SLOTS
    def fetch(i):
        slot = lax.rem(i, RING)
        for g in range(BATCH):
            it = jnp.minimum(items[BATCH + i * BATCH + g], dummy - 1)
            pltpu.make_async_copy(k_hbm.at[it], kbuf.at[slot, g], ksem.at[slot]).start()
            pltpu.make_async_copy(v_hbm.at[it], vbuf.at[slot, g], vsem.at[slot]).start()

    def prime(i, c):
        fetch(i)
        return c
    some = lax.fori_loop(0, rows // 4, listing, 0, unroll=4)
    early = jnp.minimum(some // BATCH, RING - 1)
    lax.fori_loop(0, early, prime, 0)
    total = lax.fori_loop(rows // 4, rows, listing, some, unroll=4)
    for g in range(2 * BATCH):
        items[BATCH + total + g] = dummy
    batches = (total + BATCH - 1) // BATCH
    lax.fori_loop(early, jnp.minimum(batches, RING - 1), prime, 0)

    for c in news:
        c.wait()
    for c in range(rows // 16):
        q, kn, vn = [jnp.swapaxes(new[j, :, c * 16:c * 16 + 16, :], 0, 1) for j in range(3)]
        qb[c * 16:c * 16 + 16] = q
        s = jnp.sum(q.astype(F32) * kn.astype(F32), axis=-1, keepdims=True) * scale
        m_s[c * 16:c * 16 + 16] = jnp.broadcast_to(s, (16, heads, 128))
        l_s[c * 16:c * 16 + 16] = jnp.ones((16, heads, 128), F32)
        acc[c * 16:c * 16 + 16] = vn.astype(F32)

    row = lax.broadcasted_iota(jnp.int32, (heads, wide), 0)
    col = lax.broadcasted_iota(jnp.int32, (heads, wide), 1)
    slot_of = jnp.where(lax.rem(col, heads) == row, col // heads, 1 << 20)

    def step(i, c):
        slot = lax.rem(i, RING)
        last = lax.rem(i + RING - 1, RING)
        par = lax.rem(i, 2)

        @pl.when(i < batches)
        def _():
            pltpu.make_async_copy(k_hbm.at[pl.ds(0, BATCH)], kbuf.at[slot], ksem.at[slot]).wait()

        @pl.when(i > 0)
        def _():
            pltpu.make_async_copy(v_hbm.at[pl.ds(0, BATCH)], vbuf.at[last], vsem.at[last]).wait()

        for g in range(BATCH):
            it = items[BATCH + i * BATCH + g]
            b = lax.shift_right_logical(it, shift)
            left = lens[jnp.minimum(b, rows - 1)] - (it & (per - 1)) * SLOTS
            s = _dot(qb[b], kbuf[slot, g], NT) * scale
            sbuf[par, g] = jnp.where(slot_of < left, s, -jnp.inf)

        parts = []
        for g in range(0, BATCH, 2):
            ps = []
            for u in range(2):
                s = sbuf[1 - par, g + u]
                m = jnp.max(s, axis=1, keepdims=True)
                p = jnp.exp2(s - m)
                parts.append([m, jnp.sum(p, axis=1, keepdims=True), None])
                ps.append(p.astype(BF16))
            o = _dot(jnp.concatenate(ps, axis=0),
                     jnp.concatenate([vbuf[last, g], vbuf[last, g + 1]], axis=1))
            parts[g][2] = o[:heads, :d]
            parts[g + 1][2] = o[heads:, d:]
        for g in range(BATCH):
            b = lax.shift_right_logical(items[i * BATCH + g], shift)
            m, l, o = parts[g]
            m_old = m_s[b]
            m_new = jnp.maximum(m_old, m)
            w_old = jnp.exp2(m_old - m_new)
            w = jnp.exp2(m - m_new)
            m_s[b] = m_new
            l_s[b] = l_s[b] * w_old + l * w
            acc[b] = acc[b] * w_old + o * w

        @pl.when(i + RING - 1 < batches)
        def _():
            fetch(i + RING - 1)
        return c

    lax.fori_loop(0, batches + 1, step, 0)

    def leave(c):
        at = pl.ds(c * 16, 16)
        return pltpu.make_async_copy(o_ref.at[:, at], o_hbm.at[:, at], osem.at[c])

    lane = lax.broadcasted_iota(jnp.int32, (16, 128), 1)
    for c in range(rows // 16):
        l = l_s[c * 16:c * 16 + 16]
        o = acc[c * 16:c * 16 + 16] / l
        lse = m_s[c * 16:c * 16 + 16] + jnp.log2(l)
        o_ref[:heads, c * 16:c * 16 + 16, :] = jnp.swapaxes(o, 0, 1)
        lse = jnp.swapaxes(lse, 0, 1)
        out = jnp.zeros((16, 128), F32)
        for h in range(heads):
            out = jnp.where(lane == h, lse[h], out)
        o_ref[heads, c * 16:c * 16 + 16, :] = out
        leave(c).start()
    for c in range(rows // 16):
        leave(c).wait()


def _suffix(lens, q, kn, vn, k, v, scale):
    _, heads, rows, d = q.shape
    slots = k.shape[1]
    per = slots // SLOTS
    wide = SLOTS * heads
    k = k.reshape(rows * per, wide, d)
    v = v.reshape(rows * per, wide, d)
    return pl.pallas_call(
        functools.partial(_suffix_kernel, scale),
        in_specs=[pl.BlockSpec(memory_space=pltpu.SMEM)] + [pl.BlockSpec(memory_space=pl.ANY)] * 5,
        out_specs=pl.BlockSpec(memory_space=pl.ANY),
        out_shape=jax.ShapeDtypeStruct((heads + 1, rows, d), F32),
        scratch_shapes=[
            VM((heads + 1, rows, d), F32),
            pltpu.SemaphoreType.DMA((rows // 16,)),
            VM((3, heads, rows, d), BF16),
            pltpu.SemaphoreType.DMA((3,)),
            pltpu.SMEM((rows * per + 4 * BATCH,), jnp.int32),
            VM((rows + 1, heads, d), BF16),
            VM((rows + 1, heads, d), F32),
            VM((rows + 1, heads, 128), F32),
            VM((rows + 1, heads, 128), F32),
            VM((RING, BATCH, wide, d), BF16),
            VM((RING, BATCH, wide, d), BF16),
            VM((2, BATCH, heads, wide), F32),
            pltpu.SemaphoreType.DMA((RING,)),
            pltpu.SemaphoreType.DMA((RING,)),
        ],
        compiler_params=pltpu.CompilerParams(vmem_limit_bytes=LIMIT),
        cost_estimate=_cost(2e10, 4 * k.size),
    )(lens, q, kn, vn, k, v)


def solution(mesh):
    row_axes = ('dp', 'ctx')
    def device_step(hidden, w_q, w_k, w_v, w_o, k_prefix, v_prefix, k_suffix, v_suffix, seq_lens):
        scale = LOG2E * k_prefix.shape[2] ** -0.5
        q, kn, vn = _front(hidden, w_q, w_k, w_v, k_prefix.shape[2])
        suf = _suffix(seq_lens, q, kn, vn, k_suffix, v_suffix, scale)
        return _back(q, k_prefix, v_prefix, suf, hidden, w_o, scale)

    spec_in = (P(row_axes, None), P(None, 'tp'), P(None, 'tp'), P(None, 'tp'), P('tp', None),
               P(row_axes, 'tp', None), P(row_axes, 'tp', None), P(row_axes, None, 'tp', None),
               P(row_axes, None, 'tp', None), P(row_axes))
    return jax.shard_map(device_step, mesh=mesh, in_specs=spec_in, out_specs=P(row_axes, None), check_vma=False)
```

```python
import functools

import jax
import jax.numpy as jnp
from jax import lax
from jax.experimental import pallas as pl
from jax.experimental.pallas import tpu as pltpu
from jax.sharding import PartitionSpec as P

F32 = jnp.float32
BF16 = jnp.bfloat16
VM = pltpu.VMEM
LOG2E = 1.4426950408889634
BATCH = 16
SLOTS = 16
RING = 6
CHUNK = 512
RINGW = 6
LIMIT = 56 * 2**20


def _cost(flops, nbytes):
    return pl.CostEstimate(flops=int(flops), bytes_accessed=int(nbytes), transcendentals=0)


def _dot(a, b, dims=(((1,), (0,)), ((), ()))):
    return lax.dot_general(a, b, dims, preferred_element_type=F32)


NT = (((1,), (1,)), ((), ()))


MESH = pl.DeviceIdType.MESH


def _stream(x_ref, ws, bufs, sem, acc, emit, extra_start=None, extra_body=None):
    ring, chunk, _ = bufs.shape
    n = ws[0].shape[0] // chunk
    total = n * len(ws)
    part = 512

    def start(g):
        slot = lax.rem(g, ring)
        for i, w in enumerate(ws):
            @pl.when((g >= i * n) & (g < (i + 1) * n))
            def _():
                at = pl.multiple_of((g - i * n) * chunk, chunk)
                pltpu.make_async_copy(w.at[pl.ds(at, chunk)], bufs.at[slot, :, :w.shape[1]], sem.at[slot]).start()
        if extra_start is not None:
            extra_start(g)

    def prime():
        def body(g, c):
            start(g)
            return c
        lax.fori_loop(0, min(ring, total), body, 0)

    def run():
        for i, w in enumerate(ws):
            cols = w.shape[1]
            acc[...] = jnp.zeros_like(acc)

            def body(c, carry):
                g = i * n + c
                slot = lax.rem(g, ring)
                pltpu.make_async_copy(w.at[pl.ds(0, chunk)], bufs.at[slot, :, :cols], sem.at[slot]).wait()
                x = x_ref[:, pl.ds(pl.multiple_of(c * chunk, chunk), chunk)]
                for j in range(0, cols, part):
                    acc[:, j:j + part] += _dot(x, bufs[slot, :, j:j + part])
                if extra_body is not None:
                    extra_body(i, g)
                start(g + ring)
                return carry
            lax.fori_loop(0, n, body, 0)
            emit(i)
    return prime, run


def _peers():
    me = lax.axis_index('ctx')
    return me + 1 - 2 * lax.rem(me, 2), me + 2 - 4 * (me // 2)


def _remote(src, dst, s, r, **to):
    return pltpu.make_async_remote_copy(src_ref=src, dst_ref=dst, send_sem=s, recv_sem=r,
                                        device_id=to, device_id_type=MESH)


def _front_kernel(x_hbm, wq_hbm, wk_hbm, wv_hbm, q_hbm, kn_hbm, vn_hbm,
                  x_ref, bufs, acc, qs, kvn, xsem, sem, osem, q_s, q_r):
    _, heads, _, d = qs.shape
    near, far = _peers()
    cp = pltpu.make_async_copy(x_hbm, x_ref, xsem)
    cp.start()
    hh = heads // 2
    half = [pl.ds(j * hh, hh) for j in range(2)]
    q_near = [_remote(qs.at[0, at], qs.at[1, at], q_s.at[0, j], q_r.at[0, j], ctx=near) for j, at in enumerate(half)]
    q_far = [_remote(qs.at[0, at], qs.at[2, at], q_s.at[1, j], q_r.at[1, j], ctx=far) for j, at in enumerate(half)]
    outs = [pltpu.make_async_copy(qs.at[0], q_hbm.at[0], osem.at[0]),
            pltpu.make_async_copy(kvn.at[0], kn_hbm, osem.at[1]),
            pltpu.make_async_copy(kvn.at[1], vn_hbm, osem.at[2])]
    rest = [pltpu.make_async_copy(qs.at[j], q_hbm.at[j], osem.at[2 + j]) for j in (1, 2)]

    def emit(i):
        if i < 2:
            for h in range(hh):
                qs[0, i * hh + h] = acc[:, h * d:(h + 1) * d].astype(BF16)
            if i == 0:
                pl.semaphore_wait(barrier, 2)
            q_far[i].start()
            q_near[i].start()
        else:
            for h in range(heads):
                kvn[i - 2, h] = acc[:, h * d:(h + 1) * d].astype(BF16)
        if i > 0:
            outs[i - 1].start()

    wq_half = [wq_hbm.at[:, pl.ds(j * hh * d, hh * d)] for j in range(2)]
    prime, run = _stream(x_ref, wq_half + [wk_hbm, wv_hbm], bufs, sem, acc, emit)
    prime()
    barrier = pltpu.get_barrier_semaphore()
    for to in (near, far):
        pl.semaphore_signal(barrier, inc=1, device_id={'ctx': to}, device_id_type=MESH)
    cp.wait()
    run()
    for cs, r in zip((q_near, q_far), rest):
        for c in cs:
            c.wait_recv()
        r.start()
    for c in outs + rest:
        c.wait()
    for c in q_near + q_far:
        c.wait_send()


def _front(x, wq, wk, wv, d):
    rows, depth = x.shape
    cols = wq.shape[1]
    dma = pltpu.SemaphoreType.DMA
    blk = (cols // d, rows, d)
    return pl.pallas_call(
        _front_kernel,
        in_specs=[pl.BlockSpec(memory_space=pl.ANY)] * 4,
        out_specs=[pl.BlockSpec(memory_space=pl.ANY)] * 3,
        out_shape=[jax.ShapeDtypeStruct((3,) + blk, BF16)] + [jax.ShapeDtypeStruct(blk, BF16)] * 2,
        scratch_shapes=[
            VM((rows, depth), BF16), VM((RINGW, CHUNK, cols), BF16), VM((rows, cols), F32),
            VM((3,) + blk, BF16), VM((2,) + blk, BF16),
            dma, dma((RINGW,)), dma((5,)), dma((2, 2)), dma((2, 2))],
        compiler_params=pltpu.CompilerParams(vmem_limit_bytes=LIMIT, collective_id=0, has_side_effects=True),
        cost_estimate=_cost(2e10, 6 * depth * cols),
    )(x, wq, wk, wv)


def _back_kernel(scale, q_hbm, kp_hbm, vp_hbm, suf_hbm, x_hbm, w_hbm, y_hbm,
                 y_ref, raw, qs, kt, vt, suf, x_ref, wo, ds, dr, ns, nr, fo, mo, xs, xr, xl, xlr, att, keep, ps, pr, sb, mb,
                 qsem, ksem, wsem, osem, q_s, q_r, d_s, d_r, n_s, n_r, x_s, x_r, p_s, p_r, y_s, y_r):
    heads, n_pos, d = kt.shape
    rows = x_ref.shape[0]
    rh = rows // 2
    half = x_ref.shape[1] // 2
    near, far = _peers()
    tp = lax.axis_index('tp')
    steps = 4
    group = heads // steps
    wide = ps.shape[-1]
    blocks = half // wide

    barrier = pltpu.get_barrier_semaphore()
    for to in ({'ctx': near}, {'ctx': far}, {'tp': 1 - tp}):
        pl.semaphore_signal(barrier, inc=1, device_id=to, device_id_type=MESH)
    ring, _, pos = raw.shape[:3]
    q_cp = [pltpu.make_async_copy(q_hbm.at[j], qs.at[j], qsem.at[2 + j]) for j in range(3)]
    q_cp[2].start()

    def piece(g):
        slot = lax.rem(g, ring)
        return [pltpu.make_async_copy(src.at[pl.ds(g * pos, pos)], raw.at[slot, j], ksem.at[slot, j])
                for j, src in enumerate((kp_hbm, vp_hbm))]
    for g in range(ring):
        for c in piece(g):
            c.start()
    q_cp[0].start()
    q_cp[1].start()
    suf_cp = pltpu.make_async_copy(suf_hbm, suf, qsem.at[0])
    x_cp = pltpu.make_async_copy(x_hbm, x_ref, qsem.at[1])
    wr = w_hbm.shape[0] // 4
    w_cp = [pltpu.make_async_copy(w_hbm.at[pl.ds(i * wr, wr)], wo.at[pl.ds(i * wr, wr)], wsem.at[i]) for i in range(4)]
    q_diag = _remote(qs.at[2], qs.at[3], q_s.at[0], q_r.at[0], ctx=near)

    def relayout(g, c):
        slot = lax.rem(g, ring)
        for cp in piece(g):
            cp.wait()
        for j, dst in enumerate((kt, vt)):
            for u in range(pos // 16):
                to = pl.multiple_of(g * pos + u * 16, 16)
                dst[:, pl.ds(to, 16), :] = jnp.swapaxes(raw[slot, j, u * 16:u * 16 + 16], 0, 1)

        @pl.when(g + ring < n_pos // pos)
        def _():
            for cp in piece(g + ring):
                cp.start()
        return c
    lax.fori_loop(0, ring, relayout, 0)
    q_cp[2].wait()
    pl.semaphore_wait(barrier, 3)
    q_diag.start()
    lax.fori_loop(ring, n_pos // pos, relayout, 0)
    for c in [suf_cp, x_cp] + w_cp:
        c.start()

    lane = lax.broadcasted_iota(jnp.int32, (rh, d), 1)

    def d_copy(a, i):
        at = pl.ds(i * group, group)
        return _remote(ds.at[a, at], dr.at[a, at], d_s.at[a, i], d_r.at[a, i], ctx=near)

    def n_copy(a, i):
        at = pl.ds(i * group, group)
        return _remote(ns.at[a, at], nr.at[a, at], n_s.at[a, i], n_r.at[a, i], ctx=near)

    def x_copy(a, i):
        at = pl.ds(i * group, group)
        return _remote(xs.at[a, at], xr.at[a, at], x_s.at[a, i], x_r.at[a, i], ctx=far)

    def l_copy(a):
        return _remote(xl.at[a], xlr.at[a], x_s.at[a, steps], x_r.at[a, steps], ctx=far)

    def p_copy(a, j):
        return _remote(ps.at[a, j], pr.at[a, j], p_s.at[a, j], p_r.at[a, j], tp=1 - tp)

    def y_copy(a, j):
        at = (pl.ds(a * rh, rh), pl.ds(pl.multiple_of(tp * half + j * wide, wide), wide))
        return _remote(y_ref.at[at], y_ref.at[at], y_s.at[a, j], y_r.at[a, j], tp=1 - tp)

    def scores(a, h, q0, q1, slot):
        at = pl.ds(pl.multiple_of(a * rh, rh), rh)
        q = jnp.concatenate([qs[q0, h, at], qs[q1, h, at]], axis=0)
        s = _dot(q, kt[h], NT)
        sb[slot] = s
        mb[slot] = jnp.broadcast_to(jnp.max(s, axis=1, keepdims=True) * scale, (rows, d))

    def weigh(h, slot, dst0, dst1):
        m = mb[slot]
        es, l = [], None
        for k in range(0, n_pos, d):
            e = jnp.exp2(sb[slot, :, k:k + d] * scale - m)
            l = e if l is None else l + e
            es.append(e.astype(BF16))
        l = jnp.sum(l, axis=1, keepdims=True)
        o = _dot(jnp.concatenate(es, axis=1), vt[h]) / l
        lse = m + jnp.log2(l)
        dst0[h, 0], dst0[h, 1] = o[:rh], lse[:rh]
        dst1[h, 0], dst1[h, 1] = o[rh:], lse[rh:]

    def attend(i, this, after, dst0, dst1):
        over = (i + 1) // steps
        for u in range(group):
            h = i * group + u
            if u < group - 1:
                scores(this[0], h + 1, this[1], this[2], (u + 1) % 4)
            else:
                to = [t + over * (n - t) for t, n in zip(this, after)]
                scores(to[0], lax.rem(h + 1, heads), to[1], to[2], (u + 1) % 4)
            weigh(h, u % 4, dst0, dst1)

    def merge_far(a, i):
        d_copy(a, i).wait_recv()
        for u in range(group):
            h = i * group + u
            l0, l1 = fo[h, 1], dr[a, h, 1]
            m = jnp.maximum(l0, l1)
            w0, w1 = jnp.exp2(l0 - m), jnp.exp2(l1 - m)
            t = w0 + w1
            xs[a, h] = ((w0 * fo[h, 0] + w1 * dr[a, h, 0]) / t).astype(BF16)
            xl[a] = jnp.where(lane == h, m + jnp.log2(t), xl[a])
        x_copy(a, i).start()

    def add_peer(a, js):
        for j in js:
            p_copy(a, j).wait_recv()
            y = (keep[a, j] + pr[a, j].astype(F32)).astype(BF16)
            y_ref[a * rh:(a + 1) * rh, pl.ds(pl.multiple_of(tp * half + j * wide, wide), wide)] = y
            y_copy(a, j).start()

    xl[...] = jnp.zeros_like(xl)
    q_cp[0].wait()
    q_cp[1].wait()
    q_diag.wait_recv()
    for a in range(2):
        def far_step(i, c):
            attend(i, (a, 3, 2), (a, 1, 0), ds.at[a], fo)
            d_copy(a, i).start()
            if a == 1:
                for j in range(2):
                    @pl.when(i == 2 + j)
                    def _():
                        add_peer(0, [j])

            @pl.when(i > 0)
            def _():
                merge_far(a, i - 1)
            return c
        if a == 0:
            scores(a, 0, 3, 2, 0)
        lax.fori_loop(0, steps, far_step, 0)

        def near_step(i, c):
            attend(i, (a, 1, 0), (1, 3, 2), ns.at[a], mo)
            n_copy(a, i).start()

            @pl.when(i == 0)
            def _():
                merge_far(a, steps - 1)
                l_copy(a).start()
            if a == 1:
                for j in range(2):
                    @pl.when(i == j)
                    def _():
                        add_peer(0, range(2 + j, blocks, 2))
            return c
        lax.fori_loop(0, steps, near_step, 0)

        if a == 0:
            suf_cp.wait()
            x_cp.wait()
        at = slice(a * rh, (a + 1) * rh)
        l_copy(a).wait_recv()
        far_lse, suf_lse = xlr[a], suf[heads, at]
        for h in range(heads):
            if h % group == 0:
                n_copy(a, h // group).wait_recv()
                x_copy(a, h // group).wait_recv()
            ls = [mo[h, 1], nr[a, h, 1], jnp.broadcast_to(far_lse[:, h:h + 1], (rh, d)),
                  jnp.broadcast_to(suf_lse[:, h:h + 1], (rh, d))]
            m = functools.reduce(jnp.maximum, ls)
            ws = [jnp.exp2(l - m) for l in ls]
            o = ws[0] * mo[h, 0] + ws[1] * nr[a, h, 0] + ws[2] * xr[a, h].astype(F32) + ws[3] * suf[h, at]
            att[:, h * d:(h + 1) * d] = (o / functools.reduce(jnp.add, ws)).astype(BF16)
        if a == 0:
            for c in w_cp:
                c.wait()

        def send_block(j, c):
            cols_at = pl.ds(pl.multiple_of((1 - tp) * half + j * wide, wide), wide)
            ps[a, j] = _dot(att[...], wo[:, cols_at]).astype(BF16)
            p_copy(a, j).start()
            return c
        lax.fori_loop(0, blocks, send_block, 0)

        def keep_block(j, c):
            cols_at = pl.ds(pl.multiple_of(tp * half + j * wide, wide), wide)
            keep[a, j] = _dot(att[...], wo[:, cols_at]) + x_ref[at, cols_at].astype(F32)
            return c
        lax.fori_loop(0, blocks, keep_block, 0)

    outs = []
    for a in range(2):
        if a == 1:
            add_peer(1, range(blocks))
        for j in range(blocks):
            y_copy(a, j).wait_recv()
        at = pl.ds(a * rh, rh)
        outs.append(pltpu.make_async_copy(y_ref.at[at], y_hbm.at[at], osem.at[a]))
        outs[-1].start()
    q_diag.wait_send()
    for a in range(2):
        for j in range(blocks):
            y_copy(a, j).wait_send()
            p_copy(a, j).wait_send()
        for i in range(steps):
            d_copy(a, i).wait_send()
            n_copy(a, i).wait_send()
            x_copy(a, i).wait_send()
        l_copy(a).wait_send()
    for c in outs:
        c.wait()


def _back(q, kp, vp, suf, x, w_o, scale):
    _, heads, rows, d = q.shape
    n = kp.shape[0]
    depth, cols = w_o.shape
    dma = pltpu.SemaphoreType.DMA
    rh, wide, steps = rows // 2, 512, 4
    blocks = cols // 2 // wide
    return pl.pallas_call(
        functools.partial(_back_kernel, scale),
        in_specs=[pl.BlockSpec(memory_space=pl.ANY)] * 6,
        out_specs=pl.BlockSpec(memory_space=pl.ANY),
        out_shape=jax.ShapeDtypeStruct((rows, cols), BF16),
        scratch_shapes=[
            VM((rows, cols), BF16), VM((4, 2, 128, heads, d), BF16),
            VM((4, heads, rows, d), BF16), VM((heads, n, d), BF16), VM((heads, n, d), BF16), VM(suf.shape, F32), VM((rows, cols), BF16),
            VM(w_o.shape, BF16)]
        + [VM((2, heads, 2, rh, d), F32)] * 4 + [VM((heads, 2, rh, d), F32)] * 2
        + [VM((2, heads, rh, d), BF16)] * 2 + [VM((2, rh, d), F32)] * 2
        + [VM((rh, depth), BF16), VM((2, blocks, rh, wide), F32)] + [VM((2, blocks, rh, wide), BF16)] * 2
        + [VM((4, rows, n), F32), VM((4, rows, d), F32)]
        + [dma((5,)), dma((4, 2)), dma((4,)), dma((2,)), dma((1,)), dma((1,))]
        + [dma((2, steps))] * 4 + [dma((2, steps + 1))] * 2 + [dma((2, blocks))] * 4,
        compiler_params=pltpu.CompilerParams(vmem_limit_bytes=62 * 2**20, collective_id=1, has_side_effects=True),
        cost_estimate=_cost(5e10, 2 * depth * cols),
    )(q, kp, vp, suf, x, w_o)


def _suffix_kernel(scale, lens, q_hbm, kn_hbm, vn_hbm, k_hbm, v_hbm, o_hbm,
                   o_ref, osem, new, newsem, items, qb, acc, m_s, l_s, kbuf, vbuf, sbuf, ksem, vsem):
    _, heads, rows, d = new.shape
    news = [pltpu.make_async_copy(src, new.at[j], newsem.at[j])
            for j, src in enumerate((q_hbm.at[0], kn_hbm, vn_hbm))]
    for c in news:
        c.start()
    per = k_hbm.shape[0] // rows
    shift = per.bit_length() - 1
    wide = SLOTS * heads
    dummy = rows * per

    for g in range(BATCH):
        items[g] = dummy

    def listing(b, t):
        for j in range(per):
            items[BATCH + t + j] = b * per + j
        return t + (lens[b] + SLOTS - 1) // SLOTS
    def fetch(i):
        slot = lax.rem(i, RING)
        for g in range(BATCH):
            it = jnp.minimum(items[BATCH + i * BATCH + g], dummy - 1)
            pltpu.make_async_copy(k_hbm.at[it], kbuf.at[slot, g], ksem.at[slot]).start()
            pltpu.make_async_copy(v_hbm.at[it], vbuf.at[slot, g], vsem.at[slot]).start()

    def prime(i, c):
        fetch(i)
        return c
    some = lax.fori_loop(0, rows // 4, listing, 0, unroll=4)
    early = jnp.minimum(some // BATCH, RING - 1)
    lax.fori_loop(0, early, prime, 0)
    total = lax.fori_loop(rows // 4, rows, listing, some, unroll=4)
    for g in range(2 * BATCH):
        items[BATCH + total + g] = dummy
    batches = (total + BATCH - 1) // BATCH
    lax.fori_loop(early, jnp.minimum(batches, RING - 1), prime, 0)

    for c in news:
        c.wait()
    for c in range(rows // 16):
        q, kn, vn = [jnp.swapaxes(new[j, :, c * 16:c * 16 + 16, :], 0, 1) for j in range(3)]
        qb[c * 16:c * 16 + 16] = q
        s = jnp.sum(q.astype(F32) * kn.astype(F32), axis=-1, keepdims=True) * scale
        m_s[c * 16:c * 16 + 16] = jnp.broadcast_to(s, (16, heads, 128))
        l_s[c * 16:c * 16 + 16] = jnp.ones((16, heads, 128), F32)
        acc[c * 16:c * 16 + 16] = vn.astype(F32)

    row = lax.broadcasted_iota(jnp.int32, (heads, wide), 0)
    col = lax.broadcasted_iota(jnp.int32, (heads, wide), 1)
    slot_of = jnp.where(lax.rem(col, heads) == row, col // heads, 1 << 20)

    def step(i, c):
        slot = lax.rem(i, RING)
        last = lax.rem(i + RING - 1, RING)
        par = lax.rem(i, 2)

        @pl.when(i < batches)
        def _():
            pltpu.make_async_copy(k_hbm.at[pl.ds(0, BATCH)], kbuf.at[slot], ksem.at[slot]).wait()

        @pl.when(i > 0)
        def _():
            pltpu.make_async_copy(v_hbm.at[pl.ds(0, BATCH)], vbuf.at[last], vsem.at[last]).wait()

        for g in range(BATCH):
            it = items[BATCH + i * BATCH + g]
            b = lax.shift_right_logical(it, shift)
            left = lens[jnp.minimum(b, rows - 1)] - (it & (per - 1)) * SLOTS
            s = _dot(qb[b], kbuf[slot, g], NT) * scale
            sbuf[par, g] = jnp.where(slot_of < left, s, -jnp.inf)

        parts = []
        for g in range(0, BATCH, 2):
            ps = []
            for u in range(2):
                s = sbuf[1 - par, g + u]
                m = jnp.max(s, axis=1, keepdims=True)
                p = jnp.exp2(s - m)
                parts.append([m, jnp.sum(p, axis=1, keepdims=True), None])
                ps.append(p.astype(BF16))
            o = _dot(jnp.concatenate(ps, axis=0),
                     jnp.concatenate([vbuf[last, g], vbuf[last, g + 1]], axis=1))
            parts[g][2] = o[:heads, :d]
            parts[g + 1][2] = o[heads:, d:]
        for g in range(BATCH):
            b = lax.shift_right_logical(items[i * BATCH + g], shift)
            m, l, o = parts[g]
            m_old = m_s[b]
            m_new = jnp.maximum(m_old, m)
            w_old = jnp.exp2(m_old - m_new)
            w = jnp.exp2(m - m_new)
            m_s[b] = m_new
            l_s[b] = l_s[b] * w_old + l * w
            acc[b] = acc[b] * w_old + o * w

        @pl.when(i + RING - 1 < batches)
        def _():
            fetch(i + RING - 1)
        return c

    lax.fori_loop(0, batches + 1, step, 0)

    def leave(c):
        at = pl.ds(c * 16, 16)
        return pltpu.make_async_copy(o_ref.at[:, at], o_hbm.at[:, at], osem.at[c])

    lane = lax.broadcasted_iota(jnp.int32, (16, 128), 1)
    for c in range(rows // 16):
        l = l_s[c * 16:c * 16 + 16]
        o = acc[c * 16:c * 16 + 16] / l
        lse = m_s[c * 16:c * 16 + 16] + jnp.log2(l)
        o_ref[:heads, c * 16:c * 16 + 16, :] = jnp.swapaxes(o, 0, 1)
        lse = jnp.swapaxes(lse, 0, 1)
        out = jnp.zeros((16, 128), F32)
        for h in range(heads):
            out = jnp.where(lane == h, lse[h], out)
        o_ref[heads, c * 16:c * 16 + 16, :] = out
        leave(c).start()
    for c in range(rows // 16):
        leave(c).wait()


def _suffix(lens, q, kn, vn, k, v, scale):
    _, heads, rows, d = q.shape
    slots = k.shape[1]
    per = slots // SLOTS
    wide = SLOTS * heads
    k = k.reshape(rows * per, wide, d)
    v = v.reshape(rows * per, wide, d)
    return pl.pallas_call(
        functools.partial(_suffix_kernel, scale),
        in_specs=[pl.BlockSpec(memory_space=pltpu.SMEM)] + [pl.BlockSpec(memory_space=pl.ANY)] * 5,
        out_specs=pl.BlockSpec(memory_space=pl.ANY),
        out_shape=jax.ShapeDtypeStruct((heads + 1, rows, d), F32),
        scratch_shapes=[
            VM((heads + 1, rows, d), F32),
            pltpu.SemaphoreType.DMA((rows // 16,)),
            VM((3, heads, rows, d), BF16),
            pltpu.SemaphoreType.DMA((3,)),
            pltpu.SMEM((rows * per + 4 * BATCH,), jnp.int32),
            VM((rows + 1, heads, d), BF16),
            VM((rows + 1, heads, d), F32),
            VM((rows + 1, heads, 128), F32),
            VM((rows + 1, heads, 128), F32),
            VM((RING, BATCH, wide, d), BF16),
            VM((RING, BATCH, wide, d), BF16),
            VM((2, BATCH, heads, wide), F32),
            pltpu.SemaphoreType.DMA((RING,)),
            pltpu.SemaphoreType.DMA((RING,)),
        ],
        compiler_params=pltpu.CompilerParams(vmem_limit_bytes=LIMIT),
        cost_estimate=_cost(2e10, 4 * k.size),
    )(lens, q, kn, vn, k, v)


def solution(mesh):
    row_axes = ('dp', 'ctx')
    def device_step(hidden, w_q, w_k, w_v, w_o, k_prefix, v_prefix, k_suffix, v_suffix, seq_lens):
        scale = LOG2E * k_prefix.shape[2] ** -0.5
        q, kn, vn = _front(hidden, w_q, w_k, w_v, k_prefix.shape[2])
        suf = _suffix(seq_lens, q, kn, vn, k_suffix, v_suffix, scale)
        return _back(q, k_prefix, v_prefix, suf, hidden, w_o, scale)

    spec_in = (P(row_axes, None), P(None, 'tp'), P(None, 'tp'), P(None, 'tp'), P('tp', None),
               P(row_axes, 'tp', None), P(row_axes, 'tp', None), P(row_axes, None, 'tp', None),
               P(row_axes, None, 'tp', None), P(row_axes))
    return jax.shard_map(device_step, mesh=mesh, in_specs=spec_in, out_specs=P(row_axes, None), check_vma=False)
```
